16 devices in a mesh: fsdp: 16 (over z, y, x, core).
Axes of the slice: x: 2, y: 2, z: 2, core: 2. Of those that a mesh axis runs over, the one named last changes fastest.
Arguments:
- act_in: bfloat16 [512, 49, 512], P('fsdp')
- labels: int32 [512], P('fsdp')
- layer_p: float32 [2, 2127872], P(None, 'fsdp')
- head_w: float32 [512, 1000], P('fsdp')
- small_p: float32 [2048], P('fsdp')
- layer_m: float32 [2, 2127872], P(None, 'fsdp')
- head_m: float32 [512, 1000], P('fsdp')
- small_m: float32 [2048], P('fsdp')
- layer_v: float32 [2, 2127872], P(None, 'fsdp')
- head_v: float32 [512, 1000], P('fsdp')
- small_v: float32 [2048], P('fsdp')
Outputs:
- output 1: float32 [], replicated
- output 2: float32 [2, 2127872], P(None, 'fsdp')
- output 3: float32 [512, 1000], P('fsdp')
- output 4: float32 [2048], P('fsdp')
- output 5: float32 [2, 2127872], P(None, 'fsdp')
- output 6: float32 [512, 1000], P('fsdp')
- output 7: float32 [2048], P('fsdp')
- output 8: float32 [2, 2127872], P(None, 'fsdp')
- output 9: float32 [512, 1000], P('fsdp')
- output 10: float32 [2048], P('fsdp')
All inputs are finite; a program needn't handle non-finite values.
Results may differ from the reference program's by a relative error of at most 0.001.
Values are sent between devices in bfloat16 or wider.
A program may use at most 1 GiB of HBM per device.

```python
import jax
import jax.numpy as jnp
from jax import lax

CHANNELS = 512
TOKENS = 49
TOKEN_HID = 256
CHAN_HID = 2048
CLASSES = 1000
BATCH_DEV = 32
FSDP_DEVS = 16
ADAM_STEP = 10

GLOBAL_BATCH = BATCH_DEV * FSDP_DEVS
PAD_UNIT = 128 * FSDP_DEVS
MAT_LEN = 2 * TOKENS * TOKEN_HID + 2 * CHANNELS * CHAN_HID
LAYER_LEN = MAT_LEN + 5 * CHANNELS + TOKEN_HID + TOKENS + CHAN_HID
LAYER_PAD = (LAYER_LEN + PAD_UNIT - 1) // PAD_UNIT * PAD_UNIT
SMALL_LEN = 2 * CHANNELS + CLASSES
SMALL_PAD = (SMALL_LEN + PAD_UNIT - 1) // PAD_UNIT * PAD_UNIT
PIECE_SIZES = (TOKENS * TOKEN_HID, TOKEN_HID * TOKENS, CHANNELS * CHAN_HID, CHAN_HID * CHANNELS, CHANNELS, CHANNELS, TOKEN_HID, TOKENS, CHANNELS, CHANNELS, CHAN_HID, CHANNELS)
LN_EPS = 1e-6
LEARN_RATE = 0.003
BETA_ONE = 0.9
BETA_TWO = 0.999
ADAM_EPS = 1e-8
WEIGHT_DECAY = 0.03


def unpack_layer(flat):
    pieces = []
    piece_start = 0
    for piece_len in PIECE_SIZES:
        pieces.append(flat[piece_start:piece_start + piece_len])
        piece_start = piece_start + piece_len
    w_tok1 = pieces[0].reshape(TOKENS, TOKEN_HID)
    w_tok2 = pieces[1].reshape(TOKEN_HID, TOKENS)
    w_ch1 = pieces[2].reshape(CHANNELS, CHAN_HID)
    w_ch2 = pieces[3].reshape(CHAN_HID, CHANNELS)
    return [w_tok1, w_tok2, w_ch1, w_ch2] + pieces[4:12]


def layer_norm(x_in, ln_gain, ln_shift):
    x_f = x_in.astype(jnp.float32)
    mean_val = jnp.mean(x_f, axis=-1, keepdims=True)
    var_val = jnp.mean(jnp.square(x_f - mean_val), axis=-1, keepdims=True)
    normed = (x_f - mean_val) * lax.rsqrt(var_val + LN_EPS)
    return (normed * ln_gain.astype(jnp.float32) + ln_shift.astype(jnp.float32)).astype(jnp.bfloat16)


def mixer_layer(x_in, flat):
    w_tok1, w_tok2, w_ch1, w_ch2, ln1_g, ln1_b, b_tok1, b_tok2, ln2_g, ln2_b, b_ch1, b_ch2 = unpack_layer(flat)
    normed = layer_norm(x_in, ln1_g, ln1_b)
    hid_tok = jnp.einsum('bsc,sj->bcj', normed.astype(jnp.float32), w_tok1.astype(jnp.float32)) + b_tok1.astype(jnp.float32)
    act_tok = jax.nn.gelu(hid_tok).astype(jnp.bfloat16)
    tok_out = jnp.einsum('bcj,js->bsc', act_tok.astype(jnp.float32), w_tok2.astype(jnp.float32)) + b_tok2.astype(jnp.float32)[:, None]
    after_tok = (x_in.astype(jnp.float32) + tok_out).astype(jnp.bfloat16)
    normed2 = layer_norm(after_tok, ln2_g, ln2_b)
    hid_ch = jnp.einsum('bsc,cd->bsd', normed2.astype(jnp.float32), w_ch1.astype(jnp.float32)) + b_ch1.astype(jnp.float32)
    act_ch = jax.nn.gelu(hid_ch).astype(jnp.bfloat16)
    ch_out = jnp.einsum('bsd,dc->bsc', act_ch.astype(jnp.float32), w_ch2.astype(jnp.float32)) + b_ch2.astype(jnp.float32)
    return (after_tok.astype(jnp.float32) + ch_out).astype(jnp.bfloat16)


def block_loss(layer_p, head_w, small_p, x_block, label_block):
    layers_bf = layer_p.astype(jnp.bfloat16)
    hidden = x_block
    for layer_idx in range(2):
        hidden = mixer_layer(hidden, layers_bf[layer_idx])
    small_bf = small_p.astype(jnp.bfloat16)
    lnf_g = small_bf[:CHANNELS]
    lnf_b = small_bf[CHANNELS:2 * CHANNELS]
    head_b = small_bf[2 * CHANNELS:2 * CHANNELS + CLASSES]
    normed = layer_norm(hidden, lnf_g, lnf_b)
    pooled = jnp.mean(normed.astype(jnp.float32), axis=1).astype(jnp.bfloat16)
    logits = jnp.dot(pooled, head_w.astype(jnp.bfloat16), preferred_element_type=jnp.float32) + head_b.astype(jnp.float32)
    log_norm = jax.nn.logsumexp(logits, axis=-1)
    is_label = jnp.arange(CLASSES)[None, :] == label_block[:, None]
    picked = jnp.sum(jnp.where(is_label, logits, 0.0), axis=-1)
    return jnp.sum(log_norm - picked) / GLOBAL_BATCH


def loss_and_grads(act_in, labels, layer_p, head_w, small_p):
    x_blocks = act_in.reshape(FSDP_DEVS, BATCH_DEV, TOKENS, CHANNELS)
    label_blocks = labels.reshape(FSDP_DEVS, BATCH_DEV)
    grad_fn = jax.value_and_grad(block_loss, argnums=(0, 1, 2))

    def scan_body(running, block_pair):
        loss_part, grad_parts = grad_fn(layer_p, head_w, small_p, block_pair[0], block_pair[1])
        return (running[0] + loss_part, running[1] + grad_parts[0], running[2] + grad_parts[1], running[3] + grad_parts[2]), None

    start_val = (jnp.zeros((), jnp.float32), jnp.zeros_like(layer_p), jnp.zeros_like(head_w), jnp.zeros_like(small_p))
    totals, _ = lax.scan(scan_body, start_val, (x_blocks, label_blocks))
    return totals


def adam_update(master, gradient, moment, second, decay_rate):
    moment_new = BETA_ONE * moment + (1.0 - BETA_ONE) * gradient
    second_new = BETA_TWO * second + (1.0 - BETA_TWO) * gradient * gradient
    m_hat = moment_new / (1.0 - BETA_ONE ** ADAM_STEP)
    v_hat = second_new / (1.0 - BETA_TWO ** ADAM_STEP)
    master_new = master - LEARN_RATE * (m_hat / (jnp.sqrt(v_hat) + ADAM_EPS) + decay_rate * master)
    return master_new, moment_new, second_new


def draw_layer(key):
    subkeys = jax.random.split(key, 13)
    normal = jax.random.normal
    pieces = [
        normal(subkeys[0], (TOKENS * TOKEN_HID,), jnp.float32) * TOKENS ** -0.5,
        normal(subkeys[1], (TOKEN_HID * TOKENS,), jnp.float32) * TOKEN_HID ** -0.5,
        normal(subkeys[2], (CHANNELS * CHAN_HID,), jnp.float32) * CHANNELS ** -0.5,
        normal(subkeys[3], (CHAN_HID * CHANNELS,), jnp.float32) * CHAN_HID ** -0.5,
        1.0 + 0.2 * normal(subkeys[4], (CHANNELS,), jnp.float32),
        0.2 * normal(subkeys[5], (CHANNELS,), jnp.float32),
        0.3 * normal(subkeys[6], (TOKEN_HID,), jnp.float32),
        0.3 * normal(subkeys[7], (TOKENS,), jnp.float32),
        1.0 + 0.2 * normal(subkeys[8], (CHANNELS,), jnp.float32),
        0.2 * normal(subkeys[9], (CHANNELS,), jnp.float32),
        0.3 * normal(subkeys[10], (CHAN_HID,), jnp.float32),
        0.3 * normal(subkeys[11], (CHANNELS,), jnp.float32),
        0.02 * normal(subkeys[12], (LAYER_PAD - LAYER_LEN,), jnp.float32),
    ]
    return jnp.concatenate(pieces)


def setup_inputs(seed: int = 0) -> dict:
    keys = jax.random.split(jax.random.key(seed), 12)
    normal = jax.random.normal
    base = normal(keys[0], (GLOBAL_BATCH, 1, CHANNELS), jnp.float32)
    noise = normal(keys[1], (GLOBAL_BATCH, TOKENS, CHANNELS), jnp.float32)
    act_in = (base + noise).astype(jnp.bfloat16)
    labels = jax.random.randint(keys[2], (GLOBAL_BATCH,), 0, CLASSES, jnp.int32)
    layer_p = jnp.stack([draw_layer(keys[3]), draw_layer(keys[4])])
    head_w = normal(keys[5], (CHANNELS, CLASSES), jnp.float32) * CHANNELS ** -0.5
    small_p = jnp.concatenate([
        2.0 + 0.3 * normal(keys[6], (CHANNELS,), jnp.float32),
        0.3 * normal(keys[7], (CHANNELS,), jnp.float32),
        normal(keys[8], (CLASSES,), jnp.float32),
        0.02 * normal(keys[9], (SMALL_PAD - SMALL_LEN,), jnp.float32),
    ])
    _, g_layer, g_head, g_small = loss_and_grads(act_in, labels, layer_p, head_w, small_p)
    layer_rms = jnp.sqrt(jnp.mean(jnp.square(g_layer), axis=1, keepdims=True))
    head_rms = jnp.sqrt(jnp.mean(jnp.square(g_head)))
    small_rms = jnp.sqrt(jnp.mean(jnp.square(g_small)))
    mkeys = jax.random.split(keys[10], 6)
    uniform = jax.random.uniform
    layer_m = 0.3 * layer_rms * normal(mkeys[0], layer_p.shape, jnp.float32)
    head_m = 0.3 * head_rms * normal(mkeys[1], head_w.shape, jnp.float32)
    small_m = 0.3 * small_rms * normal(mkeys[2], small_p.shape, jnp.float32)
    layer_v = 0.01 * jnp.square(layer_rms) * uniform(mkeys[3], layer_p.shape, jnp.float32, 0.5, 2.0)
    head_v = 0.01 * jnp.square(head_rms) * uniform(mkeys[4], head_w.shape, jnp.float32, 0.5, 2.0)
    small_v = 0.01 * jnp.square(small_rms) * uniform(mkeys[5], small_p.shape, jnp.float32, 0.5, 2.0)
    return {'act_in': act_in, 'labels': labels, 'layer_p': layer_p, 'head_w': head_w, 'small_p': small_p, 'layer_m': layer_m, 'head_m': head_m, 'small_m': small_m, 'layer_v': layer_v, 'head_v': head_v, 'small_v': small_v}


def reference(act_in, labels, layer_p, head_w, small_p, layer_m, head_m, small_m, layer_v, head_v, small_v):
    loss_value, g_layer, g_head, g_small = loss_and_grads(act_in, labels, layer_p, head_w, small_p)
    sq_total = jnp.sum(jnp.square(g_layer)) + jnp.sum(jnp.square(g_head)) + jnp.sum(jnp.square(g_small))
    clip_scale = 1.0 / jnp.maximum(1.0, jnp.sqrt(sq_total))
    layer_decay = jnp.where(jnp.arange(LAYER_PAD) < MAT_LEN, WEIGHT_DECAY, 0.0)[None, :]
    new_lp, new_lm, new_lv = adam_update(layer_p, g_layer * clip_scale, layer_m, layer_v, layer_decay)
    new_hw, new_hm, new_hv = adam_update(head_w, g_head * clip_scale, head_m, head_v, WEIGHT_DECAY)
    new_sp, new_sm, new_sv = adam_update(small_p, g_small * clip_scale, small_m, small_v, 0.0)
    return (loss_value, new_lp, new_hw, new_sp, new_lm, new_hm, new_sm, new_lv, new_hv, new_sv)
```

```python
import functools
import math
import jax
import jax.numpy as jnp
from jax import lax
from jax.experimental import pallas as pl
from jax.experimental.pallas import tpu as pltpu
from jax.sharding import PartitionSpec as P

MESH_ID = pl.DeviceIdType.MESH
F32 = jnp.float32
BF16 = jnp.bfloat16
VMEM_CAP = 64 * 1024 * 1024 - 128 * 1024

SHARD_ROWS = 1039
SLOT_ROWS = 1040
ROW_C1 = 196
ROW_C2 = 8388
ROW_VEC = 16580
FLAT_ROWS = 16624
SLAB_ROWS = 240
HEAD_OFF = 2 * SLOT_ROWS
SMALL_OFF = HEAD_OFF + 256
AG_ROWS = SMALL_OFF + 16
RS_ROWS = SMALL_OFF + 8
ORDERS = ((2, 1, 0), (1, 0, 2), (0, 2, 1))
AXIS_STEP = (8, 4, 2)


def place():
    me = lax.axis_index('fsdp')
    coords = [me // 8, (me // 4) % 2, (me // 2) % 2]
    core = me % 2
    neighbours = [me + AXIS_STEP[a] - 2 * AXIS_STEP[a] * coords[a] for a in range(3)]
    partner = me + 1 - 2 * core
    return me, coords, core, neighbours, partner


def enter_barrier(neighbours, partner):
    barrier = pltpu.get_barrier_semaphore()
    for other in list(neighbours) + [partner]:
        pl.semaphore_signal(barrier, inc=1, device_id=(other,), device_id_type=MESH_ID)
    pl.semaphore_wait(barrier, 4)


def slot_view(buf, coords, core, free_axes, row0, rows):
    index = [pl.ds(0, 2) if a in free_axes else coords[a] for a in range(3)]
    return buf.at[index[0], index[1], index[2], core, pl.ds(row0, rows), :]


class Gather:
    def __init__(self, buf, where, row_groups, send_sem, recv_sem, sem0):
        self.buf, self.where, self.groups = buf, where, row_groups
        self.send_sem, self.recv_sem, self.sem0 = send_sem, recv_sem, sem0
        self.pending = []

    def copy(self, view, sem, device):
        return pltpu.make_async_remote_copy(src_ref=view, dst_ref=view, send_sem=self.send_sem.at[self.sem0 + sem], recv_sem=self.recv_sem.at[self.sem0 + sem], device_id=(device,), device_id_type=MESH_ID)

    def link(self, group, phase):
        me, coords, core, neighbours, partner = self.where
        order = ORDERS[group]
        row0, rows = self.groups[group]
        view = slot_view(self.buf, coords, core, order[:phase], row0, rows)
        return self.copy(view, group * 3 + phase, neighbours[order[phase]])

    def chip(self, group, phase):
        me, coords, core, neighbours, partner = self.where
        order = ORDERS[group]
        row0, rows = self.groups[group]
        if phase < 0:
            view = slot_view(self.buf, coords, core, (), row0, rows)
        else:
            far = list(coords)
            far[order[phase]] = 1 - coords[order[phase]]
            view = slot_view(self.buf, far, core, order[:phase], row0, rows)
        return self.copy(view, 9 + group * 4 + phase + 1, partner)

    def start(self):
        for group in range(3):
            self.link(group, 0).start()
        for group in range(3):
            self.chip(group, -1).start()

    def step(self, phase):
        for group in range(3):
            self.link(group, phase).wait_recv()
            if phase < 2:
                self.link(group, phase + 1).start()
            self.chip(group, phase).start()

    def finish(self):
        for group in range(3):
            for phase in range(-1, 3):
                self.chip(group, phase).wait()
            for phase in range(3):
                self.link(group, phase).wait_send()


def unflatten_layer(gath, layer, flat, w1_ref, w2_ref, slab_ref):
    base = layer * SLOT_ROWS

    def spread(dev, carry):
        z, y, x, core = dev // 8, (dev // 4) % 2, (dev // 2) % 2, dev % 2

        def chunk(k, inner):
            block = gath[z, y, x, core, pl.ds(base + 16 * k, 16), :]
            flat[pl.ds(dev * SHARD_ROWS + 16 * k, 16), :] = block.astype(F32)
            return inner
        return lax.fori_loop(0, SLOT_ROWS // 16, chunk, carry, unroll=5)
    lax.fori_loop(0, 16, spread, 0)

    def first(rb, carry):
        for j in range(16):
            block = flat[pl.ds(ROW_C1 + 256 * rb + j, 16, stride=16), :]
            w1_ref[layer, pl.ds(pl.multiple_of(16 * rb, 16), 16), 128 * j:128 * j + 128] = block.astype(BF16)
        return carry
    lax.fori_loop(0, 32, first, 0)

    def second(rb, carry):
        for j in range(4):
            block = flat[pl.ds(ROW_C2 + 64 * rb + j, 16, stride=4), :]
            w2_ref[layer, pl.ds(pl.multiple_of(16 * rb, 16), 16), 128 * j:128 * j + 128] = block.astype(BF16)
        return carry
    lax.fori_loop(0, 128, second, 0)
    slab_ref[layer, 0:196, :] = flat[0:196, :]
    slab_ref[layer, 196:240, :] = flat[ROW_VEC:FLAT_ROWS, :]


def gather_kernel(pack_ref, w1_ref, w2_ref, slab_ref, head_ref, small_ref, gath, flat, send_sem, recv_sem, load_sem):
    where = place()
    me, coords, core, neighbours, partner = where
    load = pltpu.make_async_copy(pack_ref, gath.at[coords[0], coords[1], coords[2], core], load_sem)
    load.start()
    enter_barrier(neighbours, partner)
    load.wait()
    third = AG_ROWS // 3
    work = Gather(gath, where, [(third * g, third) for g in range(3)], send_sem, recv_sem, 0)
    work.start()
    for phase in range(3):
        work.step(phase)
    work.finish()
    for layer in range(2):
        unflatten_layer(gath, layer, flat, w1_ref, w2_ref, slab_ref)

    def spread_head(dev, carry):
        z, y, x, own = dev // 8, (dev // 4) % 2, (dev // 2) % 2, dev % 2
        for j in range(8):
            head_ref[pl.ds(pl.multiple_of(32 * dev, 32), 32), 128 * j:128 * j + 128] = gath[z, y, x, own, pl.ds(HEAD_OFF + 32 * j, 32), :]
        small_ref[pl.ds(dev, 1), :] = gath[z, y, x, own, pl.ds(SMALL_OFF, 16), :].astype(F32)[0:1, :]
        return carry
    lax.fori_loop(0, 16, spread_head, 0)


def gather_weights(pack):
    vmem = pl.BlockSpec(memory_space=pltpu.VMEM)
    return pl.pallas_call(
        gather_kernel,
        out_shape=(jax.ShapeDtypeStruct((2, 512, 2048), BF16), jax.ShapeDtypeStruct((2, 2048, 512), BF16), jax.ShapeDtypeStruct((2, SLAB_ROWS, 128), F32), jax.ShapeDtypeStruct((512, 1024), BF16), jax.ShapeDtypeStruct((16, 128), F32)),
        in_specs=[vmem],
        out_specs=(vmem,) * 5,
        scratch_shapes=[
            pltpu.VMEM((2, 2, 2, 2, AG_ROWS, 128), BF16),
            pltpu.VMEM((16640, 128), F32),
            pltpu.SemaphoreType.DMA((21,)),
            pltpu.SemaphoreType.DMA((21,)),
            pltpu.SemaphoreType.DMA,
        ],
        compiler_params=pltpu.CompilerParams(collective_id=0, has_side_effects=True, vmem_limit_bytes=VMEM_CAP),
        name='gather_weights',
    )(pack)


class Reduce:
    def __init__(self, buf, temps, where, row_groups, send_sem, recv_sem, sem0):
        self.buf, self.temps, self.where, self.groups = buf, temps, where, row_groups
        self.send_sem, self.recv_sem, self.sem0 = send_sem, recv_sem, sem0

    def views(self, group, phase):
        me, coords, core, neighbours, partner = self.where
        row0, rows = self.groups[group]
        order = ORDERS[group]
        if phase == 0:
            free = (0, 1, 2)
            leave = slot_view(self.buf, coords, 1 - core, free, row0, rows)
            device = partner
            stay = coords
        else:
            axis = order[phase - 1]
            free = tuple(a for a in range(3) if a in order[phase:])
            far = list(coords)
            far[axis] = 1 - coords[axis]
            leave = slot_view(self.buf, far, core, free, row0, rows)
            device = neighbours[axis]
            stay = coords
        land = self.temps[phase].at[(slice(None),) * len(free) + (pl.ds(row0, rows), slice(None))]
        return leave, land, device, free, stay

    def copy(self, group, phase):
        leave, land, device, free, stay = self.views(group, phase)
        sem = self.sem0 + group * 4 + phase
        return pltpu.make_async_remote_copy(src_ref=leave, dst_ref=land, send_sem=self.send_sem.at[sem], recv_sem=self.recv_sem.at[sem], device_id=(device,), device_id_type=MESH_ID)

    def add(self, group, phase):
        me, coords, core, neighbours, partner = self.where
        leave, land, device, free, stay = self.views(group, phase)
        row0, rows = self.groups[group]
        temp = self.temps[phase]
        count = 2 ** len(free)
        per = max(1, 8 // count)
        while rows % (8 * per):
            per //= 2

        def chunk(k, carry):
            for part in range(per):
                start = pl.multiple_of(row0 + 8 * (per * k + part), 8)
                for n in range(count):
                    index = list(coords)
                    bits = []
                    for pos, a in enumerate(free):
                        bit = (n // 2 ** (len(free) - 1 - pos)) % 2
                        index[a] = bit
                        bits.append(bit)
                    target = (index[0], index[1], index[2], core, pl.ds(start, 8), slice(None))
                    self.buf[target] = self.buf[target] + temp[tuple(bits) + (pl.ds(start, 8), slice(None))]
            return carry
        lax.fori_loop(0, rows // (8 * per), chunk, 0)

    def start(self):
        for group in range(3):
            self.copy(group, 0).start()

    def step(self, phase):
        for group in range(3):
            self.copy(group, phase).wait_recv()
            self.add(group, phase)
            if phase < 3:
                self.copy(group, phase + 1).start()

    def finish(self):
        for group in range(3):
            for phase in range(4):
                self.copy(group, phase).wait_send()


def flatten_layer(layer, flat, w1_ref, w2_ref, slab_ref, grad):
    base = layer * SLOT_ROWS

    def first(rb, carry):
        for j in range(16):
            flat[pl.ds(ROW_C1 + 128 * rb + j, 8, stride=16), :] = w1_ref[pl.ds(pl.multiple_of(8 * rb, 8), 8), 128 * j:128 * j + 128]
        return carry
    lax.fori_loop(0, 64, first, 0)

    def second(rb, carry):
        for j in range(4):
            flat[pl.ds(ROW_C2 + 32 * rb + j, 8, stride=4), :] = w2_ref[pl.ds(pl.multiple_of(8 * rb, 8), 8), 128 * j:128 * j + 128]
        return carry
    lax.fori_loop(0, 256, second, 0, unroll=2)
    flat[0:196, :] = slab_ref[layer, 0:196, :]
    flat[ROW_VEC:FLAT_ROWS, :] = slab_ref[layer, 196:240, :]

    def spread(dev, carry):
        z, y, x, core = dev // 8, (dev // 4) % 2, (dev // 2) % 2, dev % 2

        def chunk(k, inner):
            grad[z, y, x, core, pl.ds(pl.multiple_of(base + 8 * k, 8), 8), :] = flat[pl.ds(dev * SHARD_ROWS + 8 * k, 8), :]
            return inner
        return lax.fori_loop(0, SLOT_ROWS // 8, chunk, carry, unroll=10)
    lax.fori_loop(0, 16, spread, 0)


def square_sum(ref, coords, core, row0, rows):
    def chunk(k, total):
        block = ref[coords[0], coords[1], coords[2], core, pl.ds(pl.multiple_of(row0 + 8 * k, 8), 8), :]
        return total + block * block
    return lax.fori_loop(0, rows // 8, chunk, jnp.zeros((8, 128), F32), unroll=2)


def reduce_kernel(gw1_hbm, gw2_hbm, slab_ref, gh_ref, gs_ref, loss_ref, gl_ref, ghead_ref, gsmall_ref, stat_ref, stage1, stage2, flat, grad, t0, t1, t2, t3, msg, box, send_sem, recv_sem, load_sem, tiny_send, tiny_recv):
    where = place()
    me, coords, core, neighbours, partner = where
    enter_barrier(neighbours, partner)
    flat[FLAT_ROWS:16640, :] = jnp.zeros((16, 128), F32)

    def load(layer):
        return pltpu.make_async_copy(gw1_hbm.at[layer], stage1, load_sem.at[0]), pltpu.make_async_copy(gw2_hbm.at[layer], stage2, load_sem.at[1])
    for layer in (1, 0):
        for item in load(layer):
            item.start()
        for item in load(layer):
            item.wait()
        flatten_layer(layer, flat, stage1, stage2, slab_ref, grad)

    def spread_head(dev, carry):
        z, y, x, own = dev // 8, (dev // 4) % 2, (dev // 2) % 2, dev % 2
        for j in range(8):
            grad[z, y, x, own, HEAD_OFF + 32 * j:HEAD_OFF + 32 * j + 32, :] = gh_ref[pl.ds(pl.multiple_of(32 * dev, 32), 32), 128 * j:128 * j + 128]
        grad[z, y, x, own, SMALL_OFF:AG_ROWS, :] = jnp.zeros((16, 128), F32)
        grad[z, y, x, own, SMALL_OFF:SMALL_OFF + 1, :] = gs_ref[pl.ds(dev, 1), :]
        grad[z, y, x, own, SMALL_OFF + 8:SMALL_OFF + 16, :] = loss_ref[...]
        return carry
    lax.fori_loop(0, 16, spread_head, 0)
    third = AG_ROWS // 3
    work = Reduce(grad, (t0, t1, t2, t3), where, [(third * g, third) for g in range(3)], send_sem, recv_sem, 0)
    work.start()
    for phase in range(4):
        work.step(phase)
    work.finish()
    own = (coords[0], coords[1], coords[2], core)
    for layer in range(2):
        last = layer * SLOT_ROWS + SHARD_ROWS
        grad[own + (pl.ds(last, 1), slice(None))] = jnp.zeros((1, 128), F32)
    total = square_sum(grad, coords, core, 0, SMALL_OFF + 8)
    msg[0] = jnp.broadcast_to(jnp.sum(total), (8, 128))
    for n, device in enumerate([partner, neighbours[2], neighbours[1], neighbours[0]]):
        copy = pltpu.make_async_remote_copy(src_ref=msg.at[n], dst_ref=box.at[n], send_sem=tiny_send.at[n], recv_sem=tiny_recv.at[n], device_id=(device,), device_id_type=MESH_ID)
        copy.start()
        copy.wait()
        msg[n + 1] = msg[n] + box[n]
    stat_ref[0] = msg[4]
    stat_ref[1] = grad[own + (pl.ds(SMALL_OFF + 8, 8), slice(None))]
    for layer in range(2):
        gl_ref[layer] = grad[own + (pl.ds(layer * SLOT_ROWS, SLOT_ROWS), slice(None))]
    ghead_ref[...] = grad[own + (pl.ds(HEAD_OFF, 256), slice(None))]
    gsmall_ref[...] = grad[own + (pl.ds(SMALL_OFF, 8), slice(None))]


def reduce_grads(gw1, gw2, slab, gh, gs, loss):
    vmem = pl.BlockSpec(memory_space=pltpu.VMEM)
    hbm = pl.BlockSpec(memory_space=pl.ANY)
    return pl.pallas_call(
        reduce_kernel,
        out_shape=(jax.ShapeDtypeStruct((2, SLOT_ROWS, 128), F32), jax.ShapeDtypeStruct((256, 128), F32), jax.ShapeDtypeStruct((8, 128), F32), jax.ShapeDtypeStruct((2, 8, 128), F32)),
        in_specs=[hbm, hbm, vmem, vmem, vmem, vmem],
        out_specs=(vmem,) * 4,
        scratch_shapes=[
            pltpu.VMEM((512, 2048), F32),
            pltpu.VMEM((2048, 512), F32),
            pltpu.VMEM((16640, 128), F32),
            pltpu.VMEM((2, 2, 2, 2, AG_ROWS, 128), F32),
            pltpu.VMEM((2, 2, 2, AG_ROWS, 128), F32),
            pltpu.VMEM((2, 2, AG_ROWS, 128), F32),
            pltpu.VMEM((2, AG_ROWS, 128), F32),
            pltpu.VMEM((AG_ROWS, 128), F32),
            pltpu.VMEM((5, 8, 128), F32),
            pltpu.VMEM((4, 8, 128), F32),
            pltpu.SemaphoreType.DMA((12,)),
            pltpu.SemaphoreType.DMA((12,)),
            pltpu.SemaphoreType.DMA((2,)),
            pltpu.SemaphoreType.DMA((4,)),
            pltpu.SemaphoreType.DMA((4,)),
        ],
        compiler_params=pltpu.CompilerParams(collective_id=1, has_side_effects=True, vmem_limit_bytes=VMEM_CAP),
        name='reduce_grads',
    )(gw1, gw2, slab, gh, gs, loss)


LN_EPS = 1e-6
LEARN_RATE = 0.003
BETA_ONE = 0.9
BETA_TWO = 0.999
ADAM_EPS = 1e-8
WEIGHT_DECAY = 0.03
ADAM_STEP = 10


def piece_shapes(num_tokens, num_chans):
    tok_hid = num_chans // 2
    ch_hid = 4 * num_chans
    return [(num_tokens, tok_hid), (tok_hid, num_tokens), (num_chans, ch_hid), (ch_hid, num_chans), (num_chans,), (num_chans,), (tok_hid,), (num_tokens,), (num_chans,), (num_chans,), (ch_hid,), (num_chans,)]


def layer_length(num_tokens, num_chans):
    return sum(math.prod(shape_one) for shape_one in piece_shapes(num_tokens, num_chans))


def unpack_layer(parts, num_tokens, num_chans):
    w_ch1, w_ch2, slab = parts
    shapes = piece_shapes(num_tokens, num_chans)
    w_tok1 = slab[0:98].reshape(shapes[0]).astype(BF16)
    w_tok2 = slab[98:196].reshape(shapes[1]).astype(BF16)
    tail = slab[196:].reshape(-1)
    pieces = [w_tok1, w_tok2, w_ch1, w_ch2]
    piece_start = 0
    for shape_one in shapes[4:]:
        piece_len = math.prod(shape_one)
        pieces.append(tail[piece_start:piece_start + piece_len])
        piece_start = piece_start + piece_len
    return pieces


def layer_norm(x_in, ln_gain, ln_shift):
    x_f = x_in.astype(jnp.float32)
    mean_val = jnp.mean(x_f, axis=-1, keepdims=True)
    var_val = jnp.mean(jnp.square(x_f - mean_val), axis=-1, keepdims=True)
    normed = (x_f - mean_val) * lax.rsqrt(var_val + LN_EPS)
    return (normed * ln_gain.astype(jnp.float32) + ln_shift.astype(jnp.float32)).astype(jnp.bfloat16)


def gelu_bf16(hidden):
    return jax.nn.gelu(hidden).astype(jnp.bfloat16)


def gelu_grad(hidden, d_act):
    _, pullback = jax.vjp(gelu_bf16, hidden)
    return pullback(d_act.astype(jnp.bfloat16))[0]


def norm_grad(x_in, ln_gain, ln_shift, d_normed):
    _, pullback = jax.vjp(layer_norm, x_in, ln_gain.astype(jnp.float32), ln_shift.astype(jnp.float32))
    d_x, d_gain, d_shift = pullback(d_normed.astype(jnp.bfloat16))
    return d_x.astype(jnp.float32), d_gain, d_shift


def layer_forward(x_in, flat, num_tokens, num_chans):
    w_tok1, w_tok2, w_ch1, w_ch2, ln1_g, ln1_b, b_tok1, b_tok2, ln2_g, ln2_b, b_ch1, b_ch2 = unpack_layer(flat, num_tokens, num_chans)
    normed = layer_norm(x_in, ln1_g, ln1_b)
    hid_tok = jnp.einsum('bsc,sj->bcj', normed, w_tok1, preferred_element_type=jnp.float32) + b_tok1.astype(jnp.float32)
    act_tok = gelu_bf16(hid_tok)
    tok_out = jnp.einsum('bcj,js->bsc', act_tok, w_tok2, preferred_element_type=jnp.float32) + b_tok2.astype(jnp.float32)[:, None]
    after_tok = (x_in.astype(jnp.float32) + tok_out).astype(jnp.bfloat16)
    normed2 = layer_norm(after_tok, ln2_g, ln2_b)
    hid_ch = jnp.einsum('bsc,cd->bsd', normed2, w_ch1, preferred_element_type=jnp.float32) + b_ch1.astype(jnp.float32)
    act_ch = gelu_bf16(hid_ch)
    ch_out = jnp.einsum('bsd,dc->bsc', act_ch, w_ch2, preferred_element_type=jnp.float32) + b_ch2.astype(jnp.float32)
    layer_out = (after_tok.astype(jnp.float32) + ch_out).astype(jnp.bfloat16)
    return layer_out, (x_in, normed, hid_tok, act_tok, after_tok, normed2, hid_ch, act_ch)


def layer_backward(d_out, flat, cache, num_tokens, num_chans):
    w_tok1, w_tok2, w_ch1, w_ch2, ln1_g, ln1_b, b_tok1, b_tok2, ln2_g, ln2_b, b_ch1, b_ch2 = unpack_layer(flat, num_tokens, num_chans)
    x_in, normed, hid_tok, act_tok, after_tok, normed2, hid_ch, act_ch = cache
    d_out_bf = d_out.astype(jnp.bfloat16)
    g_b_ch2 = jnp.sum(d_out, axis=(0, 1))
    g_w_ch2 = jnp.einsum('bsd,bsc->dc', act_ch, d_out_bf, preferred_element_type=jnp.float32)
    d_act_ch = jnp.einsum('bsc,dc->bsd', d_out_bf, w_ch2, preferred_element_type=jnp.float32)
    d_hid_ch = gelu_grad(hid_ch, d_act_ch)
    d_hid_ch_bf = d_hid_ch.astype(jnp.bfloat16)
    g_b_ch1 = jnp.sum(d_hid_ch, axis=(0, 1))
    g_w_ch1 = jnp.einsum('bsc,bsd->cd', normed2, d_hid_ch_bf, preferred_element_type=jnp.float32)
    d_normed2 = jnp.einsum('bsd,cd->bsc', d_hid_ch_bf, w_ch1, preferred_element_type=jnp.float32)
    d_after_ln, g_ln2_g, g_ln2_b = norm_grad(after_tok, ln2_g, ln2_b, d_normed2)
    d_after = d_after_ln + d_out
    d_after_bf = d_after.astype(jnp.bfloat16)
    g_b_tok2 = jnp.sum(d_after, axis=(0, 2))
    g_w_tok2 = jnp.einsum('bcj,bsc->js', act_tok, d_after_bf, preferred_element_type=jnp.float32)
    d_act_tok = jnp.einsum('bsc,js->bcj', d_after_bf, w_tok2, preferred_element_type=jnp.float32)
    d_hid_tok = gelu_grad(hid_tok, d_act_tok)
    d_hid_tok_bf = d_hid_tok.astype(jnp.bfloat16)
    g_b_tok1 = jnp.sum(d_hid_tok, axis=(0, 1))
    g_w_tok1 = jnp.einsum('bsc,bcj->sj', normed, d_hid_tok_bf, preferred_element_type=jnp.float32)
    d_normed = jnp.einsum('bcj,sj->bsc', d_hid_tok_bf, w_tok1, preferred_element_type=jnp.float32)
    d_in_ln, g_ln1_g, g_ln1_b = norm_grad(x_in, ln1_g, ln1_b, d_normed)
    d_in = d_in_ln + d_after
    tail = jnp.concatenate([g_ln1_g, g_ln1_b, g_b_tok1, g_b_tok2, g_ln2_g, g_ln2_b, g_b_ch1, g_b_ch2, jnp.zeros((719,), jnp.float32)])
    slab = jnp.concatenate([g_w_tok1.reshape(98, 128), g_w_tok2.reshape(98, 128), tail.reshape(44, 128)])
    return d_in, (g_w_ch1, g_w_ch2, slab)


def head_step(hidden, labels, small_full, head_full, global_b):
    num_tokens = hidden.shape[1]
    num_chans = hidden.shape[2]
    num_classes = head_full.shape[1]
    lnf_g = small_full[:num_chans]
    lnf_b = small_full[num_chans:2 * num_chans]
    head_b = small_full[2 * num_chans:2 * num_chans + num_classes]
    normed = layer_norm(hidden, lnf_g, lnf_b)
    pooled = (jnp.sum(normed, axis=1, dtype=jnp.float32) / num_tokens).astype(jnp.bfloat16)
    logits = jnp.dot(pooled, head_full, preferred_element_type=jnp.float32) + head_b.astype(jnp.float32)
    log_norm = jax.nn.logsumexp(logits, axis=-1)
    is_label = jnp.arange(num_classes)[None, :] == labels[:, None]
    picked = jnp.sum(jnp.where(is_label, logits, 0.0), axis=-1)
    loss_sum = jnp.sum(log_norm - picked)
    d_logits = (jnp.exp(logits - log_norm[:, None]) - is_label.astype(jnp.float32)) / global_b
    d_logits_bf = d_logits.astype(jnp.bfloat16)
    g_head_b = jnp.sum(d_logits, axis=0)
    g_head_w = jnp.einsum('bc,bk->ck', pooled, d_logits_bf, preferred_element_type=jnp.float32)
    d_pooled = jnp.einsum('bk,ck->bc', d_logits_bf, head_full, preferred_element_type=jnp.float32)
    d_normed = jnp.broadcast_to((d_pooled / num_tokens)[:, None, :], normed.shape)
    d_hidden, g_lnf_g, g_lnf_b = norm_grad(hidden, lnf_g, lnf_b, d_normed)
    g_small = jnp.concatenate([g_lnf_g, g_lnf_b, g_head_b])
    return loss_sum, d_hidden, g_head_w, g_small


def adam_update(master, gradient, moment, second, decay_rate):
    moment_new = BETA_ONE * moment + (1.0 - BETA_ONE) * gradient
    second_new = BETA_TWO * second + (1.0 - BETA_TWO) * gradient * gradient
    m_hat = moment_new / (1.0 - BETA_ONE ** ADAM_STEP)
    v_hat = second_new / (1.0 - BETA_TWO ** ADAM_STEP)
    master_new = master - LEARN_RATE * (m_hat / (jnp.sqrt(v_hat) + ADAM_EPS) + decay_rate * master)
    return master_new, moment_new, second_new


def solution(mesh):
    group = mesh.shape['fsdp']
    row_spec = P('fsdp')
    layer_spec = P(None, 'fsdp')
    in_specs = (row_spec, row_spec, layer_spec, row_spec, row_spec, layer_spec, row_spec, row_spec, layer_spec, row_spec, row_spec)
    out_specs = (P(),) + in_specs[2:]

    def device_step(act_in, labels, layer_p, head_w, small_p, layer_m, head_m, small_m, layer_v, head_v, small_v):
        local_b, num_tokens, num_chans = act_in.shape
        global_b = local_b * group
        num_layers = layer_p.shape[0]
        mat_len = 2 * num_tokens * (num_chans // 2) + 8 * num_chans * num_chans
        caches = []
        hidden = act_in
        layer_bf = jnp.pad(layer_p.astype(BF16).reshape(2, SHARD_ROWS, 128), ((0, 0), (0, 1), (0, 0)))
        head_bf = jnp.pad(head_w.astype(BF16), ((0, 0), (0, 24))).reshape(32, 8, 128).transpose(1, 0, 2).reshape(256, 128)
        small_bf = jnp.pad(small_p.astype(BF16).reshape(1, 128), ((0, 15), (0, 0)))
        w1_all, w2_all, slab_all, head_all, small_all = gather_weights(jnp.concatenate([layer_bf.reshape(2 * SLOT_ROWS, 128), head_bf, small_bf]))
        for layer_idx in range(num_layers):
            hidden, cache = layer_forward(hidden, (w1_all[layer_idx], w2_all[layer_idx], slab_all[layer_idx]), num_tokens, num_chans)
            caches.append(cache)
        loss_sum, d_hidden, g_head_w, g_small = head_step(hidden, labels, small_all.reshape(-1), head_all[:, :head_w.shape[1]], global_b)
        grads = [None] * num_layers
        for layer_idx in reversed(range(num_layers)):
            d_hidden, grads[layer_idx] = layer_backward(d_hidden, (w1_all[layer_idx], w2_all[layer_idx], slab_all[layer_idx]), caches[layer_idx], num_tokens, num_chans)
        gl, ghead, gsmall, stat = reduce_grads(
            jnp.stack([grads[0][0], grads[1][0]]), jnp.stack([grads[0][1], grads[1][1]]), jnp.stack([grads[0][2], grads[1][2]]),
            jnp.pad(g_head_w, ((0, 0), (0, 24))), jnp.pad(g_small, (0, 24)).reshape(16, 128), jnp.broadcast_to(loss_sum, (8, 128)))
        layer_g = gl[:, :SHARD_ROWS].reshape(2, SHARD_ROWS * 128)
        head_g = ghead.reshape(8, 32, 128).transpose(1, 0, 2).reshape(32, 1024)[:, :head_w.shape[1]]
        small_g = gsmall[0]
        loss_value = stat[1, 0, 0] / global_b
        clip_scale = 1.0 / jnp.maximum(1.0, jnp.sqrt(stat[0, 0, 0]))
        shard_len = layer_p.shape[1]
        flat_pos = lax.axis_index('fsdp') * shard_len + jnp.arange(shard_len)
        layer_decay = jnp.where(flat_pos < mat_len, WEIGHT_DECAY, 0.0)[None, :]
        new_lp, new_lm, new_lv = adam_update(layer_p, layer_g * clip_scale, layer_m, layer_v, layer_decay)
        new_hw, new_hm, new_hv = adam_update(head_w, head_g * clip_scale, head_m, head_v, WEIGHT_DECAY)
        new_sp, new_sm, new_sv = adam_update(small_p, small_g * clip_scale, small_m, small_v, 0.0)
        return (loss_value, new_lp, new_hw, new_sp, new_lm, new_hm, new_sm, new_lv, new_hv, new_sv)

    return jax.shard_map(device_step, mesh=mesh, in_specs=in_specs, out_specs=out_specs, check_vma=False)
```

```python
import functools
import math
import jax
import jax.numpy as jnp
from jax import lax
from jax.experimental import pallas as pl
from jax.experimental.pallas import tpu as pltpu
from jax.sharding import PartitionSpec as P

ZERO = 0
ONE = 1
TWO = 2
THREE = 3
FOUR = 4
FIVE = 5
SIX = 6
SEVEN = 7
EIGHT = 8
NINE = 9
SIXTEEN = 16
LANES = 128
IMAGES = 32
LAST_IMAGE = 31
CH = 512
CLASS_PAD = 1024
HID = 2048
TH = 256
F_ZERO = 0.0
F_ONE = 1.0
TWENTY_FOUR = 24
TOKEN_PAD = 56
QVALID = 196
SIXTY_FOUR = 64
TEN = 10
MESH_ID = pl.DeviceIdType.MESH
F32 = jnp.float32
BF16 = jnp.bfloat16
VMEM_CAP = 64 * 1024 * 1024 - 128 * 1024

SHARD_ROWS = 1039
SLOT_ROWS = 1040
ROW_C1 = 196
ROW_C2 = 8388
ROW_VEC = 16580
FLAT_ROWS = 16624
SLAB_ROWS = 240
HEAD_OFF = 2 * SLOT_ROWS
SMALL_OFF = HEAD_OFF + 256
AG_ROWS = SMALL_OFF + 16
RS_ROWS = SMALL_OFF + 8
ORDERS = ((2, 1, 0), (1, 0, 2), (0, 2, 1))
AXIS_STEP = (8, 4, 2)


def place():
    me = lax.axis_index('fsdp')
    coords = [me // EIGHT, (me // FOUR) % TWO, (me // TWO) % TWO]
    core = me % TWO
    neighbours = [me + AXIS_STEP[a] - TWO * AXIS_STEP[a] * coords[a] for a in range(THREE)]
    partner = me + ONE - TWO * core
    return me, coords, core, neighbours, partner


def enter_barrier(neighbours, partner):
    barrier = pltpu.get_barrier_semaphore()
    for other in list(neighbours) + [partner]:
        pl.semaphore_signal(barrier, inc=ONE, device_id=(other,), device_id_type=MESH_ID)
    pl.semaphore_wait(barrier, FOUR)


def slot_view(buf, coords, core, free_axes, row0, rows):
    index = [pl.ds(ZERO, TWO) if a in free_axes else coords[a] for a in range(THREE)]
    return buf.at[index[ZERO], index[ONE], index[TWO], core, pl.ds(row0, rows), :]


class Gather:
    def __init__(self, buf, where, row_groups, send_sem, recv_sem, sem0):
        self.buf, self.where, self.groups = buf, where, row_groups
        self.send_sem, self.recv_sem, self.sem0 = send_sem, recv_sem, sem0
        self.pending = []

    def copy(self, view, sem, device):
        return pltpu.make_async_remote_copy(src_ref=view, dst_ref=view, send_sem=self.send_sem.at[self.sem0 + sem], recv_sem=self.recv_sem.at[self.sem0 + sem], device_id=(device,), device_id_type=MESH_ID)

    def link(self, group, phase):
        me, coords, core, neighbours, partner = self.where
        order = ORDERS[group]
        row0, rows = self.groups[group]
        view = slot_view(self.buf, coords, core, order[:phase], row0, rows)
        return self.copy(view, group * THREE + phase, neighbours[order[phase]])

    def chip(self, group, phase):
        me, coords, core, neighbours, partner = self.where
        order = ORDERS[group]
        row0, rows = self.groups[group]
        if phase < ZERO:
            view = slot_view(self.buf, coords, core, (), row0, rows)
        else:
            far = list(coords)
            far[order[phase]] = ONE - coords[order[phase]]
            view = slot_view(self.buf, far, core, order[:phase], row0, rows)
        return self.copy(view, NINE + group * FOUR + phase + ONE, partner)

    def start(self):
        for group in range(THREE):
            self.link(group, ZERO).start()
        for group in range(THREE):
            self.chip(group, -ONE).start()

    def step(self, phase):
        for group in range(THREE):
            self.link(group, phase).wait_recv()
            if phase < TWO:
                self.link(group, phase + ONE).start()
            self.chip(group, phase).start()

    def finish(self):
        for group in range(THREE):
            for phase in range(-ONE, THREE):
                self.chip(group, phase).wait()
            for phase in range(THREE):
                self.link(group, phase).wait_send()


def unflatten_layer(gath, layer, flat, w1_ref, w2_ref, slab_ref):
    base = layer * SLOT_ROWS

    def spread(dev, carry):
        z, y, x, core = dev // EIGHT, (dev // FOUR) % TWO, (dev // TWO) % TWO, dev % TWO

        def chunk(k, inner):
            block = gath[z, y, x, core, pl.ds(base + SIXTEEN * k, SIXTEEN), :]
            flat[pl.ds(dev * SHARD_ROWS + SIXTEEN * k, SIXTEEN), :] = block.astype(F32)
            return inner
        return lax.fori_loop(ZERO, SLOT_ROWS // SIXTEEN, chunk, carry, unroll=FIVE)
    lax.fori_loop(ZERO, SIXTEEN, spread, ZERO)

    def first(rb, carry):
        for j in range(SIXTEEN):
            block = flat[pl.ds(ROW_C1 + TH * rb + j, SIXTEEN, stride=SIXTEEN), :]
            w1_ref[layer, pl.ds(pl.multiple_of(SIXTEEN * rb, SIXTEEN), SIXTEEN), LANES * j:LANES * j + LANES] = block.astype(BF16)
        return carry
    lax.fori_loop(ZERO, IMAGES, first, ZERO)

    def second(rb, carry):
        for j in range(FOUR):
            block = flat[pl.ds(ROW_C2 + SIXTY_FOUR * rb + j, SIXTEEN, stride=FOUR), :]
            w2_ref[layer, pl.ds(pl.multiple_of(SIXTEEN * rb, SIXTEEN), SIXTEEN), LANES * j:LANES * j + LANES] = block.astype(BF16)
        return carry
    lax.fori_loop(ZERO, LANES, second, ZERO)
    slab_ref[layer, ZERO:QVALID, :] = flat[ZERO:QVALID, :]
    slab_ref[layer, QVALID:240, :] = flat[ROW_VEC:FLAT_ROWS, :]


def gather_kernel(pack_ref, w1_ref, w2_ref, slab_ref, head_ref, small_ref, gath, flat, send_sem, recv_sem, load_sem):
    where = place()
    me, coords, core, neighbours, partner = where
    load = pltpu.make_async_copy(pack_ref, gath.at[coords[ZERO], coords[ONE], coords[TWO], core], load_sem)
    load.start()
    enter_barrier(neighbours, partner)
    load.wait()
    third = AG_ROWS // THREE
    work = Gather(gath, where, [(third * g, third) for g in range(THREE)], send_sem, recv_sem, ZERO)
    work.start()
    for phase in range(THREE):
        work.step(phase)
    work.finish()
    for layer in range(TWO):
        unflatten_layer(gath, layer, flat, w1_ref, w2_ref, slab_ref)

    def spread_head(dev, carry):
        z, y, x, own = dev // EIGHT, (dev // FOUR) % TWO, (dev // TWO) % TWO, dev % TWO
        for j in range(EIGHT):
            head_ref[pl.ds(pl.multiple_of(IMAGES * dev, IMAGES), IMAGES), LANES * j:LANES * j + LANES] = gath[z, y, x, own, pl.ds(HEAD_OFF + IMAGES * j, IMAGES), :]
        small_ref[pl.ds(dev, ONE), :] = gath[z, y, x, own, pl.ds(SMALL_OFF, SIXTEEN), :].astype(F32)[ZERO:ONE, :]
        return carry
    lax.fori_loop(ZERO, SIXTEEN, spread_head, ZERO)


def gather_weights(pack):
    vmem = pl.BlockSpec(memory_space=pltpu.VMEM)
    return pl.pallas_call(
        gather_kernel,
        out_shape=(jax.ShapeDtypeStruct((TWO, CH, HID), BF16), jax.ShapeDtypeStruct((TWO, HID, CH), BF16), jax.ShapeDtypeStruct((TWO, SLAB_ROWS, LANES), F32), jax.ShapeDtypeStruct((CH, CLASS_PAD), BF16), jax.ShapeDtypeStruct((SIXTEEN, LANES), F32)),
        in_specs=[vmem],
        out_specs=(vmem,) * FIVE,
        scratch_shapes=[
            pltpu.VMEM((TWO, TWO, TWO, TWO, AG_ROWS, LANES), BF16),
            pltpu.VMEM((16640, LANES), F32),
            pltpu.SemaphoreType.DMA((21,)),
            pltpu.SemaphoreType.DMA((21,)),
            pltpu.SemaphoreType.DMA,
        ],
        compiler_params=pltpu.CompilerParams(collective_id=ZERO, has_side_effects=True, vmem_limit_bytes=VMEM_CAP),
        name='gather_weights',
    )(pack)


class Reduce:
    def __init__(self, buf, temps, where, row_groups, send_sem, recv_sem, sem0):
        self.buf, self.temps, self.where, self.groups = buf, temps, where, row_groups
        self.send_sem, self.recv_sem, self.sem0 = send_sem, recv_sem, sem0

    def views(self, group, phase):
        me, coords, core, neighbours, partner = self.where
        row0, rows = self.groups[group]
        order = ORDERS[group]
        if phase == ZERO:
            free = (ZERO, ONE, TWO)
            leave = slot_view(self.buf, coords, ONE - core, free, row0, rows)
            device = partner
            stay = coords
        else:
            axis = order[phase - ONE]
            free = tuple(a for a in range(THREE) if a in order[phase:])
            far = list(coords)
            far[axis] = ONE - coords[axis]
            leave = slot_view(self.buf, far, core, free, row0, rows)
            device = neighbours[axis]
            stay = coords
        land = self.temps[phase].at[(slice(None),) * len(free) + (pl.ds(row0, rows), slice(None))]
        return leave, land, device, free, stay

    def copy(self, group, phase):
        leave, land, device, free, stay = self.views(group, phase)
        sem = self.sem0 + group * FOUR + phase
        return pltpu.make_async_remote_copy(src_ref=leave, dst_ref=land, send_sem=self.send_sem.at[sem], recv_sem=self.recv_sem.at[sem], device_id=(device,), device_id_type=MESH_ID)

    def add(self, group, phase):
        me, coords, core, neighbours, partner = self.where
        leave, land, device, free, stay = self.views(group, phase)
        row0, rows = self.groups[group]
        temp = self.temps[phase]
        count = TWO ** len(free)
        per = max(ONE, EIGHT // count)
        while rows % (EIGHT * per):
            per //= TWO

        def chunk(k, carry):
            for part in range(per):
                start = pl.multiple_of(row0 + EIGHT * (per * k + part), EIGHT)
                for n in range(count):
                    index = list(coords)
                    bits = []
                    for pos, a in enumerate(free):
                        bit = (n // TWO ** (len(free) - ONE - pos)) % TWO
                        index[a] = bit
                        bits.append(bit)
                    target = (index[ZERO], index[ONE], index[TWO], core, pl.ds(start, EIGHT), slice(None))
                    self.buf[target] = self.buf[target] + temp[tuple(bits) + (pl.ds(start, EIGHT), slice(None))]
            return carry
        lax.fori_loop(ZERO, rows // (EIGHT * per), chunk, ZERO)

    def start(self):
        for group in range(THREE):
            self.copy(group, ZERO).start()

    def step(self, phase):
        for group in range(THREE):
            self.copy(group, phase).wait_recv()
            self.add(group, phase)
            if phase < THREE:
                self.copy(group, phase + ONE).start()

    def finish(self):
        for group in range(THREE):
            for phase in range(FOUR):
                self.copy(group, phase).wait_send()


def spread_layer(layer, flat, grad):
    base = layer * SLOT_ROWS

    def spread(dev, carry):
        z, y, x, core = dev // EIGHT, (dev // FOUR) % TWO, (dev // TWO) % TWO, dev % TWO

        def chunk(k, inner):
            grad[z, y, x, core, pl.ds(pl.multiple_of(base + EIGHT * k, EIGHT), EIGHT), :] = flat[pl.ds(dev * SHARD_ROWS + EIGHT * k, EIGHT), :]
            return inner
        return lax.fori_loop(ZERO, SLOT_ROWS // EIGHT, chunk, carry, unroll=TEN)
    lax.fori_loop(ZERO, SIXTEEN, spread, ZERO)


def square_sum(ref, coords, core, row0, rows):
    def chunk(k, total):
        block = ref[coords[ZERO], coords[ONE], coords[TWO], core, pl.ds(pl.multiple_of(row0 + EIGHT * k, EIGHT), EIGHT), :]
        return total + block * block
    return lax.fori_loop(ZERO, rows // EIGHT, chunk, jnp.zeros((EIGHT, LANES), F32), unroll=TWO)


def reduce_kernel(flat_hbm, gh_ref, gs_ref, loss_ref, gl_ref, ghead_ref, gsmall_ref, stat_ref, flat, grad, t0, t1, t2, t3, msg, box, send_sem, recv_sem, load_sem, tiny_send, tiny_recv):
    where = place()
    me, coords, core, neighbours, partner = where
    enter_barrier(neighbours, partner)
    for layer in (ONE, ZERO):
        copy = pltpu.make_async_copy(flat_hbm.at[layer], flat, load_sem)
        copy.start()
        copy.wait()
        spread_layer(layer, flat, grad)

    def spread_head(dev, carry):
        z, y, x, own = dev // EIGHT, (dev // FOUR) % TWO, (dev // TWO) % TWO, dev % TWO
        for j in range(EIGHT):
            grad[z, y, x, own, HEAD_OFF + IMAGES * j:HEAD_OFF + IMAGES * j + IMAGES, :] = gh_ref[pl.ds(pl.multiple_of(IMAGES * dev, IMAGES), IMAGES), LANES * j:LANES * j + LANES]
        grad[z, y, x, own, SMALL_OFF:AG_ROWS, :] = jnp.zeros((SIXTEEN, LANES), F32)
        grad[z, y, x, own, SMALL_OFF:SMALL_OFF + ONE, :] = gs_ref[pl.ds(dev, ONE), :]
        grad[z, y, x, own, SMALL_OFF + EIGHT:SMALL_OFF + SIXTEEN, :] = loss_ref[...]
        return carry
    lax.fori_loop(ZERO, SIXTEEN, spread_head, ZERO)
    third = AG_ROWS // THREE
    work = Reduce(grad, (t0, t1, t2, t3), where, [(third * g, third) for g in range(THREE)], send_sem, recv_sem, ZERO)
    work.start()
    for phase in range(FOUR):
        work.step(phase)
    work.finish()
    own = (coords[ZERO], coords[ONE], coords[TWO], core)
    for layer in range(TWO):
        last = layer * SLOT_ROWS + SHARD_ROWS
        grad[own + (pl.ds(last, ONE), slice(None))] = jnp.zeros((ONE, LANES), F32)
    total = square_sum(grad, coords, core, ZERO, SMALL_OFF + EIGHT)
    msg[ZERO] = jnp.broadcast_to(jnp.sum(total), (EIGHT, LANES))
    for n, device in enumerate([partner, neighbours[TWO], neighbours[ONE], neighbours[ZERO]]):
        copy = pltpu.make_async_remote_copy(src_ref=msg.at[n], dst_ref=box.at[n], send_sem=tiny_send.at[n], recv_sem=tiny_recv.at[n], device_id=(device,), device_id_type=MESH_ID)
        copy.start()
        copy.wait()
        msg[n + ONE] = msg[n] + box[n]
    stat_ref[ZERO] = msg[FOUR]
    stat_ref[ONE] = grad[own + (pl.ds(SMALL_OFF + EIGHT, EIGHT), slice(None))]
    for layer in range(TWO):
        gl_ref[layer] = grad[own + (pl.ds(layer * SLOT_ROWS, SLOT_ROWS), slice(None))]
    ghead_ref[...] = grad[own + (pl.ds(HEAD_OFF, TH), slice(None))]
    gsmall_ref[...] = grad[own + (pl.ds(SMALL_OFF, EIGHT), slice(None))]


def reduce_grads(flat, gh, gs, loss):
    vmem = pl.BlockSpec(memory_space=pltpu.VMEM)
    hbm = pl.BlockSpec(memory_space=pl.ANY)
    return pl.pallas_call(
        reduce_kernel,
        out_shape=(jax.ShapeDtypeStruct((TWO, SLOT_ROWS, LANES), F32), jax.ShapeDtypeStruct((TH, LANES), F32), jax.ShapeDtypeStruct((EIGHT, LANES), F32), jax.ShapeDtypeStruct((TWO, EIGHT, LANES), F32)),
        in_specs=[hbm, vmem, vmem, vmem],
        out_specs=(vmem,) * FOUR,
        scratch_shapes=[
            pltpu.VMEM((16640, LANES), F32),
            pltpu.VMEM((TWO, TWO, TWO, TWO, AG_ROWS, LANES), F32),
            pltpu.VMEM((TWO, TWO, TWO, AG_ROWS, LANES), F32),
            pltpu.VMEM((TWO, TWO, AG_ROWS, LANES), F32),
            pltpu.VMEM((TWO, AG_ROWS, LANES), F32),
            pltpu.VMEM((AG_ROWS, LANES), F32),
            pltpu.VMEM((FIVE, EIGHT, LANES), F32),
            pltpu.VMEM((FOUR, EIGHT, LANES), F32),
            pltpu.SemaphoreType.DMA((12,)),
            pltpu.SemaphoreType.DMA((12,)),
            pltpu.SemaphoreType.DMA,
            pltpu.SemaphoreType.DMA((FOUR,)),
            pltpu.SemaphoreType.DMA((FOUR,)),
        ],
        compiler_params=pltpu.CompilerParams(collective_id=ONE, has_side_effects=True, vmem_limit_bytes=VMEM_CAP),
        name='reduce_grads',
    )(flat, gh, gs, loss)

QUADS = 8
QROWS = 208
TOKENS = 49
ALL_ROWS = QUADS * QROWS
CHUNK = 256
BLOCK = 416
CLASSES = 1000
GLOBAL_IMAGES = 512.0
LN_EPS = 1e-6
GELU_A = 0.7978845608028654
GELU_B = GELU_A * 0.044715
HALF = 0.5
ROW_T2 = 98
INV49 = 81
LOW7 = 127
SLAB_VEC = 196
V_BT1 = 204
V_MIS = 206
STEP8 = 8


def mm(a, b):
    return jnp.dot(a, b, preferred_element_type=F32)


def mm_nt(a, b):
    return lax.dot_general(a, b, (((ONE,), (ONE,)), ((), ())), preferred_element_type=F32)


def iota(shape, axis):
    return lax.broadcasted_iota(jnp.int32, shape, axis)


def aligned(start, unit):
    return pl.multiple_of(start * unit, unit)


def stats(x):
    mean = jnp.mean(x, axis=-ONE, keepdims=True)
    centered = x - mean
    scale = lax.rsqrt(jnp.mean(centered * centered, axis=-ONE, keepdims=True) + LN_EPS)
    return centered * scale, scale


def fold8(x):
    return jnp.sum(x.reshape(x.shape[ZERO] // STEP8, STEP8, x.shape[ONE]), axis=ZERO)


def gelu_tanh(h):
    sq = h * h
    return sq, jnp.tanh(h * (GELU_A + GELU_B * sq))


def gelu(h):
    sq, t = gelu_tanh(h)
    half = HALF * h
    return (half + half * t).astype(BF16)


def gelu_both(h):
    sq, t = gelu_tanh(h)
    half = HALF * h
    slope = (HALF + HALF * t) + half * (F_ONE - t * t) * (GELU_A + (3.0 * GELU_B) * sq)
    return (half + half * t).astype(BF16), slope


def norm_back(xh, scale, gain, dy):
    dxh = dy * gain
    return scale * (dxh - jnp.mean(dxh, axis=-ONE, keepdims=True) - xh * jnp.mean(dxh * xh, axis=-ONE, keepdims=True))


def token_maps():
    s = iota((TOKEN_PAD, LANES), ZERO)
    lane = iota((TOKEN_PAD, LANES), ONE)
    j = ((lane - s) * INV49) & LOW7
    row = jnp.where(s < TOKENS, (j * TOKENS + s) >> SEVEN, -ONE)
    perm = (iota((LANES, LANES), ZERO) == ((iota((LANES, LANES), ONE) * TOKENS) & LOW7))
    return s, row, perm


def skew(x, s, left):
    for bit in range(SEVEN):
        amount = TWO ** bit
        x = jnp.where(((s >> bit) & ONE) == ONE, pltpu.roll(x, LANES - amount if left else amount, ONE), x)
    return x


def prep_layer(l, slab, vrow, bd, v2, ma1, mb1, ma2, mb2, col):
    for k in range(FOUR):
        lanes = slice(LANES * k, LANES * k + LANES)
        vrow[l, ZERO:ONE, lanes] = slab[l, SLAB_VEC + k:SLAB_VEC + k + ONE, :]
        vrow[l, ONE:TWO, lanes] = slab[l, SLAB_VEC + FOUR + k:SLAB_VEC + FIVE + k, :]
    lane = iota((IMAGES, LANES), ONE)
    cut = LANES - TOKENS
    v2[...] = jnp.where(lane < cut, pltpu.roll(slab[l, V_MIS:V_MIS + IMAGES, :], cut, ONE), pltpu.roll(slab[l, V_MIS + ONE:V_MIS + 33, :], cut, ONE))
    for row, first, count in ((TWO, ZERO, FOUR), (THREE, FOUR, FOUR), (FOUR, EIGHT, SIXTEEN), (FIVE, TWENTY_FOUR, FOUR)):
        for k in range(count):
            vrow[l, row:row + ONE, LANES * k:LANES * k + LANES] = v2[first + k:first + k + ONE, :]
    bd[...] = jnp.zeros_like(bd)
    for h in range(TWO):
        w = slab[l, pl.ds(h, TOKENS, stride=TWO), :]
        for i in range(FOUR):
            bd[TOKENS * i:TOKENS * i + TOKENS, TH * i + LANES * h:TH * i + LANES * h + LANES] = w
    mb1[l] = bd[ZERO:QROWS, :].astype(BF16)
    for h in range(TWO):
        for i in range(FOUR):
            bd[QVALID:QVALID + ONE, TH * i + LANES * h:TH * i + LANES * h + LANES] = slab[l, V_BT1 + h:V_BT1 + h + ONE, :]
    ma1[l] = bd[...].T[:, ZERO:QROWS].astype(BF16)
    bd[...] = jnp.zeros_like(bd)
    s, row, perm = token_maps()
    for h in range(TWO):
        def pick(r, acc):
            return jnp.where(row == r, slab[l, pl.ds(ROW_T2 + TOKENS * h + r, ONE), :], acc)
        x = skew(lax.fori_loop(ZERO, TOKENS, pick, jnp.zeros((TOKEN_PAD, LANES), F32)), s, True)
        w = mm(x.astype(BF16), perm.astype(BF16))[ZERO:TOKENS]
        for i in range(FOUR):
            bd[TOKENS * i:TOKENS * i + TOKENS, TH * i + LANES * h:TH * i + LANES * h + LANES] = w
    ma2[l] = bd[ZERO:QROWS, :].astype(BF16)
    mb2[l] = bd[...].T[:, ZERO:QROWS].astype(BF16)
    bias = jnp.where(iota((ONE, LANES), ONE) < TOKENS, slab[l, V_MIS:V_MIS + ONE, :], F_ZERO)
    wide = jnp.concatenate([jnp.broadcast_to(bias, (LANES, LANES)), jnp.zeros((LANES, LANES), F32)], axis=ONE)
    spread = wide
    for i in range(ONE, FOUR):
        spread = spread + pltpu.roll(wide, TOKENS * i, ONE)
    col[l] = spread.T[ZERO:QROWS, :]


def forward_layer(l, x_in, x_mid, x_out, vrow, ma1, ma2, col, w1, w2, uq, uch):
    def quad(q, carry):
        rows = pl.ds(aligned(q, QROWS), QROWS)
        xq = x_in[rows, :].astype(F32)
        n = token_input(xq, vrow, l)[TWO]
        for i in range(FOUR):
            uq[TH * i:TH * i + TH, :] = gelu(mm(ma1[l, TH * i:TH * i + TH, :], n))
        y = mm(ma2[l], uq[...])
        x1 = (xq + (y + jnp.concatenate([col[l]] * FOUR, axis=ONE))).astype(BF16)
        x_mid[rows, :] = x1
        x1 = x1.astype(F32)
        n2 = (stats(x1)[ZERO] * vrow[l, TWO:THREE, ZERO:CH] + vrow[l, THREE:FOUR, ZERO:CH]).astype(BF16)
        for c in range(FOUR):
            lanes = slice(CH * c, CH * c + CH)
            uch[:, lanes] = gelu(mm(n2, w1[l, :, lanes]) + vrow[l, FOUR:FIVE, lanes])
        x_out[rows, :] = (x1 + (mm(uch[...], w2[l]) + vrow[l, FIVE:SIX, ZERO:CH])).astype(BF16)
        return carry
    lax.fori_loop(ZERO, QUADS, quad, ZERO)


def token_input(xq, vrow, l):
    xh, scale = stats(xq)
    n = xh * vrow[l, ZERO:ONE, ZERO:CH] + vrow[l, ONE:TWO, ZERO:CH]
    return xh, scale, jnp.where(iota((QROWS, CH), ZERO) == QVALID, F_ONE, n).astype(BF16)


def image_of(shape, axis):
    c = iota(shape, axis)
    return jnp.where(c < QVALID, (c >= TOKENS).astype(jnp.int32) + (c >= TWO * TOKENS).astype(jnp.int32) + (c >= THREE * TOKENS).astype(jnp.int32), IMAGES)


def head_pass(x_out, labels, small, head, d, pool, srow, gsum, gh, gs, loss):
    for k in range(FOUR):
        lanes = slice(LANES * k, LANES * k + LANES)
        srow[ZERO:ONE, lanes] = small[k:k + ONE, :]
        srow[ONE:TWO, lanes] = small[FOUR + k:FIVE + k, :]
    for k in range(EIGHT):
        srow[TWO:THREE, LANES * k:LANES * k + LANES] = small[EIGHT + k:NINE + k, :]
    gain, shift = srow[ZERO:ONE, ZERO:CH], srow[ONE:TWO, ZERO:CH]
    pool[...] = jnp.zeros_like(pool)

    def quad(q, carry):
        xh, scale = stats(x_out[pl.ds(aligned(q, QROWS), QROWS), :].astype(F32))
        pick = (iota((IMAGES, QROWS), ZERO) == image_of((IMAGES, QROWS), ONE) + FOUR * q)
        pool[...] += mm(pick.astype(BF16), (xh * gain + shift).astype(BF16))
        return carry
    lax.fori_loop(ZERO, QUADS, quad, ZERO)
    pooled = (pool[...] / TOKENS).astype(BF16)
    real = iota((IMAGES, CLASS_PAD), ONE) < CLASSES
    logits = jnp.where(real, mm(pooled, head[...]) + srow[TWO:THREE, :], -1e30)
    top = jnp.max(logits, axis=-ONE, keepdims=True)
    log_norm = top + jnp.log(jnp.sum(jnp.exp(logits - top), axis=-ONE, keepdims=True))
    hit = iota((IMAGES, CLASS_PAD), ONE) == labels[:, ZERO:ONE]
    picked = jnp.sum(jnp.where(hit, logits, F_ZERO), axis=-ONE, keepdims=True)
    loss[...] = jnp.broadcast_to(jnp.sum(log_norm - picked), loss.shape)
    d_logits = (jnp.exp(logits - log_norm) - hit.astype(F32)) / GLOBAL_IMAGES
    d_bf = d_logits.astype(BF16)
    gh[...] = mm(pool_t(pooled), d_bf)
    d_pool = (mm_nt(d_bf, head[...]) / TOKENS).astype(BF16)
    gsum[...] = jnp.zeros_like(gsum)

    def back(q, carry):
        rows = pl.ds(aligned(q, QROWS), QROWS)
        xh, scale = stats(x_out[rows, :].astype(F32))
        pick = (iota((QROWS, IMAGES), ONE) == image_of((QROWS, IMAGES), ZERO) + FOUR * q)
        dy = mm(pick.astype(BF16), d_pool)
        gsum[ZERO] += fold8(dy * xh)
        gsum[ONE] += fold8(dy)
        d[rows, :] = norm_back(xh, scale, gain, dy)
        return carry
    lax.fori_loop(ZERO, QUADS, back, ZERO)
    g_gain = jnp.sum(gsum[ZERO], axis=ZERO, keepdims=True)
    g_shift = jnp.sum(gsum[ONE], axis=ZERO, keepdims=True)
    g_bias = jnp.sum(d_logits, axis=ZERO, keepdims=True)
    for k in range(FOUR):
        lanes = slice(LANES * k, LANES * k + LANES)
        gs[k:k + ONE, :] = g_gain[:, lanes]
        gs[FOUR + k:FIVE + k, :] = g_shift[:, lanes]
    for k in range(EIGHT):
        gs[EIGHT + k:NINE + k, :] = g_bias[:, LANES * k:LANES * k + LANES]


def pool_t(pooled):
    return pooled.astype(F32).T.astype(BF16)


def channel_back(l, x_mid, d, vrow, w1, w2, n2, dbf, n2t, dt, uh, dh, dn2, flat, gsum, gb1):
    gsum[...] = jnp.zeros_like(gsum)
    gb1[...] = jnp.zeros_like(gb1)

    def quad(q, carry):
        rows = pl.ds(aligned(q, QROWS), QROWS)
        n2[rows, :] = (stats(x_mid[rows, :].astype(F32))[ZERO] * vrow[l, TWO:THREE, ZERO:CH] + vrow[l, THREE:FOUR, ZERO:CH]).astype(BF16)
        dq = d[rows, :]
        gsum[FOUR] += fold8(dq)
        dbf[rows, :] = dq.astype(BF16)
        dn2[rows, :] = jnp.zeros((QROWS, CH), F32)
        return carry
    lax.fori_loop(ZERO, QUADS, quad, ZERO)
    for k in range(ALL_ROWS // LANES):
        lanes = slice(LANES * k, LANES * k + LANES)
        n2t[:, lanes] = n2[lanes, :].T
        dt[:, lanes] = dbf[lanes, :].T

    def chunk(c, carry):
        lanes = pl.ds(aligned(c, CHUNK), CHUNK)

        def block(b, inner):
            rows = pl.ds(aligned(b, BLOCK), BLOCK)
            u, slope = gelu_both(mm(n2[rows, :], w1[l, :, lanes]) + vrow[l, FOUR:FIVE, lanes])
            uh[rows, :] = u
            dhid = mm_nt(dbf[rows, :], w2[l, lanes, :]).astype(BF16).astype(F32) * slope
            gb1[:, lanes] += fold8(dhid)
            dhid = dhid.astype(BF16)
            dh[rows, :] = dhid
            dn2[rows, :] += mm_nt(dhid, w1[l, :, lanes])
            return inner
        lax.fori_loop(ZERO, ALL_ROWS // BLOCK, block, ZERO)
        g1 = mm(n2t[...], dh[...])
        for r in range(CH // STEP8):
            for k in range(TWO):
                flat[pl.ds(ROW_C1 + LANES * r + k + TWO * c, STEP8, stride=SIXTEEN), :] = g1[STEP8 * r:STEP8 * r + STEP8, LANES * k:LANES * k + LANES]
        g2 = mm(dt[...], uh[...]).T
        for r in range(CHUNK // STEP8):
            for k in range(FOUR):
                flat[pl.ds(ROW_C2 + FOUR * (STEP8 * r) + k + FOUR * CHUNK * c, STEP8, stride=FOUR), :] = g2[STEP8 * r:STEP8 * r + STEP8, LANES * k:LANES * k + LANES]
        return carry
    lax.fori_loop(ZERO, HID // CHUNK, chunk, ZERO)


def token_back(l, x_in, x_mid, d, vrow, dn2, ma1, mb1, ma2, mb2, uq, dq_ref, acc1, acc2, rowsum, colsum, gsum):
    for ref in (acc1, acc2, rowsum, colsum):
        ref[...] = jnp.zeros_like(ref)

    def quad(q, carry):
        rows = pl.ds(aligned(q, QROWS), QROWS)
        xh, scale = stats(x_mid[rows, :].astype(F32))
        dy = dn2[rows, :].astype(BF16).astype(F32)
        gsum[TWO] += fold8(dy * xh)
        gsum[THREE] += fold8(dy)
        d_after = norm_back(xh, scale, vrow[l, TWO:THREE, ZERO:CH], dy) + d[rows, :]
        part = d_after[:, ZERO:LANES]
        for k in range(ONE, FOUR):
            part = part + d_after[:, LANES * k:LANES * k + LANES]
        colsum[ZERO:QROWS, :] += part
        d_bf = d_after.astype(BF16)
        xh, scale, n = token_input(x_in[rows, :].astype(F32), vrow, l)
        for i in range(FOUR):
            part = slice(TH * i, TH * i + TH)
            u, slope = gelu_both(mm(ma1[l, part, :], n))
            uq[part, :] = u
            dhid = mm(mb2[l, part, :], d_bf).astype(BF16).astype(F32) * slope
            total = dhid[:, ZERO:LANES]
            for k in range(ONE, FOUR):
                total = total + dhid[:, LANES * k:LANES * k + LANES]
            rowsum[part, :] += total
            dq_ref[part, :] = dhid.astype(BF16)
        acc1[...] += mm_nt(n, dq_ref[...])
        acc2[...] += mm_nt(d_bf, uq[...])
        dy = mm(mb1[l], dq_ref[...]).astype(BF16).astype(F32)
        gsum[ZERO] += fold8(dy * xh)
        gsum[ONE] += fold8(dy)
        d[rows, :] = norm_back(xh, scale, vrow[l, ZERO:ONE, ZERO:CH], dy) + d_after
        return carry
    lax.fori_loop(ZERO, QUADS, quad, ZERO)


def small_flat(l, flat, acc1, acc2, rowsum, colsum, gsum, gb1, v2):
    g = sum_images(acc1)
    for h in range(TWO):
        flat[pl.ds(h, TOKENS, stride=TWO), :] = g[:, LANES * h:LANES * h + LANES]
    g = sum_images(acc2)
    s, row, perm = token_maps()
    for h in range(TWO):
        padded = jnp.concatenate([g[:, LANES * h:LANES * h + LANES], jnp.zeros((SEVEN, LANES), F32)], axis=ZERO)
        x = skew(lax.dot_general(padded, perm.astype(F32), (((ONE,), (ONE,)), ((), ())), precision=lax.Precision.HIGHEST, preferred_element_type=F32), s, False)

        def place_row(r, carry):
            flat[pl.ds(ROW_T2 + TOKENS * h + r, ONE), :] = jnp.sum(jnp.where(row == r, x, F_ZERO), axis=ZERO, keepdims=True)
            return carry
        lax.fori_loop(ZERO, TOKENS, place_row, ZERO)
    flat[ROW_VEC:FLAT_ROWS + SIXTEEN, :] = jnp.zeros((FLAT_ROWS + SIXTEEN - ROW_VEC, LANES), F32)
    for n in range(TWO):
        v = jnp.sum(gsum[n], axis=ZERO, keepdims=True)
        for k in range(FOUR):
            flat[ROW_VEC + FOUR * n + k:ROW_VEC + FOUR * n + k + ONE, :] = v[:, LANES * k:LANES * k + LANES]
    t = jnp.sum(rowsum[...].T, axis=ZERO, keepdims=True)
    t = t[:, ZERO:TH] + t[:, TH:TWO * TH] + t[:, TWO * TH:THREE * TH] + t[:, THREE * TH:FOUR * TH]
    for h in range(TWO):
        flat[ROW_VEC + EIGHT + h:ROW_VEC + NINE + h, :] = t[:, LANES * h:LANES * h + LANES]
    v2[...] = jnp.zeros_like(v2)
    lists = [(jnp.sum(gsum[TWO], axis=ZERO, keepdims=True), ZERO, FOUR), (jnp.sum(gsum[THREE], axis=ZERO, keepdims=True), FOUR, FOUR), (jnp.sum(gb1[...], axis=ZERO, keepdims=True), EIGHT, SIXTEEN), (jnp.sum(gsum[FOUR], axis=ZERO, keepdims=True), TWENTY_FOUR, FOUR)]
    for v, first, count in lists:
        for k in range(count):
            v2[first + k:first + k + ONE, :] = v[:, LANES * k:LANES * k + LANES]
    turned = pltpu.roll(v2[...], TOKENS, ONE)
    t = jnp.broadcast_to(jnp.sum(colsum[...].T, axis=ZERO, keepdims=True), (STEP8, TWO * LANES))
    b2 = t
    for i in range(ONE, FOUR):
        b2 = b2 + pltpu.roll(t, TWO * LANES - TOKENS * i, ONE)
    before = jnp.concatenate([b2[ZERO:ONE, ZERO:LANES], turned[ZERO:LAST_IMAGE, :]], axis=ZERO)
    merged = jnp.where(iota((IMAGES, LANES), ONE) < TOKENS, before, turned)
    flat[ROW_VEC + TEN:ROW_VEC + 42, :] = merged


def sum_images(acc):
    g = acc[ZERO:TOKENS, ZERO:TH]
    for i in range(ONE, FOUR):
        g = g + acc[TOKENS * i:TOKENS * i + TOKENS, TH * i:TH * i + TH]
    return g


def step_kernel(x0, labels, w1, w2, slab, head, small, flat_out, gh, gs, loss, x1, x2, x3, x4, d, dn2, n2, dbf, n2t, dt, uh, dh, uq, dq_ref, uch, ma1, mb1, ma2, mb2, col, vrow, v2, bd, srow, pool, gsum, gb1, acc1, acc2, rowsum, colsum, flat, sem):
    for l in range(TWO):
        prep_layer(l, slab, vrow, bd, v2, ma1, mb1, ma2, mb2, col)
    forward_layer(ZERO, x0, x1, x2, vrow, ma1, ma2, col, w1, w2, uq, uch)
    forward_layer(ONE, x2, x3, x4, vrow, ma1, ma2, col, w1, w2, uq, uch)
    head_pass(x4, labels, small, head, d, pool, srow, gsum, gh, gs, loss)
    for l, x_in, x_mid in ((ONE, x2, x3), (ZERO, x0, x1)):
        channel_back(l, x_mid, d, vrow, w1, w2, n2, dbf, n2t, dt, uh, dh, dn2, flat, gsum, gb1)
        token_back(l, x_in, x_mid, d, vrow, dn2, ma1, mb1, ma2, mb2, uq, dq_ref, acc1, acc2, rowsum, colsum, gsum)
        small_flat(l, flat, acc1, acc2, rowsum, colsum, gsum, gb1, v2)
        copy = pltpu.make_async_copy(flat, flat_out.at[l], sem)
        copy.start()
        copy.wait()


def local_step(x0, labels, w1, w2, slab, head, small):
    vmem = pl.BlockSpec(memory_space=pltpu.VMEM)
    act = pltpu.VMEM((ALL_ROWS, CH), BF16)
    wide = pltpu.VMEM((ALL_ROWS, CH), F32)
    across = pltpu.VMEM((CH, ALL_ROWS), BF16)
    part = pltpu.VMEM((ALL_ROWS, CHUNK), BF16)
    tok = pltpu.VMEM((FOUR * TH, CH), BF16)
    tall = pltpu.VMEM((TWO, FOUR * TH, QROWS), BF16)
    flat_mat = pltpu.VMEM((TWO, QROWS, FOUR * TH), BF16)
    acc = pltpu.VMEM((QROWS, FOUR * TH), F32)
    return pl.pallas_call(
        step_kernel,
        out_shape=(jax.ShapeDtypeStruct((TWO, FLAT_ROWS + SIXTEEN, LANES), F32), jax.ShapeDtypeStruct((CH, CLASS_PAD), F32), jax.ShapeDtypeStruct((SIXTEEN, LANES), F32), jax.ShapeDtypeStruct((STEP8, LANES), F32)),
        in_specs=[vmem] * SEVEN,
        out_specs=(pl.BlockSpec(memory_space=pl.ANY), vmem, vmem, vmem),
        scratch_shapes=[act, act, act, act, wide, wide, act, act, across, across, part, part, tok, tok, pltpu.VMEM((QROWS, HID), BF16),
                        tall, flat_mat, flat_mat, tall, pltpu.VMEM((TWO, QROWS, LANES), F32), pltpu.VMEM((TWO, STEP8, HID), F32), pltpu.VMEM((IMAGES, LANES), F32), pltpu.VMEM((TWO * LANES, FOUR * TH), F32),
                        pltpu.VMEM((STEP8, CLASS_PAD), F32), pltpu.VMEM((IMAGES, CH), F32), pltpu.VMEM((FIVE, STEP8, CH), F32), pltpu.VMEM((STEP8, HID), F32), acc, acc,
                        pltpu.VMEM((FOUR * TH, LANES), F32), pltpu.VMEM((TWO * LANES, LANES), F32), pltpu.VMEM((FLAT_ROWS + SIXTEEN, LANES), F32), pltpu.SemaphoreType.DMA],
        compiler_params=pltpu.CompilerParams(vmem_limit_bytes=VMEM_CAP),
        name='local_step',
    )(x0, labels, w1, w2, slab, head, small)


LEARN_RATE = 0.003
BETA_ONE = 0.9
BETA_TWO = 0.999
ADAM_EPS = 1e-8
WEIGHT_DECAY = 0.03
ADAM_STEP = 10


def adam_update(master, gradient, moment, second, decay_rate):
    moment_new = BETA_ONE * moment + (F_ONE - BETA_ONE) * gradient
    second_new = BETA_TWO * second + (F_ONE - BETA_TWO) * gradient * gradient
    m_hat = moment_new / (F_ONE - BETA_ONE ** ADAM_STEP)
    v_hat = second_new / (F_ONE - BETA_TWO ** ADAM_STEP)
    master_new = master - LEARN_RATE * (m_hat / (jnp.sqrt(v_hat) + ADAM_EPS) + decay_rate * master)
    return master_new, moment_new, second_new


def solution(mesh):
    row_spec = P('fsdp')
    layer_spec = P(None, 'fsdp')
    in_specs = (row_spec, row_spec, layer_spec, row_spec, row_spec, layer_spec, row_spec, row_spec, layer_spec, row_spec, row_spec)
    out_specs = (P(),) + in_specs[TWO:]

    def device_step(act_in, labels, layer_p, head_w, small_p, layer_m, head_m, small_m, layer_v, head_v, small_v):
        mat_len = ROW_VEC * LANES
        quads = jnp.pad(act_in.reshape(QUADS, QVALID, CH), ((ZERO, ZERO), (ZERO, QROWS - QVALID), (ZERO, ZERO))).reshape(ALL_ROWS, CH)
        layer_bf = jnp.pad(layer_p.astype(BF16).reshape(TWO, SHARD_ROWS, LANES), ((ZERO, ZERO), (ZERO, ONE), (ZERO, ZERO)))
        head_bf = jnp.pad(head_w.astype(BF16), ((ZERO, ZERO), (ZERO, CLASS_PAD - CLASSES))).reshape(IMAGES, EIGHT, LANES).transpose(ONE, ZERO, TWO).reshape(TH, LANES)
        small_bf = jnp.pad(small_p.astype(BF16).reshape(ONE, LANES), ((ZERO, 15), (ZERO, ZERO)))
        weights = gather_weights(jnp.concatenate([layer_bf.reshape(TWO * SLOT_ROWS, LANES), head_bf, small_bf]))
        local = local_step(quads, jnp.broadcast_to(labels[:, None], (IMAGES, LANES)), *weights)
        gl, ghead, gsmall, stat = reduce_grads(*local)
        layer_g = gl[:, :SHARD_ROWS].reshape(TWO, SHARD_ROWS * LANES)
        head_g = ghead.reshape(EIGHT, IMAGES, LANES).transpose(ONE, ZERO, TWO).reshape(IMAGES, CLASS_PAD)[:, :CLASSES]
        small_g = gsmall[ZERO]
        loss_value = stat[ONE, ZERO, ZERO] / GLOBAL_IMAGES
        clip_scale = F_ONE / jnp.maximum(F_ONE, jnp.sqrt(stat[ZERO, ZERO, ZERO]))
        shard_len = layer_p.shape[ONE]
        flat_pos = lax.axis_index('fsdp') * shard_len + jnp.arange(shard_len)
        layer_decay = jnp.where(flat_pos < mat_len, WEIGHT_DECAY, F_ZERO)[None, :]
        new_lp, new_lm, new_lv = adam_update(layer_p, layer_g * clip_scale, layer_m, layer_v, layer_decay)
        new_hw, new_hm, new_hv = adam_update(head_w, head_g * clip_scale, head_m, head_v, WEIGHT_DECAY)
        new_sp, new_sm, new_sv = adam_update(small_p, small_g * clip_scale, small_m, small_v, F_ZERO)
        return (loss_value, new_lp, new_hw, new_sp, new_lm, new_hm, new_sm, new_lv, new_hv, new_sv)

    return jax.shard_map(device_step, mesh=mesh, in_specs=in_specs, out_specs=out_specs, check_vma=False)
```

```python
import functools
import math
import jax
import jax.numpy as jnp
from jax import lax
from jax.experimental import pallas as pl
from jax.experimental.pallas import tpu as pltpu
from jax.sharding import PartitionSpec as P

ZERO = 0
ONE = 1
TWO = 2
THREE = 3
FOUR = 4
FIVE = 5
SIX = 6
SEVEN = 7
EIGHT = 8
NINE = 9
SIXTEEN = 16
LANES = 128
IMAGES = 32
LAST_IMAGE = 31
CH = 512
CLASS_PAD = 1024
HID = 2048
TH = 256
F_ZERO = 0.0
F_ONE = 1.0
TWENTY_FOUR = 24
TOKEN_PAD = 56
QVALID = 196
SIXTY_FOUR = 64
TEN = 10
MESH_ID = pl.DeviceIdType.MESH
F32 = jnp.float32
BF16 = jnp.bfloat16

SHARD_ROWS = 1039
SLOT_ROWS = 1040
ROW_C1 = 196
ROW_C2 = 8388
ROW_VEC = 16580
FLAT_ROWS = 16624
SLAB_ROWS = 240
HEAD_OFF = 2 * SLOT_ROWS
SMALL_OFF = HEAD_OFF + 256
AG_ROWS = SMALL_OFF + 16
HEAD_ROWS = 272
ORDERS = ((2, 1, 0), (1, 0, 2), (0, 2, 1))
AXIS_STEP = (8, 4, 2)


def place():
    me = lax.axis_index('fsdp')
    coords = [me // EIGHT, (me // FOUR) % TWO, (me // TWO) % TWO]
    core = me % TWO
    neighbours = [me + AXIS_STEP[a] - TWO * AXIS_STEP[a] * coords[a] for a in range(THREE)]
    partner = me + ONE - TWO * core
    return me, coords, core, neighbours, partner


def enter_barrier(neighbours, partner):
    barrier = pltpu.get_barrier_semaphore()
    for other in list(neighbours) + [partner]:
        pl.semaphore_signal(barrier, inc=ONE, device_id=(other,), device_id_type=MESH_ID)
    pl.semaphore_wait(barrier, FOUR)


def slot_view(buf, coords, core, free_axes, row0, rows):
    index = [pl.ds(ZERO, TWO) if a in free_axes else coords[a] for a in range(THREE)]
    return buf.at[index[ZERO], index[ONE], index[TWO], core, pl.ds(row0, rows), :]


class Gather:
    def __init__(self, buf, where, row_groups, send_sem, recv_sem, sem0):
        self.buf, self.where, self.groups = buf, where, row_groups
        self.send_sem, self.recv_sem, self.sem0 = send_sem, recv_sem, sem0
        self.pending = []

    def copy(self, view, sem, device):
        return pltpu.make_async_remote_copy(src_ref=view, dst_ref=view, send_sem=self.send_sem.at[self.sem0 + sem], recv_sem=self.recv_sem.at[self.sem0 + sem], device_id=(device,), device_id_type=MESH_ID)

    def link(self, group, phase):
        me, coords, core, neighbours, partner = self.where
        order = ORDERS[group]
        row0, rows = self.groups[group]
        view = slot_view(self.buf, coords, core, order[:phase], row0, rows)
        return self.copy(view, group * THREE + phase, neighbours[order[phase]])

    def chip(self, group, phase):
        me, coords, core, neighbours, partner = self.where
        order = ORDERS[group]
        row0, rows = self.groups[group]
        if phase < ZERO:
            view = slot_view(self.buf, coords, core, (), row0, rows)
        else:
            far = list(coords)
            far[order[phase]] = ONE - coords[order[phase]]
            view = slot_view(self.buf, far, core, order[:phase], row0, rows)
        return self.copy(view, NINE + group * FOUR + phase + ONE, partner)

    def start(self):
        for group in range(THREE):
            self.link(group, ZERO).start()
        for group in range(THREE):
            self.chip(group, -ONE).start()

    def step(self, phase):
        for group in range(THREE):
            self.link(group, phase).wait_recv()
            if phase < TWO:
                self.link(group, phase + ONE).start()
            self.chip(group, phase).start()

    def finish(self):
        for group in range(THREE):
            for phase in range(-ONE, THREE):
                self.chip(group, phase).wait()
            for phase in range(THREE):
                self.link(group, phase).wait_send()


def slot_of(dev):
    return dev // EIGHT, (dev // FOUR) % TWO, (dev // TWO) % TWO, dev % TWO


def unflatten_layer(gath, layer, flat, stage, stage_sem, w1_ref, w2_ref, slab_ref):
    base = layer * SLOT_ROWS

    def fetch(dev):
        z, y, x, core = slot_of(dev)
        return pltpu.make_async_copy(gath.at[z, y, x, core, pl.ds(base, SLOT_ROWS), :], stage.at[dev % TWO], stage_sem.at[dev % TWO])
    fetch(ZERO).start()

    def spread(dev, carry):
        fetch(dev).wait()

        @pl.when(dev < 15)
        def _():
            fetch(dev + ONE).start()

        def chunk(k, inner):
            block = stage[dev % TWO, pl.ds(pl.multiple_of(SIXTEEN * k, SIXTEEN), SIXTEEN), :]
            flat[pl.ds(dev * SHARD_ROWS + SIXTEEN * k, SIXTEEN), :] = block.astype(F32)
            return inner
        return lax.fori_loop(ZERO, SLOT_ROWS // SIXTEEN, chunk, carry, unroll=FIVE)
    lax.fori_loop(ZERO, SIXTEEN, spread, ZERO)

    def first(rb, carry):
        for j in range(SIXTEEN):
            block = flat[pl.ds(ROW_C1 + TH * rb + j, SIXTEEN, stride=SIXTEEN), :]
            w1_ref[layer, pl.ds(pl.multiple_of(SIXTEEN * rb, SIXTEEN), SIXTEEN), LANES * j:LANES * j + LANES] = block.astype(BF16)
        return carry
    lax.fori_loop(ZERO, IMAGES, first, ZERO)

    def second(rb, carry):
        for j in range(FOUR):
            block = flat[pl.ds(ROW_C2 + SIXTY_FOUR * rb + j, SIXTEEN, stride=FOUR), :]
            w2_ref[layer, pl.ds(pl.multiple_of(SIXTEEN * rb, SIXTEEN), SIXTEEN), LANES * j:LANES * j + LANES] = block.astype(BF16)
        return carry
    lax.fori_loop(ZERO, LANES, second, ZERO, unroll=FOUR)
    slab_ref[layer, ZERO:QVALID, :] = flat[ZERO:QVALID, :]
    slab_ref[layer, QVALID:240, :] = flat[ROW_VEC:FLAT_ROWS, :]


def unflatten_head(gath, stage, stage_sem, head_ref, small_ref):
    def fetch(dev):
        z, y, x, core = slot_of(dev)
        return pltpu.make_async_copy(gath.at[z, y, x, core, pl.ds(HEAD_OFF, HEAD_ROWS), :], stage.at[dev % TWO, pl.ds(ZERO, HEAD_ROWS), :], stage_sem.at[dev % TWO])
    fetch(ZERO).start()

    def spread(dev, carry):
        fetch(dev).wait()

        @pl.when(dev < 15)
        def _():
            fetch(dev + ONE).start()
        for j in range(EIGHT):
            head_ref[pl.ds(pl.multiple_of(IMAGES * dev, IMAGES), IMAGES), LANES * j:LANES * j + LANES] = stage[dev % TWO, IMAGES * j:IMAGES * j + IMAGES, :]
        small_ref[pl.ds(dev, ONE), :] = stage[dev % TWO, TH:272, :].astype(F32)[ZERO:ONE, :]
        return carry
    lax.fori_loop(ZERO, SIXTEEN, spread, ZERO)


class Reduce:
    def __init__(self, flat, pitch, rows, groups, out, out_row, bufs, where, sems):
        self.flat, self.pitch, self.rows, self.groups, self.out, self.out_row = flat, pitch, rows, groups, out, out_row
        self.leaving, self.temps = bufs[ZERO], bufs[ONE:]
        self.where = where
        self.send_sem, self.recv_sem = sems

    def spread(self):
        me, coords, core, neighbours, partner = self.where

        def chunk(k, carry):
            for n in range(EIGHT):
                self.leaving[n // FOUR, (n // TWO) % TWO, n % TWO, pl.ds(pl.multiple_of(EIGHT * k, EIGHT), EIGHT), :] = self.flat[pl.ds(self.pitch * (TWO * n + ONE - core) + EIGHT * k, EIGHT), :]
            return carry
        lax.fori_loop(ZERO, self.rows // EIGHT, chunk, ZERO)

    def views(self, group, phase):
        me, coords, core, neighbours, partner = self.where
        row0, rows = self.groups[group]
        order = ORDERS[group]
        if phase == ZERO:
            free = (ZERO, ONE, TWO)
            leave = self.leaving.at[:, :, :, pl.ds(row0, rows), :]
            device = partner
        else:
            axis = order[phase - ONE]
            free = tuple(a for a in range(THREE) if a in order[phase:])
            index = [pl.ds(ZERO, TWO) if a in free else coords[a] for a in range(THREE)]
            index[axis] = ONE - coords[axis]
            leave = self.temps[ZERO].at[index[ZERO], index[ONE], index[TWO], pl.ds(row0, rows), :]
            device = neighbours[axis]
        land = self.temps[phase].at[(slice(None),) * len(free) + (pl.ds(row0, rows), slice(None))]
        return leave, land, device, free

    def copy(self, group, phase):
        leave, land, device, free = self.views(group, phase)
        sem = group * FOUR + phase
        return pltpu.make_async_remote_copy(src_ref=leave, dst_ref=land, send_sem=self.send_sem.at[sem], recv_sem=self.recv_sem.at[sem], device_id=(device,), device_id_type=MESH_ID)

    def add(self, group, phase):
        me, coords, core, neighbours, partner = self.where
        free = self.views(group, phase)[THREE]
        row0, rows = self.groups[group]
        total, temp = self.temps[ZERO], self.temps[phase]
        count = TWO ** len(free)
        per = max(ONE, EIGHT // count)
        while rows % (EIGHT * per):
            per //= TWO

        def chunk(k, carry):
            for part in range(per):
                start = pl.multiple_of(row0 + EIGHT * (per * k + part), EIGHT)
                for n in range(count):
                    index = list(coords)
                    bits = []
                    for pos, a in enumerate(free):
                        bit = (n // TWO ** (len(free) - ONE - pos)) % TWO
                        index[a] = bit
                        bits.append(bit)
                    target = (index[ZERO], index[ONE], index[TWO], pl.ds(start, EIGHT), slice(None))
                    if phase == ZERO:
                        value = total[target] + self.flat[pl.ds(self.pitch * (TWO * n + core) + start, EIGHT), :]
                    else:
                        value = total[target] + temp[tuple(bits) + (pl.ds(start, EIGHT), slice(None))]
                    if phase == THREE:
                        self.out[pl.ds(pl.multiple_of(self.out_row + start, EIGHT), EIGHT), :] = value
                    else:
                        total[target] = value
            return carry
        lax.fori_loop(ZERO, rows // (EIGHT * per), chunk, ZERO)

    def start(self):
        self.spread()
        for group in range(THREE):
            self.copy(group, ZERO).start()

    def step(self, phase):
        for group in range(THREE):
            self.copy(group, phase).wait_recv()
            self.add(group, phase)
            if phase < THREE:
                self.copy(group, phase + ONE).start()

    def finish(self):
        for group in range(THREE):
            for phase in range(FOUR):
                self.copy(group, phase).wait_send()


def square_sum(ref, row0, rows):
    def chunk(k, total):
        block = ref[pl.ds(pl.multiple_of(row0 + EIGHT * k, EIGHT), EIGHT), :]
        return total + block * block
    return lax.fori_loop(ZERO, rows // EIGHT, chunk, jnp.zeros((EIGHT, LANES), F32), unroll=TWO)


QUADS = 8
QROWS = 208
TOKENS = 49
ALL_ROWS = QUADS * QROWS
CHUNK = 256
BLOCK = 416
CLASSES = 1000
GLOBAL_IMAGES = 512.0
LN_EPS = 1e-6
GELU_A = 0.7978845608028654
GELU_B = GELU_A * 0.044715
HALF = 0.5
ROW_T2 = 98
INV49 = 81
LOW7 = 127
SLAB_VEC = 196
V_BT1 = 204
V_MIS = 206
STEP8 = 8


def mm(a, b):
    return jnp.dot(a, b, preferred_element_type=F32)


def mm_nt(a, b):
    return lax.dot_general(a, b, (((ONE,), (ONE,)), ((), ())), preferred_element_type=F32)


def iota(shape, axis):
    return lax.broadcasted_iota(jnp.int32, shape, axis)


def aligned(start, unit):
    return pl.multiple_of(start * unit, unit)


def stats(x):
    mean = jnp.mean(x, axis=-ONE, keepdims=True)
    centered = x - mean
    scale = lax.rsqrt(jnp.mean(centered * centered, axis=-ONE, keepdims=True) + LN_EPS)
    return centered * scale, scale


def fold8(x):
    return jnp.sum(x.reshape(x.shape[ZERO] // STEP8, STEP8, x.shape[ONE]), axis=ZERO)


def gelu_tanh(h):
    sq = h * h
    return sq, jnp.tanh(h * (GELU_A + GELU_B * sq))


def gelu(h):
    sq, t = gelu_tanh(h)
    half = HALF * h
    return (half + half * t).astype(BF16)


def gelu_both(h):
    sq, t = gelu_tanh(h)
    half = HALF * h
    slope = (HALF + HALF * t) + half * (F_ONE - t * t) * (GELU_A + (3.0 * GELU_B) * sq)
    return (half + half * t).astype(BF16), slope


def norm_back(xh, scale, gain, dy):
    dxh = dy * gain
    return scale * (dxh - jnp.mean(dxh, axis=-ONE, keepdims=True) - xh * jnp.mean(dxh * xh, axis=-ONE, keepdims=True))


def token_maps():
    s = iota((TOKEN_PAD, LANES), ZERO)
    lane = iota((TOKEN_PAD, LANES), ONE)
    j = ((lane - s) * INV49) & LOW7
    row = jnp.where(s < TOKENS, (j * TOKENS + s) >> SEVEN, -ONE)
    perm = (iota((LANES, LANES), ZERO) == ((iota((LANES, LANES), ONE) * TOKENS) & LOW7))
    return s, row, perm


def skew(x, s, left):
    for bit in range(SEVEN):
        amount = TWO ** bit
        x = jnp.where(((s >> bit) & ONE) == ONE, pltpu.roll(x, LANES - amount if left else amount, ONE), x)
    return x


def prep_layer(l, slab, vrow, bd, v2, ma1, mb1, ma2, mb2, col):
    for k in range(FOUR):
        lanes = slice(LANES * k, LANES * k + LANES)
        vrow[l, ZERO:ONE, lanes] = slab[l, SLAB_VEC + k:SLAB_VEC + k + ONE, :]
        vrow[l, ONE:TWO, lanes] = slab[l, SLAB_VEC + FOUR + k:SLAB_VEC + FIVE + k, :]
    lane = iota((IMAGES, LANES), ONE)
    cut = LANES - TOKENS
    v2[...] = jnp.where(lane < cut, pltpu.roll(slab[l, V_MIS:V_MIS + IMAGES, :], cut, ONE), pltpu.roll(slab[l, V_MIS + ONE:V_MIS + 33, :], cut, ONE))
    for row, first, count in ((TWO, ZERO, FOUR), (THREE, FOUR, FOUR), (FOUR, EIGHT, SIXTEEN), (FIVE, TWENTY_FOUR, FOUR)):
        for k in range(count):
            vrow[l, row:row + ONE, LANES * k:LANES * k + LANES] = v2[first + k:first + k + ONE, :]
    bd[...] = jnp.zeros_like(bd)
    for h in range(TWO):
        w = slab[l, pl.ds(h, TOKENS, stride=TWO), :]
        for i in range(FOUR):
            bd[TOKENS * i:TOKENS * i + TOKENS, TH * i + LANES * h:TH * i + LANES * h + LANES] = w
    mb1[l] = bd[ZERO:QROWS, :].astype(BF16)
    for h in range(TWO):
        for i in range(FOUR):
            bd[QVALID:QVALID + ONE, TH * i + LANES * h:TH * i + LANES * h + LANES] = slab[l, V_BT1 + h:V_BT1 + h + ONE, :]
    ma1[l] = bd[...].T[:, ZERO:QROWS].astype(BF16)
    bd[...] = jnp.zeros_like(bd)
    s, row, perm = token_maps()
    for h in range(TWO):
        def pick(r, acc):
            return jnp.where(row == r, slab[l, pl.ds(ROW_T2 + TOKENS * h + r, ONE), :], acc)
        x = skew(lax.fori_loop(ZERO, TOKENS, pick, jnp.zeros((TOKEN_PAD, LANES), F32)), s, True)
        w = mm(x.astype(BF16), perm.astype(BF16))[ZERO:TOKENS]
        for i in range(FOUR):
            bd[TOKENS * i:TOKENS * i + TOKENS, TH * i + LANES * h:TH * i + LANES * h + LANES] = w
    ma2[l] = bd[ZERO:QROWS, :].astype(BF16)
    mb2[l] = bd[...].T[:, ZERO:QROWS].astype(BF16)
    bias = jnp.where(iota((ONE, LANES), ONE) < TOKENS, slab[l, V_MIS:V_MIS + ONE, :], F_ZERO)
    wide = jnp.concatenate([jnp.broadcast_to(bias, (LANES, LANES)), jnp.zeros((LANES, LANES), F32)], axis=ONE)
    spread = wide
    for i in range(ONE, FOUR):
        spread = spread + pltpu.roll(wide, TOKENS * i, ONE)
    col[l] = spread.T[ZERO:QROWS, :]


def forward_layer(l, x_in, x_mid, x_out, vrow, ma1, ma2, col, w1, w2, uq, uch, hook):
    def quad(q, carry):
        hook(q)
        rows = pl.ds(aligned(q, QROWS), QROWS)
        xq = x_in[rows, :].astype(F32)
        n = token_input(xq, vrow, l)[TWO]
        for i in range(FOUR):
            uq[TH * i:TH * i + TH, :] = gelu(mm(ma1[l, TH * i:TH * i + TH, :], n))
        y = mm(ma2[l], uq[...])
        x1 = (xq + (y + jnp.concatenate([col[l]] * FOUR, axis=ONE))).astype(BF16)
        x_mid[rows, :] = x1
        x1 = x1.astype(F32)
        n2 = (stats(x1)[ZERO] * vrow[l, TWO:THREE, ZERO:CH] + vrow[l, THREE:FOUR, ZERO:CH]).astype(BF16)
        for c in range(FOUR):
            lanes = slice(CH * c, CH * c + CH)
            uch[:, lanes] = gelu(mm(n2, w1[l, :, lanes]) + vrow[l, FOUR:FIVE, lanes])
        x_out[rows, :] = (x1 + (mm(uch[...], w2[l]) + vrow[l, FIVE:SIX, ZERO:CH])).astype(BF16)
        return carry
    lax.fori_loop(ZERO, QUADS, quad, ZERO)


def token_input(xq, vrow, l):
    xh, scale = stats(xq)
    n = xh * vrow[l, ZERO:ONE, ZERO:CH] + vrow[l, ONE:TWO, ZERO:CH]
    return xh, scale, jnp.where(iota((QROWS, CH), ZERO) == QVALID, F_ONE, n).astype(BF16)


def image_of(shape, axis):
    c = iota(shape, axis)
    return jnp.where(c < QVALID, (c >= TOKENS).astype(jnp.int32) + (c >= TWO * TOKENS).astype(jnp.int32) + (c >= THREE * TOKENS).astype(jnp.int32), IMAGES)


def head_pass(x_out, labels, small, head, d, pool, srow, gsum, flat):
    for k in range(FOUR):
        lanes = slice(LANES * k, LANES * k + LANES)
        srow[ZERO:ONE, lanes] = small[k:k + ONE, :]
        srow[ONE:TWO, lanes] = small[FOUR + k:FIVE + k, :]
    for k in range(EIGHT):
        srow[TWO:THREE, LANES * k:LANES * k + LANES] = small[EIGHT + k:NINE + k, :]
    gain, shift = srow[ZERO:ONE, ZERO:CH], srow[ONE:TWO, ZERO:CH]
    pool[...] = jnp.zeros_like(pool)

    def quad(q, carry):
        xh, scale = stats(x_out[pl.ds(aligned(q, QROWS), QROWS), :].astype(F32))
        pick = (iota((IMAGES, QROWS), ZERO) == image_of((IMAGES, QROWS), ONE) + FOUR * q)
        pool[...] += mm(pick.astype(BF16), (xh * gain + shift).astype(BF16))
        return carry
    lax.fori_loop(ZERO, QUADS, quad, ZERO)
    pooled = (pool[...] / TOKENS).astype(BF16)
    real = iota((IMAGES, CLASS_PAD), ONE) < CLASSES
    logits = jnp.where(real, mm(pooled, head[...]) + srow[TWO:THREE, :], -1e30)
    top = jnp.max(logits, axis=-ONE, keepdims=True)
    log_norm = top + jnp.log(jnp.sum(jnp.exp(logits - top), axis=-ONE, keepdims=True))
    hit = iota((IMAGES, CLASS_PAD), ONE) == labels[:, ZERO:ONE]
    picked = jnp.sum(jnp.where(hit, logits, F_ZERO), axis=-ONE, keepdims=True)
    loss = jnp.broadcast_to(jnp.sum(log_norm - picked), (STEP8, LANES))
    d_logits = (jnp.exp(logits - log_norm) - hit.astype(F32)) / GLOBAL_IMAGES
    d_bf = d_logits.astype(BF16)
    g_head = mm(pool_t(pooled), d_bf)
    for n in range(SIXTEEN):
        for j in range(EIGHT):
            flat[HEAD_ROWS * n + IMAGES * j:HEAD_ROWS * n + IMAGES * j + IMAGES, :] = g_head[IMAGES * n:IMAGES * n + IMAGES, LANES * j:LANES * j + LANES]
        flat[HEAD_ROWS * n + TH:HEAD_ROWS * n + 264, :] = jnp.zeros((STEP8, LANES), F32)
        flat[HEAD_ROWS * n + 264:HEAD_ROWS * n + 272, :] = loss
    d_pool = (mm_nt(d_bf, head[...]) / TOKENS).astype(BF16)
    gsum[...] = jnp.zeros_like(gsum)

    def back(q, carry):
        rows = pl.ds(aligned(q, QROWS), QROWS)
        xh, scale = stats(x_out[rows, :].astype(F32))
        pick = (iota((QROWS, IMAGES), ONE) == image_of((QROWS, IMAGES), ZERO) + FOUR * q)
        dy = mm(pick.astype(BF16), d_pool)
        gsum[ZERO] += fold8(dy * xh)
        gsum[ONE] += fold8(dy)
        d[rows, :] = norm_back(xh, scale, gain, dy)
        return carry
    lax.fori_loop(ZERO, QUADS, back, ZERO)
    g_gain = jnp.sum(gsum[ZERO], axis=ZERO, keepdims=True)
    g_shift = jnp.sum(gsum[ONE], axis=ZERO, keepdims=True)
    g_bias = jnp.sum(d_logits, axis=ZERO, keepdims=True)
    for k in range(FOUR):
        lanes = slice(LANES * k, LANES * k + LANES)
        for row, value in ((HEAD_ROWS * k, g_gain), (HEAD_ROWS * (FOUR + k), g_shift)):
            flat[row + TH:row + 257, :] = value[:, lanes]
    for k in range(EIGHT):
        row = HEAD_ROWS * (EIGHT + k) + TH
        flat[row:row + ONE, :] = g_bias[:, LANES * k:LANES * k + LANES]


def pool_t(pooled):
    return pooled.astype(F32).T.astype(BF16)


def channel_back(l, x_mid, d, vrow, w1, w2, n2, dbf, n2t, dt, uh, dh, dn2, flat, gsum, gb1, hook):
    gsum[...] = jnp.zeros_like(gsum)
    gb1[...] = jnp.zeros_like(gb1)

    def quad(q, carry):
        rows = pl.ds(aligned(q, QROWS), QROWS)
        n2[rows, :] = (stats(x_mid[rows, :].astype(F32))[ZERO] * vrow[l, TWO:THREE, ZERO:CH] + vrow[l, THREE:FOUR, ZERO:CH]).astype(BF16)
        dq = d[rows, :]
        gsum[FOUR] += fold8(dq)
        dbf[rows, :] = dq.astype(BF16)
        dn2[rows, :] = jnp.zeros((QROWS, CH), F32)
        return carry
    lax.fori_loop(ZERO, QUADS, quad, ZERO)
    for k in range(ALL_ROWS // LANES):
        lanes = slice(LANES * k, LANES * k + LANES)
        n2t[:, lanes] = n2[lanes, :].T
        dt[:, lanes] = dbf[lanes, :].T
    hook(-ONE)

    def chunk(c, carry):
        hook(c)
        lanes = pl.ds(aligned(c, CHUNK), CHUNK)

        def block(b, inner):
            rows = pl.ds(aligned(b, BLOCK), BLOCK)
            u, slope = gelu_both(mm(n2[rows, :], w1[l, :, lanes]) + vrow[l, FOUR:FIVE, lanes])
            uh[rows, :] = u
            dhid = mm_nt(dbf[rows, :], w2[l, lanes, :]).astype(BF16).astype(F32) * slope
            gb1[:, lanes] += fold8(dhid)
            dhid = dhid.astype(BF16)
            dh[rows, :] = dhid
            dn2[rows, :] += mm_nt(dhid, w1[l, :, lanes])
            return inner
        lax.fori_loop(ZERO, ALL_ROWS // BLOCK, block, ZERO)
        g1 = mm(n2t[...], dh[...])
        for r in range(CH // STEP8):
            for k in range(TWO):
                flat[pl.ds(ROW_C1 + LANES * r + k + TWO * c, STEP8, stride=SIXTEEN), :] = g1[STEP8 * r:STEP8 * r + STEP8, LANES * k:LANES * k + LANES]
        g2 = mm(dt[...], uh[...]).T
        for r in range(CHUNK // STEP8):
            for k in range(FOUR):
                flat[pl.ds(ROW_C2 + FOUR * (STEP8 * r) + k + FOUR * CHUNK * c, STEP8, stride=FOUR), :] = g2[STEP8 * r:STEP8 * r + STEP8, LANES * k:LANES * k + LANES]
        return carry
    lax.fori_loop(ZERO, HID // CHUNK, chunk, ZERO)


def token_back(l, x_in, x_mid, d, vrow, dn2, ma1, mb1, ma2, mb2, uq, dq_ref, acc1, acc2, rowsum, colsum, gsum, hook):
    for ref in (acc1, acc2, rowsum, colsum):
        ref[...] = jnp.zeros_like(ref)

    def quad(q, carry):
        hook(q)
        rows = pl.ds(aligned(q, QROWS), QROWS)
        xh, scale = stats(x_mid[rows, :].astype(F32))
        dy = dn2[rows, :].astype(BF16).astype(F32)
        gsum[TWO] += fold8(dy * xh)
        gsum[THREE] += fold8(dy)
        d_after = norm_back(xh, scale, vrow[l, TWO:THREE, ZERO:CH], dy) + d[rows, :]
        part = d_after[:, ZERO:LANES]
        for k in range(ONE, FOUR):
            part = part + d_after[:, LANES * k:LANES * k + LANES]
        colsum[ZERO:QROWS, :] += part
        d_bf = d_after.astype(BF16)
        xh, scale, n = token_input(x_in[rows, :].astype(F32), vrow, l)
        for i in range(FOUR):
            part = slice(TH * i, TH * i + TH)
            u, slope = gelu_both(mm(ma1[l, part, :], n))
            uq[part, :] = u
            dhid = mm(mb2[l, part, :], d_bf).astype(BF16).astype(F32) * slope
            total = dhid[:, ZERO:LANES]
            for k in range(ONE, FOUR):
                total = total + dhid[:, LANES * k:LANES * k + LANES]
            rowsum[part, :] += total
            dq_ref[part, :] = dhid.astype(BF16)
        acc1[...] += mm_nt(n, dq_ref[...])
        acc2[...] += mm_nt(d_bf, uq[...])
        dy = mm(mb1[l], dq_ref[...]).astype(BF16).astype(F32)
        gsum[ZERO] += fold8(dy * xh)
        gsum[ONE] += fold8(dy)
        d[rows, :] = norm_back(xh, scale, vrow[l, ZERO:ONE, ZERO:CH], dy) + d_after
        return carry
    lax.fori_loop(ZERO, QUADS, quad, ZERO)


def small_flat(l, flat, acc1, acc2, rowsum, colsum, gsum, gb1, v2):
    g = sum_images(acc1)
    for h in range(TWO):
        flat[pl.ds(h, TOKENS, stride=TWO), :] = g[:, LANES * h:LANES * h + LANES]
    g = sum_images(acc2)
    s, row, perm = token_maps()
    for h in range(TWO):
        padded = jnp.concatenate([g[:, LANES * h:LANES * h + LANES], jnp.zeros((SEVEN, LANES), F32)], axis=ZERO)
        x = skew(lax.dot_general(padded, perm.astype(F32), (((ONE,), (ONE,)), ((), ())), precision=lax.Precision.HIGHEST, preferred_element_type=F32), s, False)

        def place_row(r, carry):
            flat[pl.ds(ROW_T2 + TOKENS * h + r, ONE), :] = jnp.sum(jnp.where(row == r, x, F_ZERO), axis=ZERO, keepdims=True)
            return carry
        lax.fori_loop(ZERO, TOKENS, place_row, ZERO)
    flat[ROW_VEC:FLAT_ROWS + SIXTEEN, :] = jnp.zeros((FLAT_ROWS + SIXTEEN - ROW_VEC, LANES), F32)
    for n in range(TWO):
        v = jnp.sum(gsum[n], axis=ZERO, keepdims=True)
        for k in range(FOUR):
            flat[ROW_VEC + FOUR * n + k:ROW_VEC + FOUR * n + k + ONE, :] = v[:, LANES * k:LANES * k + LANES]
    t = jnp.sum(rowsum[...].T, axis=ZERO, keepdims=True)
    t = t[:, ZERO:TH] + t[:, TH:TWO * TH] + t[:, TWO * TH:THREE * TH] + t[:, THREE * TH:FOUR * TH]
    for h in range(TWO):
        flat[ROW_VEC + EIGHT + h:ROW_VEC + NINE + h, :] = t[:, LANES * h:LANES * h + LANES]
    v2[...] = jnp.zeros_like(v2)
    lists = [(jnp.sum(gsum[TWO], axis=ZERO, keepdims=True), ZERO, FOUR), (jnp.sum(gsum[THREE], axis=ZERO, keepdims=True), FOUR, FOUR), (jnp.sum(gb1[...], axis=ZERO, keepdims=True), EIGHT, SIXTEEN), (jnp.sum(gsum[FOUR], axis=ZERO, keepdims=True), TWENTY_FOUR, FOUR)]
    for v, first, count in lists:
        for k in range(count):
            v2[first + k:first + k + ONE, :] = v[:, LANES * k:LANES * k + LANES]
    turned = pltpu.roll(v2[...], TOKENS, ONE)
    t = jnp.broadcast_to(jnp.sum(colsum[...].T, axis=ZERO, keepdims=True), (STEP8, TWO * LANES))
    b2 = t
    for i in range(ONE, FOUR):
        b2 = b2 + pltpu.roll(t, TWO * LANES - TOKENS * i, ONE)
    before = jnp.concatenate([b2[ZERO:ONE, ZERO:LANES], turned[ZERO:LAST_IMAGE, :]], axis=ZERO)
    merged = jnp.where(iota((IMAGES, LANES), ONE) < TOKENS, before, turned)
    flat[ROW_VEC + TEN:ROW_VEC + 42, :] = merged


def sum_images(acc):
    g = acc[ZERO:TOKENS, ZERO:TH]
    for i in range(ONE, FOUR):
        g = g + acc[TOKENS * i:TOKENS * i + TOKENS, TH * i:TH * i + TH]
    return g


def no_hook(k):
    return None


def at(table):
    def hook(k):
        for key, act in table.items():
            if isinstance(k, int):
                if key == k:
                    act()
            elif key >= ZERO:
                pl.when(k == key)(act)
    return hook


def both(*acts):
    def run():
        for act in acts:
            act()
    return run


def step_kernel(x0, labels, pack, own, stat, gath, x1, x2, x3, d, dn2, n2, dbf, n2t, dt, mix, uch, ma1, mb1, ma2, mb2, col, vrow, v2, bd, srow, pool, gsum, gb1, acc2, rowsum, colsum, flat, w1, w2, slab, head, small, stage, leaving, t0, t1, t2, t3, msg, box, ag_send, ag_recv, rs_send, rs_recv, stage_sem, load_sem, tiny_send, tiny_recv, done):
    where = place()
    me, coords, core, neighbours, partner = where
    load = pltpu.make_async_copy(pack, gath.at[coords[ZERO], coords[ONE], coords[TWO], core], load_sem)
    load.start()
    enter_barrier(neighbours, partner)
    load.wait()
    first = Gather(gath, where, ((ZERO, 352), (352, 352), (704, 336)), ag_send, ag_recv, ZERO)
    rest = Gather(gath, where, ((1040, 448), (1488, 432), (1920, 432)), ag_send, ag_recv, 21)
    first.start()
    for phase in range(THREE):
        first.step(phase)
    rest.start()
    first.finish()
    mats = (ma1, mb1, ma2, mb2, col)
    unflatten_layer(gath, ZERO, flat, stage, stage_sem, w1, w2, slab)
    prep_layer(ZERO, slab, vrow, bd, v2, *mats)
    uq, dq = mix.at[ZERO:FOUR * TH, :], mix.at[FOUR * TH:EIGHT * TH, :]
    uh, dh = mix.at[ZERO:ALL_ROWS, ZERO:CHUNK], mix.at[ZERO:ALL_ROWS, CHUNK:TWO * CHUNK]
    acc1 = bd.at[ZERO:QROWS, :]
    forward_layer(ZERO, x0, x1, x2, vrow, ma1, ma2, col, w1, w2, uq, uch, at({ONE: lambda: rest.step(ZERO), THREE: lambda: rest.step(ONE), SEVEN: lambda: rest.step(TWO)}))
    rest.finish()
    unflatten_layer(gath, ONE, flat, stage, stage_sem, w1, w2, slab)
    unflatten_head(gath, stage, stage_sem, head, small)
    prep_layer(ONE, slab, vrow, bd, v2, *mats)
    forward_layer(ONE, x2, x3, n2, vrow, ma1, ma2, col, w1, w2, uq, uch, no_hook)
    head_pass(n2, labels, small, head, d, pool, srow, gsum, flat)

    bufs, sems = (leaving, t0, t1, t2, t3), (rs_send, rs_recv)
    thirds = ((ZERO, 352), (352, 352), (704, 336))
    reduces = [Reduce(flat, HEAD_ROWS, HEAD_ROWS, ((ZERO, 96), (96, 88), (184, 88)), own, HEAD_OFF, bufs, where, sems)]
    reduces += [Reduce(flat, SHARD_ROWS, SLOT_ROWS, thirds, own, l * SLOT_ROWS, bufs, where, sems) for l in (ONE, ZERO)]

    def done_one(work):
        def run():
            work.finish()
            for other in list(neighbours) + [partner]:
                pl.semaphore_signal(done, inc=ONE, device_id=(other,), device_id_type=MESH_ID)
        return run

    def go(work, phase):
        return lambda: work.step(phase)

    h, r1, r0 = reduces
    plans = [
        (ONE, x2, x3, {-ONE: go(h, ZERO), ONE: go(h, ONE), TWO: go(h, TWO), FOUR: both(go(h, THREE), done_one(h))}, {}, r1),
        (ZERO, x0, x1, {-ONE: go(r1, ZERO), FOUR: go(r1, ONE), SEVEN: go(r1, TWO)}, {TWO: both(go(r1, THREE), done_one(r1))}, r0),
    ]
    h.start()
    for l, x_in, x_mid, channel_plan, token_plan, after in plans:
        channel_back(l, x_mid, d, vrow, w1, w2, n2, dbf, n2t, dt, uh, dh, dn2, flat, gsum, gb1, at(channel_plan))
        token_back(l, x_in, x_mid, d, vrow, dn2, ma1, mb1, ma2, mb2, uq, dq, acc1, acc2, rowsum, colsum, gsum, at(token_plan))
        small_flat(l, flat, acc1, acc2, rowsum, colsum, gsum, gb1, v2)
        pl.semaphore_wait(done, FOUR)
        after.start()
    for phase in range(FOUR):
        r0.step(phase)
    r0.finish()
    for l in range(TWO):
        own[l * SLOT_ROWS + SHARD_ROWS:l * SLOT_ROWS + SLOT_ROWS, :] = jnp.zeros((ONE, LANES), F32)
    msg[ZERO] = jnp.broadcast_to(jnp.sum(square_sum(own, ZERO, SMALL_OFF + EIGHT)), (STEP8, LANES))
    for n, device in enumerate([partner, neighbours[TWO], neighbours[ONE], neighbours[ZERO]]):
        copy = pltpu.make_async_remote_copy(src_ref=msg.at[n], dst_ref=box.at[n], send_sem=tiny_send.at[n], recv_sem=tiny_recv.at[n], device_id=(device,), device_id_type=MESH_ID)
        copy.start()
        copy.wait()
        msg[n + ONE] = msg[n] + box[n]
    stat[ZERO] = msg[FOUR]
    stat[ONE] = own[SMALL_OFF + EIGHT:SMALL_OFF + SIXTEEN, :]


def train_step(x0, labels, pack):
    vmem = pl.BlockSpec(memory_space=pltpu.VMEM)
    act = pltpu.VMEM((ALL_ROWS, CH), BF16)
    wide = pltpu.VMEM((ALL_ROWS, CH), F32)
    across = pltpu.VMEM((CH, ALL_ROWS), BF16)
    tall = pltpu.VMEM((TWO, FOUR * TH, QROWS), BF16)
    flat_mat = pltpu.VMEM((TWO, QROWS, FOUR * TH), BF16)
    acc = pltpu.VMEM((QROWS, FOUR * TH), F32)
    dma = pltpu.SemaphoreType.DMA
    return pl.pallas_call(
        step_kernel,
        out_shape=(jax.ShapeDtypeStruct((AG_ROWS, LANES), F32), jax.ShapeDtypeStruct((TWO, STEP8, LANES), F32), jax.ShapeDtypeStruct((TWO, TWO, TWO, TWO, AG_ROWS, LANES), BF16)),
        in_specs=[vmem] * THREE,
        out_specs=(vmem, vmem, pl.BlockSpec(memory_space=pl.ANY)),
        scratch_shapes=[act, act, act, wide, wide, act, act, across, across, pltpu.VMEM((EIGHT * TH, CH), BF16), pltpu.VMEM((QROWS, HID), BF16),
                        tall, flat_mat, flat_mat, tall, pltpu.VMEM((TWO, QROWS, LANES), F32), pltpu.VMEM((TWO, STEP8, HID), F32), pltpu.VMEM((IMAGES, LANES), F32), pltpu.VMEM((TWO * LANES, FOUR * TH), F32),
                        pltpu.VMEM((STEP8, CLASS_PAD), F32), pltpu.VMEM((IMAGES, CH), F32), pltpu.VMEM((FIVE, STEP8, CH), F32), pltpu.VMEM((STEP8, HID), F32), acc,
                        pltpu.VMEM((FOUR * TH, LANES), F32), pltpu.VMEM((TWO * LANES, LANES), F32), pltpu.VMEM((FLAT_ROWS + SIXTEEN, LANES), F32),
                        pltpu.VMEM((TWO, CH, HID), BF16), pltpu.VMEM((TWO, HID, CH), BF16), pltpu.VMEM((TWO, SLAB_ROWS, LANES), F32), pltpu.VMEM((CH, CLASS_PAD), BF16), pltpu.VMEM((SIXTEEN, LANES), F32),
                        pltpu.VMEM((TWO, SLOT_ROWS, LANES), BF16), pltpu.VMEM((TWO, TWO, TWO, SLOT_ROWS, LANES), F32), pltpu.VMEM((TWO, TWO, TWO, SLOT_ROWS, LANES), F32), pltpu.VMEM((TWO, TWO, SLOT_ROWS, LANES), F32), pltpu.VMEM((TWO, SLOT_ROWS, LANES), F32), pltpu.VMEM((SLOT_ROWS, LANES), F32),
                        pltpu.VMEM((FIVE, STEP8, LANES), F32), pltpu.VMEM((FOUR, STEP8, LANES), F32),
                        dma((42,)), dma((42,)), dma((12,)), dma((12,)), dma((TWO,)), dma, dma((FOUR,)), dma((FOUR,)), pltpu.SemaphoreType.REGULAR],
        compiler_params=pltpu.CompilerParams(collective_id=ZERO, has_side_effects=True, vmem_limit_bytes=67043328),
        name='train_step',
    )(x0, labels, pack)


LEARN_RATE = 0.003
BETA_ONE = 0.9
BETA_TWO = 0.999
ADAM_EPS = 1e-8
WEIGHT_DECAY = 0.03
ADAM_STEP = 10


def adam_update(master, gradient, moment, second, decay_rate):
    moment_new = BETA_ONE * moment + (F_ONE - BETA_ONE) * gradient
    second_new = BETA_TWO * second + (F_ONE - BETA_TWO) * gradient * gradient
    m_hat = moment_new / (F_ONE - BETA_ONE ** ADAM_STEP)
    v_hat = second_new / (F_ONE - BETA_TWO ** ADAM_STEP)
    master_new = master - LEARN_RATE * (m_hat / (jnp.sqrt(v_hat) + ADAM_EPS) + decay_rate * master)
    return master_new, moment_new, second_new


def solution(mesh):
    row_spec = P('fsdp')
    layer_spec = P(None, 'fsdp')
    in_specs = (row_spec, row_spec, layer_spec, row_spec, row_spec, layer_spec, row_spec, row_spec, layer_spec, row_spec, row_spec)
    out_specs = (P(),) + in_specs[TWO:]

    def device_step(act_in, labels, layer_p, head_w, small_p, layer_m, head_m, small_m, layer_v, head_v, small_v):
        mat_len = ROW_VEC * LANES
        quads = jnp.pad(act_in.reshape(QUADS, QVALID, CH), ((ZERO, ZERO), (ZERO, QROWS - QVALID), (ZERO, ZERO))).reshape(ALL_ROWS, CH)
        layer_bf = jnp.pad(layer_p.astype(BF16).reshape(TWO, SHARD_ROWS, LANES), ((ZERO, ZERO), (ZERO, ONE), (ZERO, ZERO)))
        head_bf = jnp.pad(head_w.astype(BF16), ((ZERO, ZERO), (ZERO, CLASS_PAD - CLASSES))).reshape(IMAGES, EIGHT, LANES).transpose(ONE, ZERO, TWO).reshape(TH, LANES)
        small_bf = jnp.pad(small_p.astype(BF16).reshape(ONE, LANES), ((ZERO, 15), (ZERO, ZERO)))
        pack = jnp.concatenate([layer_bf.reshape(TWO * SLOT_ROWS, LANES), head_bf, small_bf])
        own, stat, _ = train_step(quads, jnp.broadcast_to(labels[:, None], (IMAGES, LANES)), pack)
        layer_g = own[:HEAD_OFF].reshape(TWO, SLOT_ROWS, LANES)[:, :SHARD_ROWS].reshape(TWO, SHARD_ROWS * LANES)
        head_g = own[HEAD_OFF:SMALL_OFF].reshape(EIGHT, IMAGES, LANES).transpose(ONE, ZERO, TWO).reshape(IMAGES, CLASS_PAD)[:, :CLASSES]
        small_g = own[SMALL_OFF]
        loss_value = stat[ONE, ZERO, ZERO] / GLOBAL_IMAGES
        clip_scale = F_ONE / jnp.maximum(F_ONE, jnp.sqrt(stat[ZERO, ZERO, ZERO]))
        shard_len = layer_p.shape[ONE]
        flat_pos = lax.axis_index('fsdp') * shard_len + jnp.arange(shard_len)
        layer_decay = jnp.where(flat_pos < mat_len, WEIGHT_DECAY, F_ZERO)[None, :]
        new_lp, new_lm, new_lv = adam_update(layer_p, layer_g * clip_scale, layer_m, layer_v, layer_decay)
        new_hw, new_hm, new_hv = adam_update(head_w, head_g * clip_scale, head_m, head_v, WEIGHT_DECAY)
        new_sp, new_sm, new_sv = adam_update(small_p, small_g * clip_scale, small_m, small_v, F_ZERO)
        return (loss_value, new_lp, new_hw, new_sp, new_lm, new_hm, new_sm, new_lv, new_hv, new_sv)

    return jax.shard_map(device_step, mesh=mesh, in_specs=in_specs, out_specs=out_specs, check_vma=False)
```

```python
import functools
import math
import jax
import jax.numpy as jnp
from jax import lax
from jax.experimental import pallas as pl
from jax.experimental.pallas import tpu as pltpu
from jax.sharding import PartitionSpec as P

ZERO = 0
ONE = 1
TWO = 2
THREE = 3
FOUR = 4
FIVE = 5
SIX = 6
SEVEN = 7
EIGHT = 8
NINE = 9
SIXTEEN = 16
LANES = 128
IMAGES = 32
LAST_IMAGE = 31
CH = 512
CLASS_PAD = 1024
HID = 2048
TH = 256
F_ZERO = 0.0
F_ONE = 1.0
TWENTY_FOUR = 24
TOKEN_PAD = 56
QVALID = 196
SIXTY_FOUR = 64
TEN = 10
MESH_ID = pl.DeviceIdType.MESH
F32 = jnp.float32
BF16 = jnp.bfloat16

SHARD_ROWS = 1039
SLOT_ROWS = 1040
ROW_C1 = 196
ROW_C2 = 8388
ROW_VEC = 16580
FLAT_ROWS = 16624
SLAB_ROWS = 240
HEAD_OFF = 2 * SLOT_ROWS
SMALL_OFF = HEAD_OFF + 256
AG_ROWS = SMALL_OFF + 16
HEAD_ROWS = 272
ORDERS = ((2, 1, 0), (1, 0, 2), (0, 2, 1))
AXIS_STEP = (8, 4, 2)


def place():
    me = lax.axis_index('fsdp')
    coords = [me // EIGHT, (me // FOUR) % TWO, (me // TWO) % TWO]
    core = me % TWO
    neighbours = [me + AXIS_STEP[a] - TWO * AXIS_STEP[a] * coords[a] for a in range(THREE)]
    partner = me + ONE - TWO * core
    return me, coords, core, neighbours, partner


def enter_barrier(neighbours, partner):
    barrier = pltpu.get_barrier_semaphore()
    for other in list(neighbours) + [partner]:
        pl.semaphore_signal(barrier, inc=ONE, device_id=(other,), device_id_type=MESH_ID)
    pl.semaphore_wait(barrier, FOUR)


def slot_view(buf, coords, core, free_axes, row0, rows):
    index = [pl.ds(ZERO, TWO) if a in free_axes else coords[a] for a in range(THREE)]
    return buf.at[index[ZERO], index[ONE], index[TWO], core, pl.ds(row0, rows), :]


class Gather:
    def __init__(self, buf, where, row_groups, send_sem, recv_sem, sem0):
        self.buf, self.where, self.groups = buf, where, row_groups
        self.send_sem, self.recv_sem, self.sem0 = send_sem, recv_sem, sem0
        self.pending = []

    def copy(self, view, sem, device):
        return pltpu.make_async_remote_copy(src_ref=view, dst_ref=view, send_sem=self.send_sem.at[self.sem0 + sem], recv_sem=self.recv_sem.at[self.sem0 + sem], device_id=(device,), device_id_type=MESH_ID)

    def link(self, group, phase):
        me, coords, core, neighbours, partner = self.where
        order = ORDERS[group]
        row0, rows = self.groups[group]
        view = slot_view(self.buf, coords, core, order[:phase], row0, rows)
        return self.copy(view, group * THREE + phase, neighbours[order[phase]])

    def chip(self, group, phase):
        me, coords, core, neighbours, partner = self.where
        order = ORDERS[group]
        row0, rows = self.groups[group]
        if phase < ZERO:
            view = slot_view(self.buf, coords, core, (), row0, rows)
        else:
            far = list(coords)
            far[order[phase]] = ONE - coords[order[phase]]
            view = slot_view(self.buf, far, core, order[:phase], row0, rows)
        return self.copy(view, NINE + group * FOUR + phase + ONE, partner)

    def start(self):
        for group in range(THREE):
            self.link(group, ZERO).start()
        for group in range(THREE):
            self.chip(group, -ONE).start()

    def step(self, phase):
        for group in range(THREE):
            self.link(group, phase).wait_recv()
            if phase < TWO:
                self.link(group, phase + ONE).start()
            self.chip(group, phase).start()

    def finish(self):
        for group in range(THREE):
            for phase in range(-ONE, THREE):
                self.chip(group, phase).wait()
            for phase in range(THREE):
                self.link(group, phase).wait_send()


def slot_of(dev):
    return dev // EIGHT, (dev // FOUR) % TWO, (dev // TWO) % TWO, dev % TWO


def fetch_layer(gath, layer, bays, stage_sem):
    copies = []
    for dev in range(SIXTEEN):
        z, y, x, core = slot_of(dev)
        land = bays[dev // FOUR].at[pl.ds(ZERO, SLOT_ROWS), pl.ds(LANES * (dev % FOUR), LANES)]
        copies.append(pltpu.make_async_copy(gath.at[z, y, x, core, pl.ds(layer * SLOT_ROWS, SLOT_ROWS), :], land, stage_sem.at[dev]))
    for copy in copies:
        copy.start()
    return copies


def unflatten_layer(gath, layer, flat, bays, stage_sem, w1_ref, w2_ref, slab_ref):
    copies = fetch_layer(gath, layer, bays, stage_sem)
    for dev in range(SIXTEEN):
        copies[dev].wait()

        def chunk(k, inner):
            block = bays[dev // FOUR][pl.ds(pl.multiple_of(SIXTEEN * k, SIXTEEN), SIXTEEN), LANES * (dev % FOUR):LANES * (dev % FOUR) + LANES]
            flat[pl.ds(dev * SHARD_ROWS + SIXTEEN * k, SIXTEEN), :] = block.astype(F32)
            return inner
        lax.fori_loop(ZERO, SLOT_ROWS // SIXTEEN, chunk, ZERO, unroll=FIVE)

    def first(rb, carry):
        for j in range(SIXTEEN):
            block = flat[pl.ds(ROW_C1 + TH * rb + j, SIXTEEN, stride=SIXTEEN), :]
            w1_ref[layer, pl.ds(pl.multiple_of(SIXTEEN * rb, SIXTEEN), SIXTEEN), LANES * j:LANES * j + LANES] = block.astype(BF16)
        return carry
    lax.fori_loop(ZERO, IMAGES, first, ZERO)

    def second(rb, carry):
        for j in range(FOUR):
            block = flat[pl.ds(ROW_C2 + SIXTY_FOUR * rb + j, SIXTEEN, stride=FOUR), :]
            w2_ref[layer, pl.ds(pl.multiple_of(SIXTEEN * rb, SIXTEEN), SIXTEEN), LANES * j:LANES * j + LANES] = block.astype(BF16)
        return carry
    lax.fori_loop(ZERO, LANES, second, ZERO, unroll=FOUR)
    slab_ref[layer, ZERO:QVALID, :] = flat[ZERO:QVALID, :]
    slab_ref[layer, QVALID:240, :] = flat[ROW_VEC:FLAT_ROWS, :]


def unflatten_head(gath, bays, stage_sem, head_ref, small_ref):
    copies = []
    for dev in range(SIXTEEN):
        z, y, x, core = slot_of(dev)
        copies.append(pltpu.make_async_copy(gath.at[z, y, x, core, pl.ds(HEAD_OFF, HEAD_ROWS), :], bays[dev // FOUR].at[pl.ds(ZERO, HEAD_ROWS), pl.ds(LANES * (dev % FOUR), LANES)], stage_sem.at[dev]))
    for copy in copies:
        copy.start()
    for dev in range(SIXTEEN):
        copies[dev].wait()
        lanes = slice(LANES * (dev % FOUR), LANES * (dev % FOUR) + LANES)
        for j in range(EIGHT):
            head_ref[IMAGES * dev:IMAGES * dev + IMAGES, LANES * j:LANES * j + LANES] = bays[dev // FOUR][IMAGES * j:IMAGES * j + IMAGES, lanes]
        small_ref[dev:dev + ONE, :] = bays[dev // FOUR][TH:272, lanes].astype(F32)[ZERO:ONE, :]


class Reduce:
    def __init__(self, flat, pitch, rows, groups, out, out_row, bufs, where, sems):
        self.flat, self.pitch, self.rows, self.groups, self.out, self.out_row = flat, pitch, rows, groups, out, out_row
        self.leaving, self.temps = bufs[ZERO], bufs[ONE:]
        self.where = where
        self.send_sem, self.recv_sem = sems

    def spread(self):
        me, coords, core, neighbours, partner = self.where

        def chunk(k, carry):
            for n in range(EIGHT):
                self.leaving[n // FOUR, (n // TWO) % TWO, n % TWO, pl.ds(pl.multiple_of(EIGHT * k, EIGHT), EIGHT), :] = self.flat[pl.ds(self.pitch * (TWO * n + ONE - core) + EIGHT * k, EIGHT), :]
            return carry
        lax.fori_loop(ZERO, self.rows // EIGHT, chunk, ZERO)

    def views(self, group, phase):
        me, coords, core, neighbours, partner = self.where
        row0, rows = self.groups[group]
        order = ORDERS[group]
        if phase == ZERO:
            free = (ZERO, ONE, TWO)
            leave = self.leaving.at[:, :, :, pl.ds(row0, rows), :]
            device = partner
        else:
            axis = order[phase - ONE]
            free = tuple(a for a in range(THREE) if a in order[phase:])
            index = [pl.ds(ZERO, TWO) if a in free else coords[a] for a in range(THREE)]
            index[axis] = ONE - coords[axis]
            leave = self.temps[ZERO].at[index[ZERO], index[ONE], index[TWO], pl.ds(row0, rows), :]
            device = neighbours[axis]
        land = self.temps[phase].at[(slice(None),) * len(free) + (pl.ds(row0, rows), slice(None))]
        return leave, land, device, free

    def copy(self, group, phase):
        leave, land, device, free = self.views(group, phase)
        sem = group * FOUR + phase
        return pltpu.make_async_remote_copy(src_ref=leave, dst_ref=land, send_sem=self.send_sem.at[sem], recv_sem=self.recv_sem.at[sem], device_id=(device,), device_id_type=MESH_ID)

    def add(self, group, phase):
        me, coords, core, neighbours, partner = self.where
        free = self.views(group, phase)[THREE]
        row0, rows = self.groups[group]
        total, temp = self.temps[ZERO], self.temps[phase]
        count = TWO ** len(free)
        per = max(ONE, EIGHT // count)
        while rows % (EIGHT * per):
            per //= TWO

        def chunk(k, carry):
            for part in range(per):
                start = pl.multiple_of(row0 + EIGHT * (per * k + part), EIGHT)
                for n in range(count):
                    index = list(coords)
                    bits = []
                    for pos, a in enumerate(free):
                        bit = (n // TWO ** (len(free) - ONE - pos)) % TWO
                        index[a] = bit
                        bits.append(bit)
                    target = (index[ZERO], index[ONE], index[TWO], pl.ds(start, EIGHT), slice(None))
                    if phase == ZERO:
                        value = total[target] + self.flat[pl.ds(self.pitch * (TWO * n + core) + start, EIGHT), :]
                    else:
                        value = total[target] + temp[tuple(bits) + (pl.ds(start, EIGHT), slice(None))]
                    if phase == THREE:
                        self.out[pl.ds(pl.multiple_of(self.out_row + start, EIGHT), EIGHT), :] = value
                    else:
                        total[target] = value
            return carry
        lax.fori_loop(ZERO, rows // (EIGHT * per), chunk, ZERO)

    def start(self):
        self.spread()
        for group in range(THREE):
            self.copy(group, ZERO).start()

    def step(self, phase):
        for group in range(THREE):
            self.copy(group, phase).wait_recv()
            self.add(group, phase)
            if phase < THREE:
                self.copy(group, phase + ONE).start()

    def finish(self):
        for group in range(THREE):
            for phase in range(FOUR):
                self.copy(group, phase).wait_send()


def square_sum(ref, row0, rows):
    def chunk(k, total):
        block = ref[pl.ds(pl.multiple_of(row0 + EIGHT * k, EIGHT), EIGHT), :]
        return total + block * block
    return lax.fori_loop(ZERO, rows // EIGHT, chunk, jnp.zeros((EIGHT, LANES), F32), unroll=TWO)


QUADS = 8
QROWS = 208
TOKENS = 49
ALL_ROWS = QUADS * QROWS
CHUNK = 256
BLOCK = 416
CLASSES = 1000
GLOBAL_IMAGES = 512.0
LN_EPS = 1e-6
GELU_A = 0.7978845608028654
GELU_B = GELU_A * 0.044715
HALF = 0.5
ROW_T2 = 98
INV49 = 81
LOW7 = 127
SLAB_VEC = 196
V_BT1 = 204
V_MIS = 206
STEP8 = 8


def mm(a, b):
    return jnp.dot(a, b, preferred_element_type=F32)


def mm_nt(a, b):
    return lax.dot_general(a, b, (((ONE,), (ONE,)), ((), ())), preferred_element_type=F32)


def iota(shape, axis):
    return lax.broadcasted_iota(jnp.int32, shape, axis)


def aligned(start, unit):
    return pl.multiple_of(start * unit, unit)


def stats(x):
    mean = jnp.mean(x, axis=-ONE, keepdims=True)
    centered = x - mean
    scale = lax.rsqrt(jnp.mean(centered * centered, axis=-ONE, keepdims=True) + LN_EPS)
    return centered * scale, scale


def fold8(x):
    return jnp.sum(x.reshape(x.shape[ZERO] // STEP8, STEP8, x.shape[ONE]), axis=ZERO)


def gelu_tanh(h):
    sq = h * h
    return sq, jnp.tanh(h * (GELU_A + GELU_B * sq))


def gelu(h):
    sq, t = gelu_tanh(h)
    half = HALF * h
    return (half + half * t).astype(BF16)


def gelu_both(h):
    sq, t = gelu_tanh(h)
    side = HALF + HALF * t
    u = h * side
    return u.astype(BF16), side + (u - u * t) * (GELU_A + (3.0 * GELU_B) * sq)


def norm_back(xh, scale, gain, dy):
    dxh = dy * gain
    return scale * (dxh - jnp.mean(dxh, axis=-ONE, keepdims=True) - xh * jnp.mean(dxh * xh, axis=-ONE, keepdims=True))


def token_maps():
    s = iota((TOKEN_PAD, LANES), ZERO)
    lane = iota((TOKEN_PAD, LANES), ONE)
    j = ((lane - s) * INV49) & LOW7
    row = jnp.where(s < TOKENS, (j * TOKENS + s) >> SEVEN, -ONE)
    perm = (iota((LANES, LANES), ZERO) == ((iota((LANES, LANES), ONE) * TOKENS) & LOW7))
    return s, row, perm


def skew(x, s, left):
    for bit in range(SEVEN):
        amount = TWO ** bit
        x = jnp.where(((s >> bit) & ONE) == ONE, pltpu.roll(x, LANES - amount if left else amount, ONE), x)
    return x


def prep_layer(l, slab, vrow, bd, v2, ma1, mb1, ma2, mb2, col):
    for k in range(FOUR):
        lanes = slice(LANES * k, LANES * k + LANES)
        vrow[l, ZERO:ONE, lanes] = slab[l, SLAB_VEC + k:SLAB_VEC + k + ONE, :]
        vrow[l, ONE:TWO, lanes] = slab[l, SLAB_VEC + FOUR + k:SLAB_VEC + FIVE + k, :]
    lane = iota((IMAGES, LANES), ONE)
    cut = LANES - TOKENS
    v2[...] = jnp.where(lane < cut, pltpu.roll(slab[l, V_MIS:V_MIS + IMAGES, :], cut, ONE), pltpu.roll(slab[l, V_MIS + ONE:V_MIS + 33, :], cut, ONE))
    for row, first, count in ((TWO, ZERO, FOUR), (THREE, FOUR, FOUR), (FOUR, EIGHT, SIXTEEN), (FIVE, TWENTY_FOUR, FOUR)):
        for k in range(count):
            vrow[l, row:row + ONE, LANES * k:LANES * k + LANES] = v2[first + k:first + k + ONE, :]
    bd[...] = jnp.zeros_like(bd)
    for h in range(TWO):
        w = slab[l, pl.ds(h, TOKENS, stride=TWO), :]
        for i in range(FOUR):
            bd[TOKENS * i:TOKENS * i + TOKENS, TH * i + LANES * h:TH * i + LANES * h + LANES] = w
    mb1[l] = bd[ZERO:QROWS, :].astype(BF16)
    for h in range(TWO):
        for i in range(FOUR):
            bd[QVALID:QVALID + ONE, TH * i + LANES * h:TH * i + LANES * h + LANES] = slab[l, V_BT1 + h:V_BT1 + h + ONE, :]
    ma1[l] = bd[...].T[:, ZERO:QROWS].astype(BF16)
    bd[...] = jnp.zeros_like(bd)
    s, row, perm = token_maps()
    for h in range(TWO):
        def pick(r, acc):
            return jnp.where(row == r, slab[l, pl.ds(ROW_T2 + TOKENS * h + r, ONE), :], acc)
        x = skew(lax.fori_loop(ZERO, TOKENS, pick, jnp.zeros((TOKEN_PAD, LANES), F32)), s, True)
        w = mm(x.astype(BF16), perm.astype(BF16))[ZERO:TOKENS]
        for i in range(FOUR):
            bd[TOKENS * i:TOKENS * i + TOKENS, TH * i + LANES * h:TH * i + LANES * h + LANES] = w
    ma2[l] = bd[ZERO:QROWS, :].astype(BF16)
    mb2[l] = bd[...].T[:, ZERO:QROWS].astype(BF16)
    bias = jnp.where(iota((ONE, LANES), ONE) < TOKENS, slab[l, V_MIS:V_MIS + ONE, :], F_ZERO)
    wide = jnp.concatenate([jnp.broadcast_to(bias, (LANES, LANES)), jnp.zeros((LANES, LANES), F32)], axis=ONE)
    spread = wide
    for i in range(ONE, FOUR):
        spread = spread + pltpu.roll(wide, TOKENS * i, ONE)
    col[l] = spread.T[ZERO:QROWS, :]


def forward_layer(l, x_in, x_mid, x_out, vrow, ma1, ma2, col, w1, w2, uq, uch, hook):
    def quad(q, carry):
        hook(q)
        rows = pl.ds(aligned(q, QROWS), QROWS)
        xq = x_in[rows, :].astype(F32)
        n = token_input(xq, vrow, l)[TWO]
        for i in range(FOUR):
            uq[TH * i:TH * i + TH, :] = gelu(mm(ma1[l, TH * i:TH * i + TH, :], n))
        y = mm(ma2[l], uq[...])
        x1 = (xq + (y + jnp.concatenate([col[l]] * FOUR, axis=ONE))).astype(BF16)
        x_mid[rows, :] = x1
        x1 = x1.astype(F32)
        n2 = (stats(x1)[ZERO] * vrow[l, TWO:THREE, ZERO:CH] + vrow[l, THREE:FOUR, ZERO:CH]).astype(BF16)
        for c in range(FOUR):
            lanes = slice(CH * c, CH * c + CH)
            uch[QROWS * c:QROWS * c + QROWS, :] = gelu(mm(n2, w1[l, :, lanes]) + vrow[l, FOUR:FIVE, lanes])
        y = mm(uch[ZERO:QROWS, :], w2[l, ZERO:CH, :])
        for c in range(ONE, FOUR):
            y = y + mm(uch[QROWS * c:QROWS * c + QROWS, :], w2[l, CH * c:CH * c + CH, :])
        x_out[rows, :] = (x1 + (y + vrow[l, FIVE:SIX, ZERO:CH])).astype(BF16)
        return carry
    lax.fori_loop(ZERO, QUADS, quad, ZERO)


def token_input(xq, vrow, l):
    xh, scale = stats(xq)
    n = xh * vrow[l, ZERO:ONE, ZERO:CH] + vrow[l, ONE:TWO, ZERO:CH]
    return xh, scale, jnp.where(iota((QROWS, CH), ZERO) == QVALID, F_ONE, n).astype(BF16)


def image_of(shape, axis):
    c = iota(shape, axis)
    return jnp.where(c < QVALID, (c >= TOKENS).astype(jnp.int32) + (c >= TWO * TOKENS).astype(jnp.int32) + (c >= THREE * TOKENS).astype(jnp.int32), IMAGES)


def head_pass(x_out, labels, small, head, d, pool, srow, gsum, flat):
    for k in range(FOUR):
        lanes = slice(LANES * k, LANES * k + LANES)
        srow[ZERO:ONE, lanes] = small[k:k + ONE, :]
        srow[ONE:TWO, lanes] = small[FOUR + k:FIVE + k, :]
    for k in range(EIGHT):
        srow[TWO:THREE, LANES * k:LANES * k + LANES] = small[EIGHT + k:NINE + k, :]
    gain, shift = srow[ZERO:ONE, ZERO:CH], srow[ONE:TWO, ZERO:CH]
    pool[...] = jnp.zeros_like(pool)

    def quad(q, carry):
        xh, scale = stats(x_out[pl.ds(aligned(q, QROWS), QROWS), :].astype(F32))
        pick = (iota((IMAGES, QROWS), ZERO) == image_of((IMAGES, QROWS), ONE) + FOUR * q)
        pool[...] += mm(pick.astype(BF16), (xh * gain + shift).astype(BF16))
        return carry
    lax.fori_loop(ZERO, QUADS, quad, ZERO)
    pooled = (pool[...] / TOKENS).astype(BF16)
    real = iota((IMAGES, CLASS_PAD), ONE) < CLASSES
    logits = jnp.where(real, mm(pooled, head[...]) + srow[TWO:THREE, :], -1e30)
    top = jnp.max(logits, axis=-ONE, keepdims=True)
    log_norm = top + jnp.log(jnp.sum(jnp.exp(logits - top), axis=-ONE, keepdims=True))
    hit = iota((IMAGES, CLASS_PAD), ONE) == labels[:, ZERO:ONE]
    picked = jnp.sum(jnp.where(hit, logits, F_ZERO), axis=-ONE, keepdims=True)
    loss = jnp.broadcast_to(jnp.sum(log_norm - picked), (STEP8, LANES))
    d_logits = (jnp.exp(logits - log_norm) - hit.astype(F32)) / GLOBAL_IMAGES
    d_bf = d_logits.astype(BF16)
    g_head = mm(pool_t(pooled), d_bf)
    for n in range(SIXTEEN):
        for j in range(EIGHT):
            flat[HEAD_ROWS * n + IMAGES * j:HEAD_ROWS * n + IMAGES * j + IMAGES, :] = g_head[IMAGES * n:IMAGES * n + IMAGES, LANES * j:LANES * j + LANES]
        flat[HEAD_ROWS * n + TH:HEAD_ROWS * n + 264, :] = jnp.zeros((STEP8, LANES), F32)
        flat[HEAD_ROWS * n + 264:HEAD_ROWS * n + 272, :] = loss
    d_pool = (mm_nt(d_bf, head[...]) / TOKENS).astype(BF16)
    gsum[...] = jnp.zeros_like(gsum)

    def back(q, carry):
        rows = pl.ds(aligned(q, QROWS), QROWS)
        xh, scale = stats(x_out[rows, :].astype(F32))
        pick = (iota((QROWS, IMAGES), ONE) == image_of((QROWS, IMAGES), ZERO) + FOUR * q)
        dy = mm(pick.astype(BF16), d_pool)
        gsum[ZERO] += fold8(dy * xh)
        gsum[ONE] += fold8(dy)
        d[rows, :] = norm_back(xh, scale, gain, dy)
        return carry
    lax.fori_loop(ZERO, QUADS, back, ZERO)
    g_gain = jnp.sum(gsum[ZERO], axis=ZERO, keepdims=True)
    g_shift = jnp.sum(gsum[ONE], axis=ZERO, keepdims=True)
    g_bias = jnp.sum(d_logits, axis=ZERO, keepdims=True)
    for k in range(FOUR):
        lanes = slice(LANES * k, LANES * k + LANES)
        for row, value in ((HEAD_ROWS * k, g_gain), (HEAD_ROWS * (FOUR + k), g_shift)):
            flat[row + TH:row + 257, :] = value[:, lanes]
    for k in range(EIGHT):
        row = HEAD_ROWS * (EIGHT + k) + TH
        flat[row:row + ONE, :] = g_bias[:, LANES * k:LANES * k + LANES]


def pool_t(pooled):
    return pooled.astype(F32).T.astype(BF16)


def channel_back(l, x_mid, d, vrow, w1, w2, n2, dbf, n2t, dt, uh, dh, dn2, flat, gsum, gb1, hook):
    gsum[...] = jnp.zeros_like(gsum)
    gb1[...] = jnp.zeros_like(gb1)

    def quad(q, carry):
        rows = pl.ds(aligned(q, QROWS), QROWS)
        n2[rows, :] = (stats(x_mid[rows, :].astype(F32))[ZERO] * vrow[l, TWO:THREE, ZERO:CH] + vrow[l, THREE:FOUR, ZERO:CH]).astype(BF16)
        dq = d[rows, :]
        gsum[FOUR] += fold8(dq)
        dbf[rows, :] = dq.astype(BF16)
        dn2[rows, :] = jnp.zeros((QROWS, CH), F32)
        return carry
    lax.fori_loop(ZERO, QUADS, quad, ZERO)
    for k in range(ALL_ROWS // LANES):
        lanes = slice(LANES * k, LANES * k + LANES)
        n2t[:, lanes] = n2[lanes, :].T
        dt[:, lanes] = dbf[lanes, :].T
    hook(-ONE)

    def chunk(c, carry):
        hook(c)
        lanes = pl.ds(aligned(c, CHUNK), CHUNK)

        for b in range(ALL_ROWS // BLOCK):
            rows = slice(BLOCK * b, BLOCK * b + BLOCK)
            u, slope = gelu_both(mm(n2[rows, :], w1[l, :, lanes]) + vrow[l, FOUR:FIVE, lanes])
            uh[rows, :] = u
            dhid = mm_nt(dbf[rows, :], w2[l, lanes, :]).astype(BF16).astype(F32) * slope
            gb1[:, lanes] += fold8(dhid)
            dhid = dhid.astype(BF16)
            dh[rows, :] = dhid
            dn2[rows, :] += mm_nt(dhid, w1[l, :, lanes])
        g1 = mm(n2t[...], dh[...])
        for r in range(CH // STEP8):
            for k in range(TWO):
                flat[pl.ds(ROW_C1 + LANES * r + k + TWO * c, STEP8, stride=SIXTEEN), :] = g1[STEP8 * r:STEP8 * r + STEP8, LANES * k:LANES * k + LANES]
        g2 = mm(dt[...], uh[...]).T
        for r in range(CHUNK // STEP8):
            for k in range(FOUR):
                flat[pl.ds(ROW_C2 + FOUR * (STEP8 * r) + k + FOUR * CHUNK * c, STEP8, stride=FOUR), :] = g2[STEP8 * r:STEP8 * r + STEP8, LANES * k:LANES * k + LANES]
        return carry
    lax.fori_loop(ZERO, HID // CHUNK, chunk, ZERO)


def token_back(l, x_in, x_mid, d, vrow, dn2, ma1, mb1, ma2, mb2, uq, dq_ref, acc1, acc2, rowsum, colsum, gsum, hook):
    for ref in (acc1, acc2, rowsum, colsum):
        ref[...] = jnp.zeros_like(ref)

    def quad(q, carry):
        hook(q)
        rows = pl.ds(aligned(q, QROWS), QROWS)
        xh, scale = stats(x_mid[rows, :].astype(F32))
        dy = dn2[rows, :].astype(BF16).astype(F32)
        gsum[TWO] += fold8(dy * xh)
        gsum[THREE] += fold8(dy)
        d_after = norm_back(xh, scale, vrow[l, TWO:THREE, ZERO:CH], dy) + d[rows, :]
        part = d_after[:, ZERO:LANES]
        for k in range(ONE, FOUR):
            part = part + d_after[:, LANES * k:LANES * k + LANES]
        colsum[ZERO:QROWS, :] += part
        d_bf = d_after.astype(BF16)
        xh, scale, n = token_input(x_in[rows, :].astype(F32), vrow, l)
        for i in range(FOUR):
            part = slice(TH * i, TH * i + TH)
            u, slope = gelu_both(mm(ma1[l, part, :], n))
            uq[part, :] = u
            dhid = mm(mb2[l, part, :], d_bf).astype(BF16).astype(F32) * slope
            total = dhid[:, ZERO:LANES]
            for k in range(ONE, FOUR):
                total = total + dhid[:, LANES * k:LANES * k + LANES]
            rowsum[part, :] += total
            dq_ref[part, :] = dhid.astype(BF16)
        acc1[...] += mm_nt(n, dq_ref[...])
        acc2[...] += mm_nt(d_bf, uq[...])
        dy = mm(mb1[l], dq_ref[...]).astype(BF16).astype(F32)
        gsum[ZERO] += fold8(dy * xh)
        gsum[ONE] += fold8(dy)
        d[rows, :] = norm_back(xh, scale, vrow[l, ZERO:ONE, ZERO:CH], dy) + d_after
        return carry
    lax.fori_loop(ZERO, QUADS, quad, ZERO)


def small_flat(l, flat, acc1, acc2, rowsum, colsum, gsum, gb1, v2):
    g = sum_images(acc1)
    for h in range(TWO):
        flat[pl.ds(h, TOKENS, stride=TWO), :] = g[:, LANES * h:LANES * h + LANES]
    g = sum_images(acc2)
    s, row, perm = token_maps()
    for h in range(TWO):
        padded = jnp.concatenate([g[:, LANES * h:LANES * h + LANES], jnp.zeros((SEVEN, LANES), F32)], axis=ZERO)
        x = skew(lax.dot_general(padded, perm.astype(F32), (((ONE,), (ONE,)), ((), ())), precision=lax.Precision.HIGHEST, preferred_element_type=F32), s, False)

        def place_row(r, carry):
            flat[pl.ds(ROW_T2 + TOKENS * h + r, ONE), :] = jnp.sum(jnp.where(row == r, x, F_ZERO), axis=ZERO, keepdims=True)
            return carry
        lax.fori_loop(ZERO, TOKENS, place_row, ZERO)
    flat[ROW_VEC:FLAT_ROWS + SIXTEEN, :] = jnp.zeros((FLAT_ROWS + SIXTEEN - ROW_VEC, LANES), F32)
    for n in range(TWO):
        v = jnp.sum(gsum[n], axis=ZERO, keepdims=True)
        for k in range(FOUR):
            flat[ROW_VEC + FOUR * n + k:ROW_VEC + FOUR * n + k + ONE, :] = v[:, LANES * k:LANES * k + LANES]
    t = jnp.sum(rowsum[...].T, axis=ZERO, keepdims=True)
    t = t[:, ZERO:TH] + t[:, TH:TWO * TH] + t[:, TWO * TH:THREE * TH] + t[:, THREE * TH:FOUR * TH]
    for h in range(TWO):
        flat[ROW_VEC + EIGHT + h:ROW_VEC + NINE + h, :] = t[:, LANES * h:LANES * h + LANES]
    v2[...] = jnp.zeros_like(v2)
    lists = [(jnp.sum(gsum[TWO], axis=ZERO, keepdims=True), ZERO, FOUR), (jnp.sum(gsum[THREE], axis=ZERO, keepdims=True), FOUR, FOUR), (jnp.sum(gb1[...], axis=ZERO, keepdims=True), EIGHT, SIXTEEN), (jnp.sum(gsum[FOUR], axis=ZERO, keepdims=True), TWENTY_FOUR, FOUR)]
    for v, first, count in lists:
        for k in range(count):
            v2[first + k:first + k + ONE, :] = v[:, LANES * k:LANES * k + LANES]
    turned = pltpu.roll(v2[...], TOKENS, ONE)
    t = jnp.broadcast_to(jnp.sum(colsum[...].T, axis=ZERO, keepdims=True), (STEP8, TWO * LANES))
    b2 = t
    for i in range(ONE, FOUR):
        b2 = b2 + pltpu.roll(t, TWO * LANES - TOKENS * i, ONE)
    before = jnp.concatenate([b2[ZERO:ONE, ZERO:LANES], turned[ZERO:LAST_IMAGE, :]], axis=ZERO)
    merged = jnp.where(iota((IMAGES, LANES), ONE) < TOKENS, before, turned)
    flat[ROW_VEC + TEN:ROW_VEC + 42, :] = merged


def sum_images(acc):
    g = acc[ZERO:TOKENS, ZERO:TH]
    for i in range(ONE, FOUR):
        g = g + acc[TOKENS * i:TOKENS * i + TOKENS, TH * i:TH * i + TH]
    return g


def no_hook(k):
    return None


def at(table):
    def hook(k):
        for key, act in table.items():
            if isinstance(k, int):
                if key == k:
                    act()
            elif key >= ZERO:
                pl.when(k == key)(act)
    return hook


def both(*acts):
    def run():
        for act in acts:
            act()
    return run


def step_kernel(x0, labels, pack, own, stat, gath, x1, x2, x3, d, dn2, n2, dbf, n2t, dt, mix, ma1, mb1, ma2, mb2, col, vrow, v2, bd, srow, pool, gsum, gb1, acc2, rowsum, colsum, flat, w1, w2, slab, head, small, leaving, t0, t1, t2, t3, msg, box, ag_send, ag_recv, rs_send, rs_recv, stage_sem, load_sem, tiny_send, tiny_recv, late_send, late_recv, done, late, late_box):
    where = place()
    me, coords, core, neighbours, partner = where
    load = pltpu.make_async_copy(pack, gath.at[coords[ZERO], coords[ONE], coords[TWO], core], load_sem)
    load.start()
    enter_barrier(neighbours, partner)
    load.wait()
    first = Gather(gath, where, ((ZERO, 352), (352, 352), (704, 336)), ag_send, ag_recv, ZERO)
    rest = Gather(gath, where, ((1040, 448), (1488, 432), (1920, 432)), ag_send, ag_recv, 21)
    first.start()
    for phase in range(THREE):
        first.step(phase)
    rest.start()
    first.finish()
    mats = (ma1, mb1, ma2, mb2, col)
    unflatten_layer(gath, ZERO, flat, (x3, n2, dbf, mix), stage_sem, w1, w2, slab)
    prep_layer(ZERO, slab, vrow, bd, v2, *mats)
    uq, dq = mix.at[ZERO:FOUR * TH, :], mix.at[FOUR * TH:EIGHT * TH, :]
    uch = mix.at[FOUR * TH:FOUR * TH + FOUR * QROWS, :]
    uh, dh = mix.at[ZERO:ALL_ROWS, ZERO:CHUNK], mix.at[ZERO:ALL_ROWS, CHUNK:TWO * CHUNK]
    acc1 = bd.at[ZERO:QROWS, :]
    forward_layer(ZERO, x0, x1, x2, vrow, ma1, ma2, col, w1, w2, uq, uch, at({ONE: lambda: rest.step(ZERO), THREE: lambda: rest.step(ONE), SEVEN: lambda: rest.step(TWO)}))
    rest.finish()
    unflatten_layer(gath, ONE, flat, (x3, n2, dbf, mix), stage_sem, w1, w2, slab)
    unflatten_head(gath, (x3, n2, dbf, mix), stage_sem, head, small)
    prep_layer(ONE, slab, vrow, bd, v2, *mats)
    forward_layer(ONE, x2, x3, n2, vrow, ma1, ma2, col, w1, w2, uq, uch, no_hook)
    head_pass(n2, labels, small, head, d, pool, srow, gsum, flat)

    bufs, sems = (leaving, t0, t1, t2, t3), (rs_send, rs_recv)
    thirds = ((ZERO, 352), (352, 352), (704, 336))
    reduces = [Reduce(flat, HEAD_ROWS, HEAD_ROWS, ((ZERO, 96), (96, 88), (184, 88)), own, HEAD_OFF, bufs, where, sems)]
    reduces += [Reduce(flat, SHARD_ROWS, SLOT_ROWS, thirds, own, l * SLOT_ROWS, bufs, where, sems) for l in (ONE, ZERO)]

    def done_one(work):
        def run():
            work.finish()
            for other in list(neighbours) + [partner]:
                pl.semaphore_signal(done, inc=ONE, device_id=(other,), device_id_type=MESH_ID)
        return run

    def go(work, phase):
        return lambda: work.step(phase)

    h, r1, r0 = reduces
    back = (d, vrow, w1, w2, n2, dbf, n2t, dt, uh, dh, dn2, flat, gsum, gb1)
    tok = (d, vrow, dn2, ma1, mb1, ma2, mb2, uq, dq, acc1, acc2, rowsum, colsum, gsum)
    small_parts = (flat, acc1, acc2, rowsum, colsum, gsum, gb1, v2)
    h.start()
    channel_back(ONE, x3, *back, at({-ONE: go(h, ZERO), ONE: go(h, ONE), TWO: go(h, TWO), FOUR: both(go(h, THREE), done_one(h))}))
    token_back(ONE, x2, x3, *tok, no_hook)
    small_flat(ONE, *small_parts)
    pl.semaphore_wait(done, FOUR)
    r1.start()
    channel_back(ZERO, x1, *back, at({-ONE: go(r1, ZERO), FOUR: go(r1, ONE), SIX: go(r1, TWO)}))
    r1.step(THREE)
    done_one(r1)()
    pl.semaphore_wait(done, FOUR)
    r0.start()
    token_back(ZERO, x0, x1, *tok, at({TWO: go(r0, ZERO)}))
    small_flat(ZERO, *small_parts)
    late[ZERO, ZERO:QVALID, :] = flat[ZERO:QVALID, :]
    late[ZERO, QVALID:240, :] = flat[ROW_VEC:FLAT_ROWS, :]
    hops = [partner, neighbours[TWO], neighbours[ONE], neighbours[ZERO]]

    def exchange(value, box_ref, sems, n):
        return pltpu.make_async_remote_copy(src_ref=value.at[n % TWO], dst_ref=box_ref.at[n], send_sem=sems[ZERO].at[n], recv_sem=sems[ONE].at[n], device_id=(hops[n],), device_id_type=MESH_ID)

    def late_copy(n):
        return exchange(late, late_box, (late_send, late_recv), n)
    late_copy(ZERO).start()
    r0.step(ONE)
    for n in range(FOUR):
        late_copy(n).wait()
        late[(n + ONE) % TWO] = late[n % TWO] + late_box[n]
        if n < THREE:
            late_copy(n + ONE).start()
        if n == TWO:
            r0.step(TWO)
    r0.step(THREE)
    r0.finish()
    own[ZERO:QVALID, :] = jnp.where(me == ZERO, late[ZERO, ZERO:QVALID, :], own[ZERO:QVALID, :])
    last = ROW_VEC - 15 * SHARD_ROWS
    own[last:SHARD_ROWS, :] = jnp.where(me == 15, late[ZERO, QVALID:240, :], own[last:SHARD_ROWS, :])
    for l in range(TWO):
        own[l * SLOT_ROWS + SHARD_ROWS:l * SLOT_ROWS + SLOT_ROWS, :] = jnp.zeros((ONE, LANES), F32)
    msg[ZERO] = jnp.broadcast_to(jnp.sum(square_sum(own, ZERO, SMALL_OFF + EIGHT)), (STEP8, LANES))
    for n in range(FOUR):
        copy = exchange(msg, box, (tiny_send, tiny_recv), n)
        copy.start()
        copy.wait()
        msg[(n + ONE) % TWO] = msg[n % TWO] + box[n]
    stat[ZERO] = msg[ZERO]
    stat[ONE] = own[SMALL_OFF + EIGHT:SMALL_OFF + SIXTEEN, :]


def train_step(x0, labels, pack):
    vmem = pl.BlockSpec(memory_space=pltpu.VMEM)
    act = pltpu.VMEM((ALL_ROWS, CH), BF16)
    wide = pltpu.VMEM((ALL_ROWS, CH), F32)
    across = pltpu.VMEM((CH, ALL_ROWS), BF16)
    tall = pltpu.VMEM((TWO, FOUR * TH, QROWS), BF16)
    flat_mat = pltpu.VMEM((TWO, QROWS, FOUR * TH), BF16)
    acc = pltpu.VMEM((QROWS, FOUR * TH), F32)
    dma = pltpu.SemaphoreType.DMA
    return pl.pallas_call(
        step_kernel,
        out_shape=(jax.ShapeDtypeStruct((AG_ROWS, LANES), F32), jax.ShapeDtypeStruct((TWO, STEP8, LANES), F32), jax.ShapeDtypeStruct((TWO, TWO, TWO, TWO, AG_ROWS, LANES), BF16)),
        in_specs=[vmem] * THREE,
        out_specs=(vmem, vmem, pl.BlockSpec(memory_space=pl.ANY)),
        scratch_shapes=[act, act, act, wide, wide, act, act, across, across, pltpu.VMEM((EIGHT * TH, CH), BF16),
                        tall, flat_mat, flat_mat, tall, pltpu.VMEM((TWO, QROWS, LANES), F32), pltpu.VMEM((TWO, STEP8, HID), F32), pltpu.VMEM((IMAGES, LANES), F32), pltpu.VMEM((TWO * LANES, FOUR * TH), F32),
                        pltpu.VMEM((STEP8, CLASS_PAD), F32), pltpu.VMEM((IMAGES, CH), F32), pltpu.VMEM((FIVE, STEP8, CH), F32), pltpu.VMEM((STEP8, HID), F32), acc,
                        pltpu.VMEM((FOUR * TH, LANES), F32), pltpu.VMEM((TWO * LANES, LANES), F32), pltpu.VMEM((FLAT_ROWS + SIXTEEN, LANES), F32),
                        pltpu.VMEM((TWO, CH, HID), BF16), pltpu.VMEM((TWO, HID, CH), BF16), pltpu.VMEM((TWO, SLAB_ROWS, LANES), F32), pltpu.VMEM((CH, CLASS_PAD), BF16), pltpu.VMEM((SIXTEEN, LANES), F32),
                        pltpu.VMEM((TWO, TWO, TWO, SLOT_ROWS, LANES), F32), pltpu.VMEM((TWO, TWO, TWO, SLOT_ROWS, LANES), F32), pltpu.VMEM((TWO, TWO, SLOT_ROWS, LANES), F32), pltpu.VMEM((TWO, SLOT_ROWS, LANES), F32), pltpu.VMEM((SLOT_ROWS, LANES), F32),
                        pltpu.VMEM((TWO, STEP8, LANES), F32), pltpu.VMEM((FOUR, STEP8, LANES), F32),
                        dma((42,)), dma((42,)), dma((12,)), dma((12,)), dma((SIXTEEN,)), dma, dma((FOUR,)), dma((FOUR,)), dma((FOUR,)), dma((FOUR,)), pltpu.SemaphoreType.REGULAR, pltpu.VMEM((TWO, SLAB_ROWS, LANES), F32), pltpu.VMEM((FOUR, SLAB_ROWS, LANES), F32)],
        compiler_params=pltpu.CompilerParams(collective_id=ZERO, has_side_effects=True, vmem_limit_bytes=67043328),
        name='train_step',
    )(x0, labels, pack)


LEARN_RATE = 0.003
BETA_ONE = 0.9
BETA_TWO = 0.999
ADAM_EPS = 1e-8
WEIGHT_DECAY = 0.03
ADAM_STEP = 10


def adam_update(master, gradient, moment, second, decay_rate):
    moment_new = BETA_ONE * moment + (F_ONE - BETA_ONE) * gradient
    second_new = BETA_TWO * second + (F_ONE - BETA_TWO) * gradient * gradient
    m_hat = moment_new / (F_ONE - BETA_ONE ** ADAM_STEP)
    v_hat = second_new / (F_ONE - BETA_TWO ** ADAM_STEP)
    master_new = master - LEARN_RATE * (m_hat / (jnp.sqrt(v_hat) + ADAM_EPS) + decay_rate * master)
    return master_new, moment_new, second_new


def solution(mesh):
    row_spec = P('fsdp')
    layer_spec = P(None, 'fsdp')
    in_specs = (row_spec, row_spec, layer_spec, row_spec, row_spec, layer_spec, row_spec, row_spec, layer_spec, row_spec, row_spec)
    out_specs = (P(),) + in_specs[TWO:]

    def device_step(act_in, labels, layer_p, head_w, small_p, layer_m, head_m, small_m, layer_v, head_v, small_v):
        mat_len = ROW_VEC * LANES
        quads = jnp.pad(act_in.reshape(QUADS, QVALID, CH), ((ZERO, ZERO), (ZERO, QROWS - QVALID), (ZERO, ZERO))).reshape(ALL_ROWS, CH)
        layer_bf = jnp.pad(layer_p.astype(BF16).reshape(TWO, SHARD_ROWS, LANES), ((ZERO, ZERO), (ZERO, ONE), (ZERO, ZERO)))
        head_bf = jnp.pad(head_w.astype(BF16), ((ZERO, ZERO), (ZERO, CLASS_PAD - CLASSES))).reshape(IMAGES, EIGHT, LANES).transpose(ONE, ZERO, TWO).reshape(TH, LANES)
        small_bf = jnp.pad(small_p.astype(BF16).reshape(ONE, LANES), ((ZERO, 15), (ZERO, ZERO)))
        pack = jnp.concatenate([layer_bf.reshape(TWO * SLOT_ROWS, LANES), head_bf, small_bf])
        own, stat, _ = train_step(quads, jnp.broadcast_to(labels[:, None], (IMAGES, LANES)), pack)
        layer_g = own[:HEAD_OFF].reshape(TWO, SLOT_ROWS, LANES)[:, :SHARD_ROWS].reshape(TWO, SHARD_ROWS * LANES)
        head_g = own[HEAD_OFF:SMALL_OFF].reshape(EIGHT, IMAGES, LANES).transpose(ONE, ZERO, TWO).reshape(IMAGES, CLASS_PAD)[:, :CLASSES]
        small_g = own[SMALL_OFF]
        loss_value = stat[ONE, ZERO, ZERO] / GLOBAL_IMAGES
        clip_scale = F_ONE / jnp.maximum(F_ONE, jnp.sqrt(stat[ZERO, ZERO, ZERO]))
        shard_len = layer_p.shape[ONE]
        flat_pos = lax.axis_index('fsdp') * shard_len + jnp.arange(shard_len)
        layer_decay = jnp.where(flat_pos < mat_len, WEIGHT_DECAY, F_ZERO)[None, :]
        new_lp, new_lm, new_lv = adam_update(layer_p, layer_g * clip_scale, layer_m, layer_v, layer_decay)
        new_hw, new_hm, new_hv = adam_update(head_w, head_g * clip_scale, head_m, head_v, WEIGHT_DECAY)
        new_sp, new_sm, new_sv = adam_update(small_p, small_g * clip_scale, small_m, small_v, F_ZERO)
        return (loss_value, new_lp, new_hw, new_sp, new_lm, new_hm, new_sm, new_lv, new_hv, new_sv)

    return jax.shard_map(device_step, mesh=mesh, in_specs=in_specs, out_specs=out_specs, check_vma=False)
```

```python
import functools
import math
import jax
import jax.numpy as jnp
from jax import lax
from jax.experimental import pallas as pl
from jax.experimental.pallas import tpu as pltpu
from jax.sharding import PartitionSpec as P

ZERO = 0
ONE = 1
TWO = 2
THREE = 3
FOUR = 4
FIVE = 5
SIX = 6
SEVEN = 7
EIGHT = 8
NINE = 9
SIXTEEN = 16
LANES = 128
IMAGES = 32
LAST_IMAGE = 31
CH = 512
CLASS_PAD = 1024
HID = 2048
TH = 256
F_ZERO = 0.0
F_ONE = 1.0
TWENTY_FOUR = 24
TOKEN_PAD = 56
QVALID = 196
SIXTY_FOUR = 64
TEN = 10
MESH_ID = pl.DeviceIdType.MESH
F32 = jnp.float32
BF16 = jnp.bfloat16

DEVICES = 16
SHARD_ROWS = 1039
UPDATE_ROWS = 130
SLOT_ROWS = 1040
ROW_C1 = 196
ROW_C2 = 8388
ROW_VEC = 16580
FLAT_ROWS = 16624
SLAB_ROWS = 240
HEAD_OFF = 2 * SLOT_ROWS
SMALL_OFF = HEAD_OFF + 256
AG_ROWS = SMALL_OFF + 16
HEAD_ROWS = 272
ORDERS = ((2, 1, 0), (1, 0, 2), (0, 2, 1))
AXIS_STEP = (8, 4, 2)


def place():
    me = lax.axis_index('fsdp')
    coords = [me // EIGHT, (me // FOUR) % TWO, (me // TWO) % TWO]
    core = me % TWO
    neighbours = [me + AXIS_STEP[a] - TWO * AXIS_STEP[a] * coords[a] for a in range(THREE)]
    partner = me + ONE - TWO * core
    return me, coords, core, neighbours, partner


def enter_barrier(me):
    barrier = pltpu.get_barrier_semaphore()
    for k in range(ONE, DEVICES):
        pl.semaphore_signal(barrier, inc=ONE, device_id=((me + k) % DEVICES,), device_id_type=MESH_ID)
    pl.semaphore_wait(barrier, DEVICES - ONE)


def slot_view(buf, coords, core, free_axes, row0, rows):
    index = [pl.ds(ZERO, TWO) if a in free_axes else coords[a] for a in range(THREE)]
    return buf.at[index[ZERO], index[ONE], index[TWO], core, pl.ds(row0, rows), :]


class Gather:
    def __init__(self, buf, where, row_groups, send_sem, recv_sem, sem0):
        self.buf, self.where, self.groups = buf, where, row_groups
        self.send_sem, self.recv_sem, self.sem0 = send_sem, recv_sem, sem0
        self.pending = []

    def copy(self, view, sem, device):
        return pltpu.make_async_remote_copy(src_ref=view, dst_ref=view, send_sem=self.send_sem.at[self.sem0 + sem], recv_sem=self.recv_sem.at[self.sem0 + sem], device_id=(device,), device_id_type=MESH_ID)

    def link(self, group, phase):
        me, coords, core, neighbours, partner = self.where
        order = ORDERS[group]
        row0, rows = self.groups[group]
        view = slot_view(self.buf, coords, core, order[:phase], row0, rows)
        return self.copy(view, group * THREE + phase, neighbours[order[phase]])

    def chip(self, group, phase):
        me, coords, core, neighbours, partner = self.where
        order = ORDERS[group]
        row0, rows = self.groups[group]
        if phase < ZERO:
            view = slot_view(self.buf, coords, core, (), row0, rows)
        else:
            far = list(coords)
            far[order[phase]] = ONE - coords[order[phase]]
            view = slot_view(self.buf, far, core, order[:phase], row0, rows)
        return self.copy(view, NINE + group * FOUR + phase + ONE, partner)

    def start(self):
        for group in range(THREE):
            self.link(group, ZERO).start()
        for group in range(THREE):
            self.chip(group, -ONE).start()

    def step(self, phase):
        for group in range(THREE):
            self.link(group, phase).wait_recv()
            if phase < TWO:
                self.link(group, phase + ONE).start()
            self.chip(group, phase).start()

    def finish(self):
        for group in range(THREE):
            for phase in range(-ONE, THREE):
                self.chip(group, phase).wait()
            for phase in range(THREE):
                self.link(group, phase).wait_send()


def slot_of(dev):
    return dev // EIGHT, (dev // FOUR) % TWO, (dev // TWO) % TWO, dev % TWO


def fetch_layer(gath, layer, bays, stage_sem):
    copies = []
    for dev in range(SIXTEEN):
        z, y, x, core = slot_of(dev)
        land = bays[dev // FOUR].at[pl.ds(ZERO, SLOT_ROWS), pl.ds(LANES * (dev % FOUR), LANES)]
        copies.append(pltpu.make_async_copy(gath.at[z, y, x, core, pl.ds(layer * SLOT_ROWS, SLOT_ROWS), :], land, stage_sem.at[dev]))
    for copy in copies:
        copy.start()
    return copies


def unflatten_layer(gath, layer, flat, bays, stage_sem, w1_ref, w2_ref, slab_ref):
    copies = fetch_layer(gath, layer, bays, stage_sem)
    for dev in range(SIXTEEN):
        copies[dev].wait()

        def chunk(k, inner):
            block = bays[dev // FOUR][pl.ds(pl.multiple_of(SIXTEEN * k, SIXTEEN), SIXTEEN), LANES * (dev % FOUR):LANES * (dev % FOUR) + LANES]
            flat[pl.ds(dev * SHARD_ROWS + SIXTEEN * k, SIXTEEN), :] = block.astype(F32)
            return inner
        lax.fori_loop(ZERO, SLOT_ROWS // SIXTEEN, chunk, ZERO, unroll=FIVE)

    def first(rb, carry):
        for j in range(SIXTEEN):
            block = flat[pl.ds(ROW_C1 + TH * rb + j, SIXTEEN, stride=SIXTEEN), :]
            w1_ref[layer, pl.ds(pl.multiple_of(SIXTEEN * rb, SIXTEEN), SIXTEEN), LANES * j:LANES * j + LANES] = block.astype(BF16)
        return carry
    lax.fori_loop(ZERO, IMAGES, first, ZERO)

    def second(rb, carry):
        for j in range(FOUR):
            block = flat[pl.ds(ROW_C2 + SIXTY_FOUR * rb + j, SIXTEEN, stride=FOUR), :]
            w2_ref[layer, pl.ds(pl.multiple_of(SIXTEEN * rb, SIXTEEN), SIXTEEN), LANES * j:LANES * j + LANES] = block.astype(BF16)
        return carry
    lax.fori_loop(ZERO, LANES, second, ZERO, unroll=FOUR)
    slab_ref[layer, ZERO:QVALID, :] = flat[ZERO:QVALID, :]
    slab_ref[layer, QVALID:240, :] = flat[ROW_VEC:FLAT_ROWS, :]


def unflatten_head(gath, bays, stage_sem, head_ref, small_ref):
    copies = []
    for dev in range(SIXTEEN):
        z, y, x, core = slot_of(dev)
        copies.append(pltpu.make_async_copy(gath.at[z, y, x, core, pl.ds(HEAD_OFF, HEAD_ROWS), :], bays[dev // FOUR].at[pl.ds(ZERO, HEAD_ROWS), pl.ds(LANES * (dev % FOUR), LANES)], stage_sem.at[dev]))
    for copy in copies:
        copy.start()
    for dev in range(SIXTEEN):
        copies[dev].wait()
        lanes = slice(LANES * (dev % FOUR), LANES * (dev % FOUR) + LANES)
        for j in range(EIGHT):
            head_ref[IMAGES * dev:IMAGES * dev + IMAGES, LANES * j:LANES * j + LANES] = bays[dev // FOUR][IMAGES * j:IMAGES * j + IMAGES, lanes]
        small_ref[dev:dev + ONE, :] = bays[dev // FOUR][TH:272, lanes].astype(F32)[ZERO:ONE, :]


class Reduce:
    def __init__(self, flat, pitch, rows, groups, out, out_row, bufs, where, sems):
        self.flat, self.pitch, self.rows, self.groups, self.out, self.out_row = flat, pitch, rows, groups, out, out_row
        self.leaving, self.temps = bufs[ZERO], bufs[ONE:]
        self.where = where
        self.send_sem, self.recv_sem = sems

    def spread(self):
        me, coords, core, neighbours, partner = self.where

        def chunk(k, carry):
            for n in range(EIGHT):
                self.leaving[n // FOUR, (n // TWO) % TWO, n % TWO, pl.ds(pl.multiple_of(EIGHT * k, EIGHT), EIGHT), :] = self.flat[pl.ds(self.pitch * (TWO * n + ONE - core) + EIGHT * k, EIGHT), :]
            return carry
        lax.fori_loop(ZERO, self.rows // EIGHT, chunk, ZERO)

    def views(self, group, phase):
        me, coords, core, neighbours, partner = self.where
        row0, rows = self.groups[group]
        order = ORDERS[group]
        if phase == ZERO:
            free = (ZERO, ONE, TWO)
            leave = self.leaving.at[:, :, :, pl.ds(row0, rows), :]
            device = partner
        else:
            axis = order[phase - ONE]
            free = tuple(a for a in range(THREE) if a in order[phase:])
            index = [pl.ds(ZERO, TWO) if a in free else coords[a] for a in range(THREE)]
            index[axis] = ONE - coords[axis]
            leave = self.temps[ZERO].at[index[ZERO], index[ONE], index[TWO], pl.ds(row0, rows), :]
            device = neighbours[axis]
        land = self.temps[phase].at[(slice(None),) * len(free) + (pl.ds(row0, rows), slice(None))]
        return leave, land, device, free

    def copy(self, group, phase):
        leave, land, device, free = self.views(group, phase)
        sem = group * FOUR + phase
        return pltpu.make_async_remote_copy(src_ref=leave, dst_ref=land, send_sem=self.send_sem.at[sem], recv_sem=self.recv_sem.at[sem], device_id=(device,), device_id_type=MESH_ID)

    def add(self, group, phase):
        me, coords, core, neighbours, partner = self.where
        free = self.views(group, phase)[THREE]
        row0, rows = self.groups[group]
        total, temp = self.temps[ZERO], self.temps[phase]
        count = TWO ** len(free)
        per = max(ONE, EIGHT // count)
        while rows % (EIGHT * per):
            per //= TWO

        def chunk(k, carry):
            for part in range(per):
                start = pl.multiple_of(row0 + EIGHT * (per * k + part), EIGHT)
                for n in range(count):
                    index = list(coords)
                    bits = []
                    for pos, a in enumerate(free):
                        bit = (n // TWO ** (len(free) - ONE - pos)) % TWO
                        index[a] = bit
                        bits.append(bit)
                    target = (index[ZERO], index[ONE], index[TWO], pl.ds(start, EIGHT), slice(None))
                    if phase == ZERO:
                        value = total[target] + self.flat[pl.ds(self.pitch * (TWO * n + core) + start, EIGHT), :]
                    else:
                        value = total[target] + temp[tuple(bits) + (pl.ds(start, EIGHT), slice(None))]
                    if phase == THREE:
                        self.out[pl.ds(pl.multiple_of(self.out_row + start, EIGHT), EIGHT), :] = value
                    else:
                        total[target] = value
            return carry
        lax.fori_loop(ZERO, rows // (EIGHT * per), chunk, ZERO)

    def start(self):
        self.spread()
        for group in range(THREE):
            self.copy(group, ZERO).start()

    def step(self, phase):
        for group in range(THREE):
            self.copy(group, phase).wait_recv()
            self.add(group, phase)
            if phase < THREE:
                self.copy(group, phase + ONE).start()

    def finish(self):
        for group in range(THREE):
            for phase in range(FOUR):
                self.copy(group, phase).wait_send()


def square_sum(ref, row0, rows):
    def chunk(k, total):
        block = ref[pl.ds(pl.multiple_of(row0 + EIGHT * k, EIGHT), EIGHT), :]
        return total + block * block
    return lax.fori_loop(ZERO, rows // EIGHT, chunk, jnp.zeros((EIGHT, LANES), F32), unroll=TWO)


QUADS = 8
QROWS = 208
TOKENS = 49
ALL_ROWS = QUADS * QROWS
CHUNK = 256
BLOCK = 416
TOK_ROWS = 256
TOK_LANES = 256
FWD_ROWS = 256
FWD_LANES = 512
CLASSES = 1000
GLOBAL_IMAGES = 512.0
LN_EPS = 1e-6
GELU_A = 0.7978845608028654
GELU_B = GELU_A * 0.044715
HALF = 0.5
ROW_T2 = 98
INV49 = 81
LOW7 = 127
SLAB_VEC = 196
V_BT1 = 204
V_MIS = 206
STEP8 = 8


def mm(a, b):
    return jnp.dot(a, b, preferred_element_type=F32)


def mm_nt(a, b):
    return lax.dot_general(a, b, (((ONE,), (ONE,)), ((), ())), preferred_element_type=F32)


def iota(shape, axis):
    return lax.broadcasted_iota(jnp.int32, shape, axis)


def aligned(start, unit):
    return pl.multiple_of(start * unit, unit)


def stats(x):
    mean = jnp.mean(x, axis=-ONE, keepdims=True)
    centered = x - mean
    scale = lax.rsqrt(jnp.mean(centered * centered, axis=-ONE, keepdims=True) + LN_EPS)
    return centered * scale, scale


def fold8(x):
    return jnp.sum(x.reshape(x.shape[ZERO] // STEP8, STEP8, x.shape[ONE]), axis=ZERO)


def gelu_tanh(h):
    sq = h * h
    return sq, jnp.tanh(h * (GELU_A + GELU_B * sq))


def gelu(h):
    sq, t = gelu_tanh(h)
    half = HALF * h
    return (half + half * t).astype(BF16)


def gelu_both(h):
    sq, t = gelu_tanh(h)
    side = HALF + HALF * t
    u = h * side
    return u.astype(BF16), side + (u - u * t) * (GELU_A + (3.0 * GELU_B) * sq)


def norm_back(xh, scale, gain, dy):
    dxh = dy * gain
    return scale * (dxh - jnp.mean(dxh, axis=-ONE, keepdims=True) - xh * jnp.mean(dxh * xh, axis=-ONE, keepdims=True))


def token_maps():
    s = iota((TOKEN_PAD, LANES), ZERO)
    lane = iota((TOKEN_PAD, LANES), ONE)
    j = ((lane - s) * INV49) & LOW7
    row = jnp.where(s < TOKENS, (j * TOKENS + s) >> SEVEN, -ONE)
    perm = (iota((LANES, LANES), ZERO) == ((iota((LANES, LANES), ONE) * TOKENS) & LOW7))
    return s, row, perm


def skew(x, s, left):
    for bit in range(SEVEN):
        amount = TWO ** bit
        x = jnp.where(((s >> bit) & ONE) == ONE, pltpu.roll(x, LANES - amount if left else amount, ONE), x)
    return x


def prep_layer(l, slab, vrow, bd, v2, ma1, mb1, ma2, mb2, col):
    for k in range(FOUR):
        lanes = slice(LANES * k, LANES * k + LANES)
        vrow[l, ZERO:ONE, lanes] = slab[l, SLAB_VEC + k:SLAB_VEC + k + ONE, :]
        vrow[l, ONE:TWO, lanes] = slab[l, SLAB_VEC + FOUR + k:SLAB_VEC + FIVE + k, :]
    lane = iota((IMAGES, LANES), ONE)
    cut = LANES - TOKENS
    v2[...] = jnp.where(lane < cut, pltpu.roll(slab[l, V_MIS:V_MIS + IMAGES, :], cut, ONE), pltpu.roll(slab[l, V_MIS + ONE:V_MIS + 33, :], cut, ONE))
    for row, first, count in ((TWO, ZERO, FOUR), (THREE, FOUR, FOUR), (FOUR, EIGHT, SIXTEEN), (FIVE, TWENTY_FOUR, FOUR)):
        for k in range(count):
            vrow[l, row:row + ONE, LANES * k:LANES * k + LANES] = v2[first + k:first + k + ONE, :]
    bd[...] = jnp.zeros_like(bd)
    for h in range(TWO):
        w = slab[l, pl.ds(h, TOKENS, stride=TWO), :]
        for i in range(FOUR):
            bd[TOKENS * i:TOKENS * i + TOKENS, TH * i + LANES * h:TH * i + LANES * h + LANES] = w
    mb1[l] = bd[ZERO:QROWS, :].astype(BF16)
    for h in range(TWO):
        for i in range(FOUR):
            bd[QVALID:QVALID + ONE, TH * i + LANES * h:TH * i + LANES * h + LANES] = slab[l, V_BT1 + h:V_BT1 + h + ONE, :]
    ma1[l] = bd[...].T[:, ZERO:QROWS].astype(BF16)
    bd[...] = jnp.zeros_like(bd)
    s, row, perm = token_maps()
    for h in range(TWO):
        def pick(r, acc):
            return jnp.where(row == r, slab[l, pl.ds(ROW_T2 + TOKENS * h + r, ONE), :], acc)
        x = skew(lax.fori_loop(ZERO, TOKENS, pick, jnp.zeros((TOKEN_PAD, LANES), F32)), s, True)
        w = mm(x.astype(BF16), perm.astype(BF16))[ZERO:TOKENS]
        for i in range(FOUR):
            bd[TOKENS * i:TOKENS * i + TOKENS, TH * i + LANES * h:TH * i + LANES * h + LANES] = w
    ma2[l] = bd[ZERO:QROWS, :].astype(BF16)
    mb2[l] = bd[...].T[:, ZERO:QROWS].astype(BF16)
    bias = jnp.where(iota((ONE, LANES), ONE) < TOKENS, slab[l, V_MIS:V_MIS + ONE, :], F_ZERO)
    wide = jnp.concatenate([jnp.broadcast_to(bias, (LANES, LANES)), jnp.zeros((LANES, LANES), F32)], axis=ONE)
    spread = wide
    for i in range(ONE, FOUR):
        spread = spread + pltpu.roll(wide, TOKENS * i, ONE)
    col[l] = spread.T[ZERO:QROWS, :]


def forward_layer(l, x_in, x_mid, x_out, vrow, ma1, ma2, col, w1, w2, uq, uch, hook):
    def quad(q, carry):
        hook(q)
        rows = pl.ds(aligned(q, QROWS), QROWS)
        xq = x_in[rows, :].astype(F32)
        n = token_input(xq, vrow, l)[TWO]
        for lane0 in range(ZERO, CH, FWD_LANES):
            for row0 in range(ZERO, FOUR * TH, FWD_ROWS):
                uq[row0:row0 + FWD_ROWS, lane0:lane0 + FWD_LANES] = gelu(mm(ma1[l, row0:row0 + FWD_ROWS, :], n[:, lane0:lane0 + FWD_LANES]))
        y = mm(ma2[l], uq[...])
        x1 = (xq + (y + jnp.concatenate([col[l]] * FOUR, axis=ONE))).astype(BF16)
        x_mid[rows, :] = x1
        x1 = x1.astype(F32)
        n2 = (stats(x1)[ZERO] * vrow[l, TWO:THREE, ZERO:CH] + vrow[l, THREE:FOUR, ZERO:CH]).astype(BF16)
        for c in range(FOUR):
            lanes = slice(CH * c, CH * c + CH)
            uch[QROWS * c:QROWS * c + QROWS, :] = gelu(mm(n2, w1[l, :, lanes]) + vrow[l, FOUR:FIVE, lanes])
        y = mm(uch[ZERO:QROWS, :], w2[l, ZERO:CH, :])
        for c in range(ONE, FOUR):
            y = y + mm(uch[QROWS * c:QROWS * c + QROWS, :], w2[l, CH * c:CH * c + CH, :])
        x_out[rows, :] = (x1 + (y + vrow[l, FIVE:SIX, ZERO:CH])).astype(BF16)
        return carry
    lax.fori_loop(ZERO, QUADS, quad, ZERO)


def token_input(xq, vrow, l):
    xh, scale = stats(xq)
    n = xh * vrow[l, ZERO:ONE, ZERO:CH] + vrow[l, ONE:TWO, ZERO:CH]
    return xh, scale, jnp.where(iota((QROWS, CH), ZERO) == QVALID, F_ONE, n).astype(BF16)


def image_of(shape, axis):
    c = iota(shape, axis)
    return jnp.where(c < QVALID, (c >= TOKENS).astype(jnp.int32) + (c >= TWO * TOKENS).astype(jnp.int32) + (c >= THREE * TOKENS).astype(jnp.int32), IMAGES)


def head_pass(x_out, labels, small, head, d, pool, srow, gsum, flat):
    for k in range(FOUR):
        lanes = slice(LANES * k, LANES * k + LANES)
        srow[ZERO:ONE, lanes] = small[k:k + ONE, :]
        srow[ONE:TWO, lanes] = small[FOUR + k:FIVE + k, :]
    for k in range(EIGHT):
        srow[TWO:THREE, LANES * k:LANES * k + LANES] = small[EIGHT + k:NINE + k, :]
    gain, shift = srow[ZERO:ONE, ZERO:CH], srow[ONE:TWO, ZERO:CH]
    pool[...] = jnp.zeros_like(pool)

    def quad(q, carry):
        xh, scale = stats(x_out[pl.ds(aligned(q, QROWS), QROWS), :].astype(F32))
        pick = (iota((IMAGES, QROWS), ZERO) == image_of((IMAGES, QROWS), ONE) + FOUR * q)
        pool[...] += mm(pick.astype(BF16), (xh * gain + shift).astype(BF16))
        return carry
    lax.fori_loop(ZERO, QUADS, quad, ZERO)
    pooled = (pool[...] / TOKENS).astype(BF16)
    real = iota((IMAGES, CLASS_PAD), ONE) < CLASSES
    logits = jnp.where(real, mm(pooled, head[...]) + srow[TWO:THREE, :], -1e30)
    top = jnp.max(logits, axis=-ONE, keepdims=True)
    log_norm = top + jnp.log(jnp.sum(jnp.exp(logits - top), axis=-ONE, keepdims=True))
    hit = iota((IMAGES, CLASS_PAD), ONE) == labels[:, ZERO:ONE]
    picked = jnp.sum(jnp.where(hit, logits, F_ZERO), axis=-ONE, keepdims=True)
    loss = jnp.broadcast_to(jnp.sum(log_norm - picked), (STEP8, LANES))
    d_logits = (jnp.exp(logits - log_norm) - hit.astype(F32)) / GLOBAL_IMAGES
    d_bf = d_logits.astype(BF16)
    g_head = mm(pool_t(pooled), d_bf)
    for n in range(SIXTEEN):
        for j in range(EIGHT):
            flat[HEAD_ROWS * n + IMAGES * j:HEAD_ROWS * n + IMAGES * j + IMAGES, :] = g_head[IMAGES * n:IMAGES * n + IMAGES, LANES * j:LANES * j + LANES]
        flat[HEAD_ROWS * n + TH:HEAD_ROWS * n + 264, :] = jnp.zeros((STEP8, LANES), F32)
        flat[HEAD_ROWS * n + 264:HEAD_ROWS * n + 272, :] = loss
    d_pool = (mm_nt(d_bf, head[...]) / TOKENS).astype(BF16)
    gsum[...] = jnp.zeros_like(gsum)

    def back(q, carry):
        rows = pl.ds(aligned(q, QROWS), QROWS)
        xh, scale = stats(x_out[rows, :].astype(F32))
        pick = (iota((QROWS, IMAGES), ONE) == image_of((QROWS, IMAGES), ZERO) + FOUR * q)
        dy = mm(pick.astype(BF16), d_pool)
        gsum[ZERO] += fold8(dy * xh)
        gsum[ONE] += fold8(dy)
        d[rows, :] = norm_back(xh, scale, gain, dy)
        return carry
    lax.fori_loop(ZERO, QUADS, back, ZERO)
    g_gain = jnp.sum(gsum[ZERO], axis=ZERO, keepdims=True)
    g_shift = jnp.sum(gsum[ONE], axis=ZERO, keepdims=True)
    g_bias = jnp.sum(d_logits, axis=ZERO, keepdims=True)
    for k in range(FOUR):
        lanes = slice(LANES * k, LANES * k + LANES)
        for row, value in ((HEAD_ROWS * k, g_gain), (HEAD_ROWS * (FOUR + k), g_shift)):
            flat[row + TH:row + 257, :] = value[:, lanes]
    for k in range(EIGHT):
        row = HEAD_ROWS * (EIGHT + k) + TH
        flat[row:row + ONE, :] = g_bias[:, LANES * k:LANES * k + LANES]


def pool_t(pooled):
    return pooled.astype(F32).T.astype(BF16)


def channel_back(l, x_mid, d, vrow, w1, w2, n2, dbf, n2t, dt, uh, dh, dn2, flat, gsum, gb1, hook):
    gsum[...] = jnp.zeros_like(gsum)
    gb1[...] = jnp.zeros_like(gb1)

    def quad(q, carry):
        rows = pl.ds(aligned(q, QROWS), QROWS)
        n2[rows, :] = (stats(x_mid[rows, :].astype(F32))[ZERO] * vrow[l, TWO:THREE, ZERO:CH] + vrow[l, THREE:FOUR, ZERO:CH]).astype(BF16)
        dq = d[rows, :]
        gsum[FOUR] += fold8(dq)
        dbf[rows, :] = dq.astype(BF16)
        dn2[rows, :] = jnp.zeros((QROWS, CH), F32)
        return carry
    lax.fori_loop(ZERO, QUADS, quad, ZERO)
    for k in range(ALL_ROWS // LANES):
        lanes = slice(LANES * k, LANES * k + LANES)
        n2t[:, lanes] = n2[lanes, :].T
        dt[:, lanes] = dbf[lanes, :].T
    hook(-ONE)

    def chunk(c, carry):
        hook(c)
        lanes = pl.ds(aligned(c, CHUNK), CHUNK)

        with jax.named_scope('ch_block'):
            for b in range(ALL_ROWS // BLOCK):
                rows = slice(BLOCK * b, BLOCK * b + BLOCK)
                u, slope = gelu_both(mm(n2[rows, :], w1[l, :, lanes]) + vrow[l, FOUR:FIVE, lanes])
                uh[rows, :] = u
                dhid = mm_nt(dbf[rows, :], w2[l, lanes, :]).astype(BF16).astype(F32) * slope
                gb1[:, lanes] += fold8(dhid)
                dhid = dhid.astype(BF16)
                dh[rows, :] = dhid
                dn2[rows, :] += mm_nt(dhid, w1[l, :, lanes])
        with jax.named_scope('ch_g1'):
            g1 = mm(n2t[...], dh[...])
            for r in range(CH // STEP8):
                for k in range(TWO):
                    flat[pl.ds(ROW_C1 + LANES * r + k + TWO * c, STEP8, stride=SIXTEEN), :] = g1[STEP8 * r:STEP8 * r + STEP8, LANES * k:LANES * k + LANES]
        with jax.named_scope('ch_g2'):
            g2 = mm(dt[...], uh[...]).T
            for r in range(CHUNK // STEP8):
                for k in range(FOUR):
                    flat[pl.ds(ROW_C2 + FOUR * (STEP8 * r) + k + FOUR * CHUNK * c, STEP8, stride=FOUR), :] = g2[STEP8 * r:STEP8 * r + STEP8, LANES * k:LANES * k + LANES]
        return carry
    lax.fori_loop(ZERO, HID // CHUNK, chunk, ZERO)


def token_back(l, x_in, x_mid, d, vrow, dn2, ma1, mb1, ma2, mb2, uq, dq_ref, acc1, acc2, rowsum, colsum, gsum, hook):
    for ref in (acc1, acc2, rowsum, colsum):
        ref[...] = jnp.zeros_like(ref)

    def quad(q, carry):
        hook(q)
        rows = pl.ds(aligned(q, QROWS), QROWS)
        xh, scale = stats(x_mid[rows, :].astype(F32))
        dy = dn2[rows, :].astype(BF16).astype(F32)
        gsum[TWO] += fold8(dy * xh)
        gsum[THREE] += fold8(dy)
        d_after = norm_back(xh, scale, vrow[l, TWO:THREE, ZERO:CH], dy) + d[rows, :]
        part = d_after[:, ZERO:LANES]
        for k in range(ONE, FOUR):
            part = part + d_after[:, LANES * k:LANES * k + LANES]
        colsum[ZERO:QROWS, :] += part
        d_bf = d_after.astype(BF16)
        xh, scale, n = token_input(x_in[rows, :].astype(F32), vrow, l)
        for lane0 in range(ZERO, CH, TOK_LANES):
            lanes = slice(lane0, lane0 + TOK_LANES)
            for row0 in range(ZERO, FOUR * TH, TOK_ROWS):
                part = slice(row0, row0 + TOK_ROWS)
                u, slope = gelu_both(mm(ma1[l, part, :], n[:, lanes]))
                uq[part, lanes] = u
                dhid = mm(mb2[l, part, :], d_bf[:, lanes]).astype(BF16).astype(F32) * slope
                total = dhid[:, ZERO:LANES]
                for k in range(ONE, TOK_LANES // LANES):
                    total = total + dhid[:, LANES * k:LANES * k + LANES]
                rowsum[part, :] += total
                dq_ref[part, lanes] = dhid.astype(BF16)
        acc1[...] += mm_nt(n, dq_ref[...])
        acc2[...] += mm_nt(d_bf, uq[...])
        dy = mm(mb1[l], dq_ref[...]).astype(BF16).astype(F32)
        gsum[ZERO] += fold8(dy * xh)
        gsum[ONE] += fold8(dy)
        d[rows, :] = norm_back(xh, scale, vrow[l, ZERO:ONE, ZERO:CH], dy) + d_after
        return carry
    lax.fori_loop(ZERO, QUADS, quad, ZERO)


def small_flat(l, flat, acc1, acc2, rowsum, colsum, gsum, gb1, v2):
    g = sum_images(acc1)
    for h in range(TWO):
        flat[pl.ds(h, TOKENS, stride=TWO), :] = g[:, LANES * h:LANES * h + LANES]
    g = sum_images(acc2)
    s, row, perm = token_maps()
    for h in range(TWO):
        padded = jnp.concatenate([g[:, LANES * h:LANES * h + LANES], jnp.zeros((SEVEN, LANES), F32)], axis=ZERO)
        x = skew(lax.dot_general(padded, perm.astype(F32), (((ONE,), (ONE,)), ((), ())), precision=lax.Precision.HIGHEST, preferred_element_type=F32), s, False)

        def place_row(r, carry):
            flat[pl.ds(ROW_T2 + TOKENS * h + r, ONE), :] = jnp.sum(jnp.where(row == r, x, F_ZERO), axis=ZERO, keepdims=True)
            return carry
        lax.fori_loop(ZERO, TOKENS, place_row, ZERO)
    flat[ROW_VEC:FLAT_ROWS + SIXTEEN, :] = jnp.zeros((FLAT_ROWS + SIXTEEN - ROW_VEC, LANES), F32)
    for n in range(TWO):
        v = jnp.sum(gsum[n], axis=ZERO, keepdims=True)
        for k in range(FOUR):
            flat[ROW_VEC + FOUR * n + k:ROW_VEC + FOUR * n + k + ONE, :] = v[:, LANES * k:LANES * k + LANES]
    t = jnp.sum(rowsum[...].T, axis=ZERO, keepdims=True)
    t = t[:, ZERO:TH] + t[:, TH:TWO * TH] + t[:, TWO * TH:THREE * TH] + t[:, THREE * TH:FOUR * TH]
    for h in range(TWO):
        flat[ROW_VEC + EIGHT + h:ROW_VEC + NINE + h, :] = t[:, LANES * h:LANES * h + LANES]
    v2[...] = jnp.zeros_like(v2)
    lists = [(jnp.sum(gsum[TWO], axis=ZERO, keepdims=True), ZERO, FOUR), (jnp.sum(gsum[THREE], axis=ZERO, keepdims=True), FOUR, FOUR), (jnp.sum(gb1[...], axis=ZERO, keepdims=True), EIGHT, SIXTEEN), (jnp.sum(gsum[FOUR], axis=ZERO, keepdims=True), TWENTY_FOUR, FOUR)]
    for v, first, count in lists:
        for k in range(count):
            v2[first + k:first + k + ONE, :] = v[:, LANES * k:LANES * k + LANES]
    turned = pltpu.roll(v2[...], TOKENS, ONE)
    t = jnp.broadcast_to(jnp.sum(colsum[...].T, axis=ZERO, keepdims=True), (STEP8, TWO * LANES))
    b2 = t
    for i in range(ONE, FOUR):
        b2 = b2 + pltpu.roll(t, TWO * LANES - TOKENS * i, ONE)
    before = jnp.concatenate([b2[ZERO:ONE, ZERO:LANES], turned[ZERO:LAST_IMAGE, :]], axis=ZERO)
    merged = jnp.where(iota((IMAGES, LANES), ONE) < TOKENS, before, turned)
    flat[ROW_VEC + TEN:ROW_VEC + 42, :] = merged


def sum_images(acc):
    g = acc[ZERO:TOKENS, ZERO:TH]
    for i in range(ONE, FOUR):
        g = g + acc[TOKENS * i:TOKENS * i + TOKENS, TH * i:TH * i + TH]
    return g


def no_hook(k):
    return None


def at(table):
    def hook(k):
        for key, act in table.items():
            if isinstance(k, int):
                if key == k:
                    act()
            elif key >= ZERO:
                pl.when(k == key)(act)
    return hook


def both(*acts):
    def run():
        for act in acts:
            act()
    return run


def step_kernel(x0, labels, pack, own, stat, gath, x1, x2, x3, d, dn2, n2, dbf, n2t, dt, mix, ma1, mb1, ma2, mb2, col, vrow, v2, bd, srow, pool, gsum, gb1, acc2, rowsum, colsum, flat, w1, w2, slab, head, small, leaving, t0, t1, t2, t3, box, ag_send, ag_recv, rs_send, rs_recv, stage_sem, load_sem, tiny_send, tiny_recv, late_send, late_recv, done, late, late_box):
    where = place()
    me, coords, core, neighbours, partner = where
    def go(work, phase):
        def run():
            with jax.named_scope('hook_rs'):
                work.step(phase)
        return run

    load = pltpu.make_async_copy(pack, gath.at[coords[ZERO], coords[ONE], coords[TWO], core], load_sem)
    load.start()
    with jax.named_scope('barrier'):
        enter_barrier(me)
    load.wait()
    first = Gather(gath, where, ((ZERO, 352), (352, 352), (704, 336)), ag_send, ag_recv, ZERO)
    rest = Gather(gath, where, ((1040, 448), (1488, 432), (1920, 432)), ag_send, ag_recv, 21)
    first.start()
    for phase in range(THREE):
        with jax.named_scope('ag_step'):
            first.step(phase)
    rest.start()
    with jax.named_scope('ag_finish'):
        first.finish()
    mats = (ma1, mb1, ma2, mb2, col)
    with jax.named_scope('unflatten'):
        unflatten_layer(gath, ZERO, flat, (x3, n2, dbf, mix), stage_sem, w1, w2, slab)
    with jax.named_scope('prep'):
        prep_layer(ZERO, slab, vrow, bd, v2, *mats)
    uq, dq = mix.at[ZERO:FOUR * TH, :], mix.at[FOUR * TH:EIGHT * TH, :]
    uch = mix.at[FOUR * TH:FOUR * TH + FOUR * QROWS, :]
    uh, dh = mix.at[ZERO:ALL_ROWS, ZERO:CHUNK], mix.at[ZERO:ALL_ROWS, CHUNK:TWO * CHUNK]
    acc1 = bd.at[ZERO:QROWS, :]
    with jax.named_scope('forward'):
        forward_layer(ZERO, x0, x1, x2, vrow, ma1, ma2, col, w1, w2, uq, uch, at({ONE: go(rest, ZERO), THREE: go(rest, ONE), SEVEN: go(rest, TWO)}))
    with jax.named_scope('rest_finish'):
        rest.finish()
    with jax.named_scope('unflatten'):
        unflatten_layer(gath, ONE, flat, (x3, n2, dbf, mix), stage_sem, w1, w2, slab)
    with jax.named_scope('unflatten_head'):
        unflatten_head(gath, (x3, n2, dbf, mix), stage_sem, head, small)
    with jax.named_scope('prep'):
        prep_layer(ONE, slab, vrow, bd, v2, *mats)
    with jax.named_scope('forward'):
        forward_layer(ONE, x2, x3, n2, vrow, ma1, ma2, col, w1, w2, uq, uch, no_hook)
    with jax.named_scope('head'):
        head_pass(n2, labels, small, head, d, pool, srow, gsum, flat)

    bufs, sems = (leaving, t0, t1, t2, t3), (rs_send, rs_recv)
    thirds = ((ZERO, 352), (352, 352), (704, 336))
    reduces = [Reduce(flat, HEAD_ROWS, HEAD_ROWS, ((ZERO, 96), (96, 88), (184, 88)), own, HEAD_OFF, bufs, where, sems)]
    reduces += [Reduce(flat, SHARD_ROWS, SLOT_ROWS, thirds, own, l * SLOT_ROWS, bufs, where, sems) for l in (ONE, ZERO)]

    def done_one(work):
        def run():
            work.finish()
            for other in list(neighbours) + [partner]:
                pl.semaphore_signal(done, inc=ONE, device_id=(other,), device_id_type=MESH_ID)
        return run

    h, r1, r0 = reduces
    back = (d, vrow, w1, w2, n2, dbf, n2t, dt, uh, dh, dn2, flat, gsum, gb1)
    tok = (d, vrow, dn2, ma1, mb1, ma2, mb2, uq, dq, acc1, acc2, rowsum, colsum, gsum)
    small_parts = (flat, acc1, acc2, rowsum, colsum, gsum, gb1, v2)
    with jax.named_scope('rs_start_head'):
        h.start()
    with jax.named_scope('channel_back'):
        channel_back(ONE, x3, *back, at({-ONE: go(h, ZERO), ONE: go(h, ONE), TWO: go(h, TWO), FOUR: both(go(h, THREE), done_one(h))}))
    with jax.named_scope('token_back'):
        token_back(ONE, x2, x3, *tok, no_hook)
    with jax.named_scope('small_flat'):
        small_flat(ONE, *small_parts)
    with jax.named_scope('done_wait'):
        pl.semaphore_wait(done, FOUR)
    with jax.named_scope('rs_start'):
        r1.start()
    with jax.named_scope('channel_back'):
        channel_back(ZERO, x1, *back, at({-ONE: go(r1, ZERO), FOUR: go(r1, ONE), SIX: go(r1, TWO)}))
    with jax.named_scope('rs_step'):
        r1.step(THREE)
    done_one(r1)()
    with jax.named_scope('done_wait'):
        pl.semaphore_wait(done, FOUR)
    with jax.named_scope('rs_start'):
        r0.start()
    with jax.named_scope('token_back'):
        token_back(ZERO, x0, x1, *tok, at({TWO: go(r0, ZERO)}))
    with jax.named_scope('small_flat'):
        small_flat(ZERO, *small_parts)
    late[ZERO, ZERO:QVALID, :] = flat[ZERO:QVALID, :]
    late[ZERO, QVALID:240, :] = flat[ROW_VEC:FLAT_ROWS, :]
    hops = [partner, neighbours[TWO], neighbours[ONE], neighbours[ZERO]]

    def exchange(value, box_ref, sems, n):
        return pltpu.make_async_remote_copy(src_ref=value.at[n % TWO], dst_ref=box_ref.at[n], send_sem=sems[ZERO].at[n], recv_sem=sems[ONE].at[n], device_id=(hops[n],), device_id_type=MESH_ID)

    def late_copy(n):
        return exchange(late, late_box, (late_send, late_recv), n)
    late_copy(ZERO).start()
    with jax.named_scope('rs_step'):
        r0.step(ONE)
    for n in range(FOUR):
        with jax.named_scope('late_wait'):
            late_copy(n).wait()
        late[(n + ONE) % TWO] = late[n % TWO] + late_box[n]
        if n < THREE:
            late_copy(n + ONE).start()
        if n == TWO:
            with jax.named_scope('rs_step'):
                r0.step(TWO)
    with jax.named_scope('rs_step'):
        r0.step(THREE)
    r0.finish()
    own[ZERO:QVALID, :] = jnp.where(me == ZERO, late[ZERO, ZERO:QVALID, :], own[ZERO:QVALID, :])
    last = ROW_VEC - 15 * SHARD_ROWS
    own[last:SHARD_ROWS, :] = jnp.where(me == 15, late[ZERO, QVALID:240, :], own[last:SHARD_ROWS, :])
    for l in range(TWO):
        own[l * SLOT_ROWS + SHARD_ROWS:l * SLOT_ROWS + SLOT_ROWS, :] = jnp.zeros((ONE, LANES), F32)
    box[me] = jnp.broadcast_to(jnp.sum(square_sum(own, ZERO, SMALL_OFF + EIGHT)), (STEP8, LANES))

    def tell(k):
        return pltpu.make_async_remote_copy(src_ref=box.at[me], dst_ref=box.at[me], send_sem=tiny_send.at[k], recv_sem=tiny_recv.at[k], device_id=((me + k) % DEVICES,), device_id_type=MESH_ID)
    for k in range(ONE, DEVICES):
        tell(k).start()
    for k in range(ONE, DEVICES):
        with jax.named_scope('norm_wait'):
            tell(k).wait()
    total = box[ZERO]
    for k in range(ONE, DEVICES):
        total = total + box[k]
    stat[ZERO] = total
    stat[ONE] = own[SMALL_OFF + EIGHT:SMALL_OFF + SIXTEEN, :]


def train_step(x0, labels, pack):
    vmem = pl.BlockSpec(memory_space=pltpu.VMEM)
    act = pltpu.VMEM((ALL_ROWS, CH), BF16)
    wide = pltpu.VMEM((ALL_ROWS, CH), F32)
    across = pltpu.VMEM((CH, ALL_ROWS), BF16)
    tall = pltpu.VMEM((TWO, FOUR * TH, QROWS), BF16)
    flat_mat = pltpu.VMEM((TWO, QROWS, FOUR * TH), BF16)
    acc = pltpu.VMEM((QROWS, FOUR * TH), F32)
    dma = pltpu.SemaphoreType.DMA
    return pl.pallas_call(
        step_kernel,
        out_shape=(jax.ShapeDtypeStruct((AG_ROWS, LANES), F32), jax.ShapeDtypeStruct((TWO, STEP8, LANES), F32), jax.ShapeDtypeStruct((TWO, TWO, TWO, TWO, AG_ROWS, LANES), BF16)),
        in_specs=[vmem] * THREE,
        out_specs=(vmem, vmem, pl.BlockSpec(memory_space=pl.ANY)),
        scratch_shapes=[act, act, act, wide, wide, act, act, across, across, pltpu.VMEM((EIGHT * TH, CH), BF16),
                        tall, flat_mat, flat_mat, tall, pltpu.VMEM((TWO, QROWS, LANES), F32), pltpu.VMEM((TWO, STEP8, HID), F32), pltpu.VMEM((IMAGES, LANES), F32), pltpu.VMEM((TWO * LANES, FOUR * TH), F32),
                        pltpu.VMEM((STEP8, CLASS_PAD), F32), pltpu.VMEM((IMAGES, CH), F32), pltpu.VMEM((FIVE, STEP8, CH), F32), pltpu.VMEM((STEP8, HID), F32), acc,
                        pltpu.VMEM((FOUR * TH, LANES), F32), pltpu.VMEM((TWO * LANES, LANES), F32), pltpu.VMEM((FLAT_ROWS + SIXTEEN, LANES), F32),
                        pltpu.VMEM((TWO, CH, HID), BF16), pltpu.VMEM((TWO, HID, CH), BF16), pltpu.VMEM((TWO, SLAB_ROWS, LANES), F32), pltpu.VMEM((CH, CLASS_PAD), BF16), pltpu.VMEM((SIXTEEN, LANES), F32),
                        pltpu.VMEM((TWO, TWO, TWO, SLOT_ROWS, LANES), F32), pltpu.VMEM((TWO, TWO, TWO, SLOT_ROWS, LANES), F32), pltpu.VMEM((TWO, TWO, SLOT_ROWS, LANES), F32), pltpu.VMEM((TWO, SLOT_ROWS, LANES), F32), pltpu.VMEM((SLOT_ROWS, LANES), F32),
                        pltpu.VMEM((DEVICES, STEP8, LANES), F32),
                        dma((42,)), dma((42,)), dma((12,)), dma((12,)), dma((SIXTEEN,)), dma, dma((DEVICES,)), dma((DEVICES,)), dma((FOUR,)), dma((FOUR,)), pltpu.SemaphoreType.REGULAR, pltpu.VMEM((TWO, SLAB_ROWS, LANES), F32), pltpu.VMEM((FOUR, SLAB_ROWS, LANES), F32)],
        compiler_params=pltpu.CompilerParams(collective_id=ZERO, has_side_effects=True, vmem_limit_bytes=67043328),
        name='train_step',
    )(x0, labels, pack)


LEARN_RATE = 0.003
BETA_ONE = 0.9
BETA_TWO = 0.999
ADAM_EPS = 1e-8
WEIGHT_DECAY = 0.03
ADAM_STEP = 10


def adam_update(master, gradient, moment, second, decay_rate):
    moment_new = BETA_ONE * moment + (F_ONE - BETA_ONE) * gradient
    second_new = BETA_TWO * second + (F_ONE - BETA_TWO) * gradient * gradient
    m_hat = moment_new / (F_ONE - BETA_ONE ** ADAM_STEP)
    v_hat = second_new / (F_ONE - BETA_TWO ** ADAM_STEP)
    master_new = master - LEARN_RATE * (m_hat / (jnp.sqrt(v_hat) + ADAM_EPS) + decay_rate * master)
    return master_new, moment_new, second_new

def adam_kernel(lp, lm, lv, hp, hm, hv, sp, sm, sv, own, stat, lp_o, lm_o, lv_o, hp_o, hm_o, hv_o, sp_o, sm_o, sv_o, loss, grad):
    step = pl.program_id(ZERO)
    clip = F_ONE / jnp.maximum(F_ONE, jnp.sqrt(stat[ZERO, ZERO:ONE, ZERO:ONE]))
    for l in range(TWO):
        for r in range(UPDATE_ROWS):
            grad[l:l + ONE, LANES * r:LANES * r + LANES] = own[pl.ds(l * SLOT_ROWS + UPDATE_ROWS * step + r, ONE), :]
    block = (TWO, UPDATE_ROWS * LANES)
    spot = iota(block, ONE) + (UPDATE_ROWS * LANES) * step + SHARD_ROWS * LANES * lax.axis_index('fsdp')
    decay = jnp.where(spot < ROW_VEC * LANES, WEIGHT_DECAY, F_ZERO)
    lp_o[...], lm_o[...], lv_o[...] = adam_update(lp[...], grad[...] * clip, lm[...], lv[...], decay)

    @pl.when(step == ZERO)
    def _():
        for j in range(EIGHT):
            lanes = slice(LANES * j, min(LANES * j + LANES, CLASSES))
            g = own[HEAD_OFF + IMAGES * j:HEAD_OFF + IMAGES * j + IMAGES, ZERO:lanes.stop - lanes.start] * clip
            hp_o[:, lanes], hm_o[:, lanes], hv_o[:, lanes] = adam_update(hp[:, lanes], g, hm[:, lanes], hv[:, lanes], WEIGHT_DECAY)
        sp_o[...], sm_o[...], sv_o[...] = adam_update(sp[...], own[SMALL_OFF:SMALL_OFF + ONE, :] * clip, sm[...], sv[...], F_ZERO)
        loss[...] = stat[ONE] / GLOBAL_IMAGES


def update(lp, lm, lv, hp, hm, hv, sp, sm, sv, own, stat):
    piece = pl.BlockSpec((TWO, UPDATE_ROWS * LANES), lambda i: (ZERO, i))

    def whole(x):
        return pl.BlockSpec(x.shape, lambda i: (ZERO,) * x.ndim)
    tile = jax.ShapeDtypeStruct((STEP8, LANES), F32)
    return pl.pallas_call(
        adam_kernel,
        grid=(pl.cdiv(SHARD_ROWS, UPDATE_ROWS),),
        out_shape=tuple(jax.ShapeDtypeStruct(x.shape, F32) for x in (lp, lm, lv, hp, hm, hv, sp, sm, sv)) + (tile,),
        in_specs=[piece] * THREE + [whole(x) for x in (hp, hm, hv, sp, sm, sv, own, stat)],
        out_specs=(piece,) * THREE + tuple(whole(x) for x in (hp, hm, hv, sp, sm, sv, tile)),
        scratch_shapes=[pltpu.VMEM((TWO, UPDATE_ROWS * LANES), F32)],
        name='update',
    )(lp, lm, lv, hp, hm, hv, sp, sm, sv, own, stat)


def solution(mesh):
    row_spec = P('fsdp')
    layer_spec = P(None, 'fsdp')
    in_specs = (row_spec, row_spec, layer_spec, row_spec, row_spec, layer_spec, row_spec, row_spec, layer_spec, row_spec, row_spec)
    out_specs = (P(),) + in_specs[TWO:]

    def device_step(act_in, labels, layer_p, head_w, small_p, layer_m, head_m, small_m, layer_v, head_v, small_v):
        quads = jnp.pad(act_in.reshape(QUADS, QVALID, CH), ((ZERO, ZERO), (ZERO, QROWS - QVALID), (ZERO, ZERO))).reshape(ALL_ROWS, CH)
        layer_bf = jnp.pad(layer_p.astype(BF16).reshape(TWO, SHARD_ROWS, LANES), ((ZERO, ZERO), (ZERO, ONE), (ZERO, ZERO)))
        head_bf = jnp.pad(head_w.astype(BF16), ((ZERO, ZERO), (ZERO, CLASS_PAD - CLASSES))).reshape(IMAGES, EIGHT, LANES).transpose(ONE, ZERO, TWO).reshape(TH, LANES)
        small_bf = jnp.pad(small_p.astype(BF16).reshape(ONE, LANES), ((ZERO, 15), (ZERO, ZERO)))
        pack = jnp.concatenate([layer_bf.reshape(TWO * SLOT_ROWS, LANES), head_bf, small_bf])
        own, stat, _ = train_step(quads, jnp.broadcast_to(labels[:, None], (IMAGES, LANES)), pack)
        flat_small = [x.reshape(ONE, LANES) for x in (small_p, small_m, small_v)]
        new_lp, new_lm, new_lv, new_hw, new_hm, new_hv, new_sp, new_sm, new_sv, loss = update(layer_p, layer_m, layer_v, head_w, head_m, head_v, *flat_small, own, stat)
        new_sp, new_sm, new_sv = [x.reshape(LANES) for x in (new_sp, new_sm, new_sv)]
        loss_value = loss[ZERO, ZERO]
        return (loss_value, new_lp, new_hw, new_sp, new_lm, new_hm, new_sm, new_lv, new_hv, new_sv)

    return jax.shard_map(device_step, mesh=mesh, in_specs=in_specs, out_specs=out_specs, check_vma=False)
```

```python
import functools
import math
import jax
import jax.numpy as jnp
from jax import lax
from jax.experimental import pallas as pl
from jax.experimental.pallas import tpu as pltpu
from jax.sharding import PartitionSpec as P

ZERO = 0
ONE = 1
TWO = 2
THREE = 3
FOUR = 4
FIVE = 5
SIX = 6
SEVEN = 7
EIGHT = 8
NINE = 9
SIXTEEN = 16
LANES = 128
IMAGES = 32
LAST_IMAGE = 31
CH = 512
CLASS_PAD = 1024
HID = 2048
TH = 256
F_ZERO = 0.0
F_ONE = 1.0
TWENTY_FOUR = 24
TOKEN_PAD = 56
QVALID = 196
SIXTY_FOUR = 64
TEN = 10
MESH_ID = pl.DeviceIdType.MESH
F32 = jnp.float32
BF16 = jnp.bfloat16

DEVICES = 16
SHARD_ROWS = 1039
UPDATE_ROWS = 130
SLOT_ROWS = 1040
ROW_C1 = 196
ROW_C2 = 8388
ROW_VEC = 16580
FLAT_ROWS = 16624
SLAB_ROWS = 240
HEAD_OFF = 2 * SLOT_ROWS
SMALL_OFF = HEAD_OFF + 256
AG_ROWS = SMALL_OFF + 16
HEAD_ROWS = 272
ORDERS = ((2, 1, 0), (1, 0, 2), (0, 2, 1))
AXIS_STEP = (8, 4, 2)


def place():
    me = lax.axis_index('fsdp')
    coords = [me // EIGHT, (me // FOUR) % TWO, (me // TWO) % TWO]
    core = me % TWO
    neighbours = [me + AXIS_STEP[a] - TWO * AXIS_STEP[a] * coords[a] for a in range(THREE)]
    partner = me + ONE - TWO * core
    return me, coords, core, neighbours, partner


def enter_barrier(me):
    barrier = pltpu.get_barrier_semaphore()
    for k in range(ONE, DEVICES):
        pl.semaphore_signal(barrier, inc=ONE, device_id=((me + k) % DEVICES,), device_id_type=MESH_ID)
    pl.semaphore_wait(barrier, DEVICES - ONE)


def slot_view(buf, coords, core, free_axes, row0, rows):
    index = [pl.ds(ZERO, TWO) if a in free_axes else coords[a] for a in range(THREE)]
    return buf.at[index[ZERO], index[ONE], index[TWO], core, pl.ds(row0, rows), :]


class Gather:
    def __init__(self, buf, where, row_groups, send_sem, recv_sem, sem0):
        self.buf, self.where, self.groups = buf, where, row_groups
        self.send_sem, self.recv_sem, self.sem0 = send_sem, recv_sem, sem0
        self.pending = []

    def copy(self, view, sem, device):
        return pltpu.make_async_remote_copy(src_ref=view, dst_ref=view, send_sem=self.send_sem.at[self.sem0 + sem], recv_sem=self.recv_sem.at[self.sem0 + sem], device_id=(device,), device_id_type=MESH_ID)

    def link(self, group, phase):
        me, coords, core, neighbours, partner = self.where
        order = ORDERS[group]
        row0, rows = self.groups[group]
        view = slot_view(self.buf, coords, core, order[:phase], row0, rows)
        return self.copy(view, group * THREE + phase, neighbours[order[phase]])

    def chip(self, group, phase):
        me, coords, core, neighbours, partner = self.where
        order = ORDERS[group]
        row0, rows = self.groups[group]
        if phase < ZERO:
            view = slot_view(self.buf, coords, core, (), row0, rows)
        else:
            far = list(coords)
            far[order[phase]] = ONE - coords[order[phase]]
            view = slot_view(self.buf, far, core, order[:phase], row0, rows)
        return self.copy(view, NINE + group * FOUR + phase + ONE, partner)

    def start(self):
        for group in range(THREE):
            self.link(group, ZERO).start()
        for group in range(THREE):
            self.chip(group, -ONE).start()

    def step(self, phase):
        for group in range(THREE):
            self.link(group, phase).wait_recv()
            if phase < TWO:
                self.link(group, phase + ONE).start()
            self.chip(group, phase).start()

    def finish(self):
        for group in range(THREE):
            for phase in range(-ONE, THREE):
                self.chip(group, phase).wait()
            for phase in range(THREE):
                self.link(group, phase).wait_send()


def slot_of(dev):
    return dev // EIGHT, (dev // FOUR) % TWO, (dev // TWO) % TWO, dev % TWO


def fetch_layer(gath, layer, bays, stage_sem):
    copies = []
    for dev in range(SIXTEEN):
        z, y, x, core = slot_of(dev)
        land = bays[dev // FOUR].at[pl.ds(ZERO, SLOT_ROWS), pl.ds(LANES * (dev % FOUR), LANES)]
        copies.append(pltpu.make_async_copy(gath.at[z, y, x, core, pl.ds(layer * SLOT_ROWS, SLOT_ROWS), :], land, stage_sem.at[dev]))
    for copy in copies:
        copy.start()
    return copies


def unflatten_layer(gath, layer, flat, bays, stage_sem, w1_ref, w2_ref, slab_ref):
    copies = fetch_layer(gath, layer, bays, stage_sem)
    for dev in range(SIXTEEN):
        copies[dev].wait()

        def chunk(k, inner):
            block = bays[dev // FOUR][pl.ds(pl.multiple_of(SIXTEEN * k, SIXTEEN), SIXTEEN), LANES * (dev % FOUR):LANES * (dev % FOUR) + LANES]
            flat[pl.ds(dev * SHARD_ROWS + SIXTEEN * k, SIXTEEN), :] = block.astype(F32)
            return inner
        lax.fori_loop(ZERO, SLOT_ROWS // SIXTEEN, chunk, ZERO, unroll=FIVE)

    def first(rb, carry):
        for j in range(SIXTEEN):
            block = flat[pl.ds(ROW_C1 + TH * rb + j, SIXTEEN, stride=SIXTEEN), :]
            w1_ref[layer, pl.ds(pl.multiple_of(SIXTEEN * rb, SIXTEEN), SIXTEEN), LANES * j:LANES * j + LANES] = block.astype(BF16)
        return carry
    lax.fori_loop(ZERO, IMAGES, first, ZERO)

    def second(rb, carry):
        for j in range(FOUR):
            block = flat[pl.ds(ROW_C2 + SIXTY_FOUR * rb + j, SIXTEEN, stride=FOUR), :]
            w2_ref[layer, pl.ds(pl.multiple_of(SIXTEEN * rb, SIXTEEN), SIXTEEN), LANES * j:LANES * j + LANES] = block.astype(BF16)
        return carry
    lax.fori_loop(ZERO, LANES, second, ZERO, unroll=FOUR)
    slab_ref[layer, ZERO:QVALID, :] = flat[ZERO:QVALID, :]
    slab_ref[layer, QVALID:240, :] = flat[ROW_VEC:FLAT_ROWS, :]


def unflatten_head(gath, bays, stage_sem, head_ref, small_ref):
    copies = []
    for dev in range(SIXTEEN):
        z, y, x, core = slot_of(dev)
        copies.append(pltpu.make_async_copy(gath.at[z, y, x, core, pl.ds(HEAD_OFF, HEAD_ROWS), :], bays[dev // FOUR].at[pl.ds(ZERO, HEAD_ROWS), pl.ds(LANES * (dev % FOUR), LANES)], stage_sem.at[dev]))
    for copy in copies:
        copy.start()
    for dev in range(SIXTEEN):
        copies[dev].wait()
        lanes = slice(LANES * (dev % FOUR), LANES * (dev % FOUR) + LANES)
        for j in range(EIGHT):
            head_ref[IMAGES * dev:IMAGES * dev + IMAGES, LANES * j:LANES * j + LANES] = bays[dev // FOUR][IMAGES * j:IMAGES * j + IMAGES, lanes]
        small_ref[dev:dev + ONE, :] = bays[dev // FOUR][TH:272, lanes].astype(F32)[ZERO:ONE, :]


class Reduce:
    def __init__(self, flat, pitch, rows, groups, out, out_row, bufs, where, sems):
        self.flat, self.pitch, self.rows, self.groups, self.out, self.out_row = flat, pitch, rows, groups, out, out_row
        self.leaving, self.temps = bufs[ZERO], bufs[ONE:]
        self.where = where
        self.send_sem, self.recv_sem = sems

    def spread(self):
        me, coords, core, neighbours, partner = self.where

        def chunk(k, carry):
            for n in range(EIGHT):
                self.leaving[n // FOUR, (n // TWO) % TWO, n % TWO, pl.ds(pl.multiple_of(EIGHT * k, EIGHT), EIGHT), :] = self.flat[pl.ds(self.pitch * (TWO * n + ONE - core) + EIGHT * k, EIGHT), :]
            return carry
        lax.fori_loop(ZERO, self.rows // EIGHT, chunk, ZERO)

    def views(self, group, phase):
        me, coords, core, neighbours, partner = self.where
        row0, rows = self.groups[group]
        order = ORDERS[group]
        if phase == ZERO:
            free = (ZERO, ONE, TWO)
            leave = self.leaving.at[:, :, :, pl.ds(row0, rows), :]
            device = partner
        else:
            axis = order[phase - ONE]
            free = tuple(a for a in range(THREE) if a in order[phase:])
            index = [pl.ds(ZERO, TWO) if a in free else coords[a] for a in range(THREE)]
            index[axis] = ONE - coords[axis]
            leave = self.temps[ZERO].at[index[ZERO], index[ONE], index[TWO], pl.ds(row0, rows), :]
            device = neighbours[axis]
        land = self.temps[phase].at[(slice(None),) * len(free) + (pl.ds(row0, rows), slice(None))]
        return leave, land, device, free

    def copy(self, group, phase):
        leave, land, device, free = self.views(group, phase)
        sem = group * FOUR + phase
        return pltpu.make_async_remote_copy(src_ref=leave, dst_ref=land, send_sem=self.send_sem.at[sem], recv_sem=self.recv_sem.at[sem], device_id=(device,), device_id_type=MESH_ID)

    def add(self, group, phase):
        me, coords, core, neighbours, partner = self.where
        free = self.views(group, phase)[THREE]
        row0, rows = self.groups[group]
        total, temp = self.temps[ZERO], self.temps[phase]
        count = TWO ** len(free)
        per = max(ONE, EIGHT // count)
        while rows % (EIGHT * per):
            per //= TWO

        def chunk(k, carry):
            for part in range(per):
                start = pl.multiple_of(row0 + EIGHT * (per * k + part), EIGHT)
                for n in range(count):
                    index = list(coords)
                    bits = []
                    for pos, a in enumerate(free):
                        bit = (n // TWO ** (len(free) - ONE - pos)) % TWO
                        index[a] = bit
                        bits.append(bit)
                    target = (index[ZERO], index[ONE], index[TWO], pl.ds(start, EIGHT), slice(None))
                    if phase == ZERO:
                        value = total[target] + self.flat[pl.ds(self.pitch * (TWO * n + core) + start, EIGHT), :]
                    else:
                        value = total[target] + temp[tuple(bits) + (pl.ds(start, EIGHT), slice(None))]
                    if phase == THREE:
                        self.out[pl.ds(pl.multiple_of(self.out_row + start, EIGHT), EIGHT), :] = value
                    else:
                        total[target] = value
            return carry
        lax.fori_loop(ZERO, rows // (EIGHT * per), chunk, ZERO)

    def start(self):
        self.spread()
        for group in range(THREE):
            self.copy(group, ZERO).start()

    def step(self, phase):
        for group in range(THREE):
            self.copy(group, phase).wait_recv()
            self.add(group, phase)
            if phase < THREE:
                self.copy(group, phase + ONE).start()

    def finish(self):
        for group in range(THREE):
            for phase in range(FOUR):
                self.copy(group, phase).wait_send()


def square_sum(ref, row0, rows):
    def chunk(k, total):
        block = ref[pl.ds(pl.multiple_of(row0 + EIGHT * k, EIGHT), EIGHT), :]
        return total + block * block
    return lax.fori_loop(ZERO, rows // EIGHT, chunk, jnp.zeros((EIGHT, LANES), F32), unroll=TWO)


QUADS = 8
QROWS = 208
TOKENS = 49
ALL_ROWS = QUADS * QROWS
CHUNK = 256
BLOCK = 416
TOK_ROWS = 256
TOK_LANES = 256
FWD_ROWS = 256
FWD_LANES = 512
CLASSES = 1000
GLOBAL_IMAGES = 512.0
LN_EPS = 1e-6
GELU_A = 0.7978845608028654
GELU_B = GELU_A * 0.044715
HALF = 0.5
ROW_T2 = 98
INV49 = 81
LOW7 = 127
SLAB_VEC = 196
V_BT1 = 204
V_MIS = 206
STEP8 = 8


def mm(a, b):
    return jnp.dot(a, b, preferred_element_type=F32)


def mm_nt(a, b):
    return lax.dot_general(a, b, (((ONE,), (ONE,)), ((), ())), preferred_element_type=F32)


def iota(shape, axis):
    return lax.broadcasted_iota(jnp.int32, shape, axis)


def aligned(start, unit):
    return pl.multiple_of(start * unit, unit)


def stats(x):
    mean = jnp.mean(x, axis=-ONE, keepdims=True)
    centered = x - mean
    scale = lax.rsqrt(jnp.mean(centered * centered, axis=-ONE, keepdims=True) + LN_EPS)
    return centered * scale, scale


def fold8(x):
    return jnp.sum(x.reshape(x.shape[ZERO] // STEP8, STEP8, x.shape[ONE]), axis=ZERO)


def gelu_tanh(h):
    sq = h * h
    return sq, jnp.tanh(h * (GELU_A + GELU_B * sq))


def gelu(h):
    sq, t = gelu_tanh(h)
    half = HALF * h
    return (half + half * t).astype(BF16)


def gelu_both(h):
    sq, t = gelu_tanh(h)
    side = HALF + HALF * t
    u = h * side
    return u.astype(BF16), side + (u - u * t) * (GELU_A + (3.0 * GELU_B) * sq)


def norm_back(xh, scale, gain, dy):
    dxh = dy * gain
    return scale * (dxh - jnp.mean(dxh, axis=-ONE, keepdims=True) - xh * jnp.mean(dxh * xh, axis=-ONE, keepdims=True))


def token_maps():
    s = iota((TOKEN_PAD, LANES), ZERO)
    lane = iota((TOKEN_PAD, LANES), ONE)
    j = ((lane - s) * INV49) & LOW7
    row = jnp.where(s < TOKENS, (j * TOKENS + s) >> SEVEN, -ONE)
    perm = (iota((LANES, LANES), ZERO) == ((iota((LANES, LANES), ONE) * TOKENS) & LOW7))
    return s, row, perm


def skew(x, s, left):
    for bit in range(SEVEN):
        amount = TWO ** bit
        x = jnp.where(((s >> bit) & ONE) == ONE, pltpu.roll(x, LANES - amount if left else amount, ONE), x)
    return x


def prep_layer(l, slab, vrow, bd, v2, ma1, mb1, ma2, mb2, col):
    for k in range(FOUR):
        lanes = slice(LANES * k, LANES * k + LANES)
        vrow[l, ZERO:ONE, lanes] = slab[l, SLAB_VEC + k:SLAB_VEC + k + ONE, :]
        vrow[l, ONE:TWO, lanes] = slab[l, SLAB_VEC + FOUR + k:SLAB_VEC + FIVE + k, :]
    lane = iota((IMAGES, LANES), ONE)
    cut = LANES - TOKENS
    v2[...] = jnp.where(lane < cut, pltpu.roll(slab[l, V_MIS:V_MIS + IMAGES, :], cut, ONE), pltpu.roll(slab[l, V_MIS + ONE:V_MIS + 33, :], cut, ONE))
    for row, first, count in ((TWO, ZERO, FOUR), (THREE, FOUR, FOUR), (FOUR, EIGHT, SIXTEEN), (FIVE, TWENTY_FOUR, FOUR)):
        for k in range(count):
            vrow[l, row:row + ONE, LANES * k:LANES * k + LANES] = v2[first + k:first + k + ONE, :]
    bd[...] = jnp.zeros_like(bd)
    for h in range(TWO):
        w = slab[l, pl.ds(h, TOKENS, stride=TWO), :]
        for i in range(FOUR):
            bd[TOKENS * i:TOKENS * i + TOKENS, TH * i + LANES * h:TH * i + LANES * h + LANES] = w
    mb1[l] = bd[ZERO:QROWS, :].astype(BF16)
    for h in range(TWO):
        for i in range(FOUR):
            bd[QVALID:QVALID + ONE, TH * i + LANES * h:TH * i + LANES * h + LANES] = slab[l, V_BT1 + h:V_BT1 + h + ONE, :]
    ma1[l] = bd[...].T[:, ZERO:QROWS].astype(BF16)
    bd[...] = jnp.zeros_like(bd)
    s, row, perm = token_maps()
    for h in range(TWO):
        def pick(r, acc):
            return jnp.where(row == r, slab[l, pl.ds(ROW_T2 + TOKENS * h + r, ONE), :], acc)
        x = skew(lax.fori_loop(ZERO, TOKENS, pick, jnp.zeros((TOKEN_PAD, LANES), F32)), s, True)
        w = mm(x.astype(BF16), perm.astype(BF16))[ZERO:TOKENS]
        for i in range(FOUR):
            bd[TOKENS * i:TOKENS * i + TOKENS, TH * i + LANES * h:TH * i + LANES * h + LANES] = w
    ma2[l] = bd[ZERO:QROWS, :].astype(BF16)
    mb2[l] = bd[...].T[:, ZERO:QROWS].astype(BF16)
    bias = jnp.where(iota((ONE, LANES), ONE) < TOKENS, slab[l, V_MIS:V_MIS + ONE, :], F_ZERO)
    wide = jnp.concatenate([jnp.broadcast_to(bias, (LANES, LANES)), jnp.zeros((LANES, LANES), F32)], axis=ONE)
    spread = wide
    for i in range(ONE, FOUR):
        spread = spread + pltpu.roll(wide, TOKENS * i, ONE)
    col[l] = spread.T[ZERO:QROWS, :]


def forward_layer(l, x_in, x_mid, x_out, vrow, ma1, ma2, col, w1, w2, uq, uch, hook):
    def quad(q, carry):
        hook(q)
        rows = pl.ds(aligned(q, QROWS), QROWS)
        xq = x_in[rows, :].astype(F32)
        n = token_input(xq, vrow, l)[TWO]
        for lane0 in range(ZERO, CH, FWD_LANES):
            for row0 in range(ZERO, FOUR * TH, FWD_ROWS):
                uq[row0:row0 + FWD_ROWS, lane0:lane0 + FWD_LANES] = gelu(mm(ma1[l, row0:row0 + FWD_ROWS, :], n[:, lane0:lane0 + FWD_LANES]))
        y = mm(ma2[l], uq[...])
        x1 = (xq + (y + jnp.concatenate([col[l]] * FOUR, axis=ONE))).astype(BF16)
        x_mid[rows, :] = x1
        x1 = x1.astype(F32)
        n2 = (stats(x1)[ZERO] * vrow[l, TWO:THREE, ZERO:CH] + vrow[l, THREE:FOUR, ZERO:CH]).astype(BF16)
        for c in range(FOUR):
            lanes = slice(CH * c, CH * c + CH)
            uch[QROWS * c:QROWS * c + QROWS, :] = gelu(mm(n2, w1[l, :, lanes]) + vrow[l, FOUR:FIVE, lanes])
        y = mm(uch[ZERO:QROWS, :], w2[l, ZERO:CH, :])
        for c in range(ONE, FOUR):
            y = y + mm(uch[QROWS * c:QROWS * c + QROWS, :], w2[l, CH * c:CH * c + CH, :])
        x_out[rows, :] = (x1 + (y + vrow[l, FIVE:SIX, ZERO:CH])).astype(BF16)
        return carry
    lax.fori_loop(ZERO, QUADS, quad, ZERO)


def token_input(xq, vrow, l):
    xh, scale = stats(xq)
    n = xh * vrow[l, ZERO:ONE, ZERO:CH] + vrow[l, ONE:TWO, ZERO:CH]
    return xh, scale, jnp.where(iota((QROWS, CH), ZERO) == QVALID, F_ONE, n).astype(BF16)


def image_of(shape, axis):
    c = iota(shape, axis)
    return jnp.where(c < QVALID, (c >= TOKENS).astype(jnp.int32) + (c >= TWO * TOKENS).astype(jnp.int32) + (c >= THREE * TOKENS).astype(jnp.int32), IMAGES)


def head_pass(x_out, labels, small, head, d, pool, srow, gsum, flat):
    for k in range(FOUR):
        lanes = slice(LANES * k, LANES * k + LANES)
        srow[ZERO:ONE, lanes] = small[k:k + ONE, :]
        srow[ONE:TWO, lanes] = small[FOUR + k:FIVE + k, :]
    for k in range(EIGHT):
        srow[TWO:THREE, LANES * k:LANES * k + LANES] = small[EIGHT + k:NINE + k, :]
    gain, shift = srow[ZERO:ONE, ZERO:CH], srow[ONE:TWO, ZERO:CH]
    pool[...] = jnp.zeros_like(pool)

    def quad(q, carry):
        xh, scale = stats(x_out[pl.ds(aligned(q, QROWS), QROWS), :].astype(F32))
        pick = (iota((IMAGES, QROWS), ZERO) == image_of((IMAGES, QROWS), ONE) + FOUR * q)
        pool[...] += mm(pick.astype(BF16), (xh * gain + shift).astype(BF16))
        return carry
    lax.fori_loop(ZERO, QUADS, quad, ZERO)
    pooled = (pool[...] / TOKENS).astype(BF16)
    real = iota((IMAGES, CLASS_PAD), ONE) < CLASSES
    logits = jnp.where(real, mm(pooled, head[...]) + srow[TWO:THREE, :], -1e30)
    top = jnp.max(logits, axis=-ONE, keepdims=True)
    log_norm = top + jnp.log(jnp.sum(jnp.exp(logits - top), axis=-ONE, keepdims=True))
    hit = iota((IMAGES, CLASS_PAD), ONE) == labels[:, ZERO:ONE]
    picked = jnp.sum(jnp.where(hit, logits, F_ZERO), axis=-ONE, keepdims=True)
    loss = jnp.broadcast_to(jnp.sum(log_norm - picked), (STEP8, LANES))
    d_logits = (jnp.exp(logits - log_norm) - hit.astype(F32)) / GLOBAL_IMAGES
    d_bf = d_logits.astype(BF16)
    g_head = mm(pool_t(pooled), d_bf)
    for n in range(SIXTEEN):
        for j in range(EIGHT):
            flat[HEAD_ROWS * n + IMAGES * j:HEAD_ROWS * n + IMAGES * j + IMAGES, :] = g_head[IMAGES * n:IMAGES * n + IMAGES, LANES * j:LANES * j + LANES]
        flat[HEAD_ROWS * n + TH:HEAD_ROWS * n + 264, :] = jnp.zeros((STEP8, LANES), F32)
        flat[HEAD_ROWS * n + 264:HEAD_ROWS * n + 272, :] = loss
    d_pool = (mm_nt(d_bf, head[...]) / TOKENS).astype(BF16)
    gsum[...] = jnp.zeros_like(gsum)

    def back(q, carry):
        rows = pl.ds(aligned(q, QROWS), QROWS)
        xh, scale = stats(x_out[rows, :].astype(F32))
        pick = (iota((QROWS, IMAGES), ONE) == image_of((QROWS, IMAGES), ZERO) + FOUR * q)
        dy = mm(pick.astype(BF16), d_pool)
        gsum[ZERO] += fold8(dy * xh)
        gsum[ONE] += fold8(dy)
        d[rows, :] = norm_back(xh, scale, gain, dy)
        return carry
    lax.fori_loop(ZERO, QUADS, back, ZERO)
    g_gain = jnp.sum(gsum[ZERO], axis=ZERO, keepdims=True)
    g_shift = jnp.sum(gsum[ONE], axis=ZERO, keepdims=True)
    g_bias = jnp.sum(d_logits, axis=ZERO, keepdims=True)
    for k in range(FOUR):
        lanes = slice(LANES * k, LANES * k + LANES)
        for row, value in ((HEAD_ROWS * k, g_gain), (HEAD_ROWS * (FOUR + k), g_shift)):
            flat[row + TH:row + 257, :] = value[:, lanes]
    for k in range(EIGHT):
        row = HEAD_ROWS * (EIGHT + k) + TH
        flat[row:row + ONE, :] = g_bias[:, LANES * k:LANES * k + LANES]


def pool_t(pooled):
    return pooled.astype(F32).T.astype(BF16)


def channel_back(l, x_mid, d, vrow, w1, w2, n2, dbf, n2t, dt, uh, dh, dn2, flat, gsum, gb1, hook):
    gsum[...] = jnp.zeros_like(gsum)
    gb1[...] = jnp.zeros_like(gb1)

    def quad(q, carry):
        rows = pl.ds(aligned(q, QROWS), QROWS)
        n2[rows, :] = (stats(x_mid[rows, :].astype(F32))[ZERO] * vrow[l, TWO:THREE, ZERO:CH] + vrow[l, THREE:FOUR, ZERO:CH]).astype(BF16)
        dq = d[rows, :]
        gsum[FOUR] += fold8(dq)
        dbf[rows, :] = dq.astype(BF16)
        dn2[rows, :] = jnp.zeros((QROWS, CH), F32)
        return carry
    lax.fori_loop(ZERO, QUADS, quad, ZERO)
    for k in range(ALL_ROWS // LANES):
        lanes = slice(LANES * k, LANES * k + LANES)
        n2t[:, lanes] = n2[lanes, :].T
        dt[:, lanes] = dbf[lanes, :].T
    hook(-ONE)

    def chunk(c, carry):
        hook(c)
        lanes = pl.ds(aligned(c, CHUNK), CHUNK)

        for b in range(ALL_ROWS // BLOCK):
            rows = slice(BLOCK * b, BLOCK * b + BLOCK)
            u, slope = gelu_both(mm(n2[rows, :], w1[l, :, lanes]) + vrow[l, FOUR:FIVE, lanes])
            uh[rows, :] = u
            dhid = mm_nt(dbf[rows, :], w2[l, lanes, :]).astype(BF16).astype(F32) * slope
            gb1[:, lanes] += fold8(dhid)
            dhid = dhid.astype(BF16)
            dh[rows, :] = dhid
            dn2[rows, :] += mm_nt(dhid, w1[l, :, lanes])
        g1 = mm(n2t[...], dh[...])
        for r in range(CH // STEP8):
            for k in range(TWO):
                flat[pl.ds(ROW_C1 + LANES * r + k + TWO * c, STEP8, stride=SIXTEEN), :] = g1[STEP8 * r:STEP8 * r + STEP8, LANES * k:LANES * k + LANES]
        g2 = mm(dt[...], uh[...]).T
        for r in range(CHUNK // STEP8):
            for k in range(FOUR):
                flat[pl.ds(ROW_C2 + FOUR * (STEP8 * r) + k + FOUR * CHUNK * c, STEP8, stride=FOUR), :] = g2[STEP8 * r:STEP8 * r + STEP8, LANES * k:LANES * k + LANES]
        return carry
    lax.fori_loop(ZERO, HID // CHUNK, chunk, ZERO)


def token_back(l, x_in, x_mid, d, vrow, dn2, ma1, mb1, ma2, mb2, uq, dq_ref, acc1, acc2, rowsum, colsum, gsum, hook):
    for ref in (acc1, acc2, rowsum, colsum):
        ref[...] = jnp.zeros_like(ref)

    def quad(q, carry):
        hook(q)
        rows = pl.ds(aligned(q, QROWS), QROWS)
        xh, scale = stats(x_mid[rows, :].astype(F32))
        dy = dn2[rows, :].astype(BF16).astype(F32)
        gsum[TWO] += fold8(dy * xh)
        gsum[THREE] += fold8(dy)
        d_after = norm_back(xh, scale, vrow[l, TWO:THREE, ZERO:CH], dy) + d[rows, :]
        part = d_after[:, ZERO:LANES]
        for k in range(ONE, FOUR):
            part = part + d_after[:, LANES * k:LANES * k + LANES]
        colsum[ZERO:QROWS, :] += part
        d_bf = d_after.astype(BF16)
        xh, scale, n = token_input(x_in[rows, :].astype(F32), vrow, l)
        for lane0 in range(ZERO, CH, TOK_LANES):
            lanes = slice(lane0, lane0 + TOK_LANES)
            for row0 in range(ZERO, FOUR * TH, TOK_ROWS):
                part = slice(row0, row0 + TOK_ROWS)
                u, slope = gelu_both(mm(ma1[l, part, :], n[:, lanes]))
                uq[part, lanes] = u
                dhid = mm(mb2[l, part, :], d_bf[:, lanes]).astype(BF16).astype(F32) * slope
                total = dhid[:, ZERO:LANES]
                for k in range(ONE, TOK_LANES // LANES):
                    total = total + dhid[:, LANES * k:LANES * k + LANES]
                rowsum[part, :] += total
                dq_ref[part, lanes] = dhid.astype(BF16)
        acc1[...] += mm_nt(n, dq_ref[...])
        acc2[...] += mm_nt(d_bf, uq[...])
        dy = mm(mb1[l], dq_ref[...]).astype(BF16).astype(F32)
        gsum[ZERO] += fold8(dy * xh)
        gsum[ONE] += fold8(dy)
        d[rows, :] = norm_back(xh, scale, vrow[l, ZERO:ONE, ZERO:CH], dy) + d_after
        return carry
    lax.fori_loop(ZERO, QUADS, quad, ZERO)


def small_flat(l, flat, acc1, acc2, rowsum, colsum, gsum, gb1, v2):
    g = sum_images(acc1)
    for h in range(TWO):
        flat[pl.ds(h, TOKENS, stride=TWO), :] = g[:, LANES * h:LANES * h + LANES]
    g = sum_images(acc2)
    s, row, perm = token_maps()
    for h in range(TWO):
        padded = jnp.concatenate([g[:, LANES * h:LANES * h + LANES], jnp.zeros((SEVEN, LANES), F32)], axis=ZERO)
        x = skew(lax.dot_general(padded, perm.astype(F32), (((ONE,), (ONE,)), ((), ())), precision=lax.Precision.HIGHEST, preferred_element_type=F32), s, False)

        def place_row(r, carry):
            flat[pl.ds(ROW_T2 + TOKENS * h + r, ONE), :] = jnp.sum(jnp.where(row == r, x, F_ZERO), axis=ZERO, keepdims=True)
            return carry
        lax.fori_loop(ZERO, TOKENS, place_row, ZERO)
    flat[ROW_VEC:FLAT_ROWS + SIXTEEN, :] = jnp.zeros((FLAT_ROWS + SIXTEEN - ROW_VEC, LANES), F32)
    for n in range(TWO):
        v = jnp.sum(gsum[n], axis=ZERO, keepdims=True)
        for k in range(FOUR):
            flat[ROW_VEC + FOUR * n + k:ROW_VEC + FOUR * n + k + ONE, :] = v[:, LANES * k:LANES * k + LANES]
    t = jnp.sum(rowsum[...].T, axis=ZERO, keepdims=True)
    t = t[:, ZERO:TH] + t[:, TH:TWO * TH] + t[:, TWO * TH:THREE * TH] + t[:, THREE * TH:FOUR * TH]
    for h in range(TWO):
        flat[ROW_VEC + EIGHT + h:ROW_VEC + NINE + h, :] = t[:, LANES * h:LANES * h + LANES]
    v2[...] = jnp.zeros_like(v2)
    lists = [(jnp.sum(gsum[TWO], axis=ZERO, keepdims=True), ZERO, FOUR), (jnp.sum(gsum[THREE], axis=ZERO, keepdims=True), FOUR, FOUR), (jnp.sum(gb1[...], axis=ZERO, keepdims=True), EIGHT, SIXTEEN), (jnp.sum(gsum[FOUR], axis=ZERO, keepdims=True), TWENTY_FOUR, FOUR)]
    for v, first, count in lists:
        for k in range(count):
            v2[first + k:first + k + ONE, :] = v[:, LANES * k:LANES * k + LANES]
    turned = pltpu.roll(v2[...], TOKENS, ONE)
    t = jnp.broadcast_to(jnp.sum(colsum[...].T, axis=ZERO, keepdims=True), (STEP8, TWO * LANES))
    b2 = t
    for i in range(ONE, FOUR):
        b2 = b2 + pltpu.roll(t, TWO * LANES - TOKENS * i, ONE)
    before = jnp.concatenate([b2[ZERO:ONE, ZERO:LANES], turned[ZERO:LAST_IMAGE, :]], axis=ZERO)
    merged = jnp.where(iota((IMAGES, LANES), ONE) < TOKENS, before, turned)
    flat[ROW_VEC + TEN:ROW_VEC + 42, :] = merged


def sum_images(acc):
    g = acc[ZERO:TOKENS, ZERO:TH]
    for i in range(ONE, FOUR):
        g = g + acc[TOKENS * i:TOKENS * i + TOKENS, TH * i:TH * i + TH]
    return g


def no_hook(k):
    return None


def at(table):
    def hook(k):
        for key, act in table.items():
            if isinstance(k, int):
                if key == k:
                    act()
            elif key >= ZERO:
                pl.when(k == key)(act)
    return hook


def both(*acts):
    def run():
        for act in acts:
            act()
    return run


def step_kernel(x0, labels, pack, own, stat, gath, x1, x2, x3, d, dn2, n2, dbf, n2t, dt, mix, ma1, mb1, ma2, mb2, col, vrow, v2, bd, srow, pool, gsum, gb1, acc2, rowsum, colsum, flat, w1, w2, slab, head, small, leaving, t0, t1, t2, t3, box, ag_send, ag_recv, rs_send, rs_recv, stage_sem, load_sem, tiny_send, tiny_recv, late_send, late_recv, done, late, late_box):
    where = place()
    me, coords, core, neighbours, partner = where
    load = pltpu.make_async_copy(pack, gath.at[coords[ZERO], coords[ONE], coords[TWO], core], load_sem)
    load.start()
    enter_barrier(me)
    load.wait()
    first = Gather(gath, where, ((ZERO, 352), (352, 352), (704, 336)), ag_send, ag_recv, ZERO)
    rest = Gather(gath, where, ((1040, 448), (1488, 432), (1920, 432)), ag_send, ag_recv, 21)
    first.start()
    for phase in range(THREE):
        first.step(phase)
    rest.start()
    first.finish()
    mats = (ma1, mb1, ma2, mb2, col)
    unflatten_layer(gath, ZERO, flat, (x3, n2, dbf, mix), stage_sem, w1, w2, slab)
    prep_layer(ZERO, slab, vrow, bd, v2, *mats)
    uq, dq = mix.at[ZERO:FOUR * TH, :], mix.at[FOUR * TH:EIGHT * TH, :]
    uch = mix.at[FOUR * TH:FOUR * TH + FOUR * QROWS, :]
    uh, dh = mix.at[ZERO:ALL_ROWS, ZERO:CHUNK], mix.at[ZERO:ALL_ROWS, CHUNK:TWO * CHUNK]
    acc1 = bd.at[ZERO:QROWS, :]
    forward_layer(ZERO, x0, x1, x2, vrow, ma1, ma2, col, w1, w2, uq, uch, at({ONE: lambda: rest.step(ZERO), THREE: lambda: rest.step(ONE), SEVEN: lambda: rest.step(TWO)}))
    rest.finish()
    unflatten_layer(gath, ONE, flat, (x3, n2, dbf, mix), stage_sem, w1, w2, slab)
    unflatten_head(gath, (x3, n2, dbf, mix), stage_sem, head, small)
    prep_layer(ONE, slab, vrow, bd, v2, *mats)
    forward_layer(ONE, x2, x3, n2, vrow, ma1, ma2, col, w1, w2, uq, uch, no_hook)
    head_pass(n2, labels, small, head, d, pool, srow, gsum, flat)

    bufs, sems = (leaving, t0, t1, t2, t3), (rs_send, rs_recv)
    thirds = ((ZERO, 352), (352, 352), (704, 336))
    reduces = [Reduce(flat, HEAD_ROWS, HEAD_ROWS, ((ZERO, 96), (96, 88), (184, 88)), own, HEAD_OFF, bufs, where, sems)]
    reduces += [Reduce(flat, SHARD_ROWS, SLOT_ROWS, thirds, own, l * SLOT_ROWS, bufs, where, sems) for l in (ONE, ZERO)]

    def done_one(work):
        def run():
            work.finish()
            for other in list(neighbours) + [partner]:
                pl.semaphore_signal(done, inc=ONE, device_id=(other,), device_id_type=MESH_ID)
        return run

    def go(work, phase):
        return lambda: work.step(phase)

    h, r1, r0 = reduces
    back = (d, vrow, w1, w2, n2, dbf, n2t, dt, uh, dh, dn2, flat, gsum, gb1)
    tok = (d, vrow, dn2, ma1, mb1, ma2, mb2, uq, dq, acc1, acc2, rowsum, colsum, gsum)
    small_parts = (flat, acc1, acc2, rowsum, colsum, gsum, gb1, v2)
    h.start()
    channel_back(ONE, x3, *back, at({-ONE: go(h, ZERO), ONE: go(h, ONE), TWO: go(h, TWO), FOUR: both(go(h, THREE), done_one(h))}))
    token_back(ONE, x2, x3, *tok, no_hook)
    small_flat(ONE, *small_parts)
    pl.semaphore_wait(done, FOUR)
    r1.start()
    channel_back(ZERO, x1, *back, at({-ONE: go(r1, ZERO), FOUR: go(r1, ONE), SIX: go(r1, TWO)}))
    r1.step(THREE)
    done_one(r1)()
    pl.semaphore_wait(done, FOUR)
    r0.start()
    token_back(ZERO, x0, x1, *tok, at({TWO: go(r0, ZERO)}))
    small_flat(ZERO, *small_parts)
    late[ZERO, ZERO:QVALID, :] = flat[ZERO:QVALID, :]
    late[ZERO, QVALID:240, :] = flat[ROW_VEC:FLAT_ROWS, :]
    hops = [partner, neighbours[TWO], neighbours[ONE], neighbours[ZERO]]

    def exchange(value, box_ref, sems, n):
        return pltpu.make_async_remote_copy(src_ref=value.at[n % TWO], dst_ref=box_ref.at[n], send_sem=sems[ZERO].at[n], recv_sem=sems[ONE].at[n], device_id=(hops[n],), device_id_type=MESH_ID)

    def late_copy(n):
        return exchange(late, late_box, (late_send, late_recv), n)
    def late_step(n):
        late_copy(n).wait()
        late[(n + ONE) % TWO] = late[n % TWO] + late_box[n]
        if n < THREE:
            late_copy(n + ONE).start()
    late_copy(ZERO).start()
    late_step(ZERO)
    r0.step(ONE)
    late_step(ONE)
    r0.step(TWO)
    late_step(TWO)
    r0.step(THREE)
    late_step(THREE)
    r0.finish()
    own[ZERO:QVALID, :] = jnp.where(me == ZERO, late[ZERO, ZERO:QVALID, :], own[ZERO:QVALID, :])
    last = ROW_VEC - 15 * SHARD_ROWS
    own[last:SHARD_ROWS, :] = jnp.where(me == 15, late[ZERO, QVALID:240, :], own[last:SHARD_ROWS, :])
    for l in range(TWO):
        own[l * SLOT_ROWS + SHARD_ROWS:l * SLOT_ROWS + SLOT_ROWS, :] = jnp.zeros((ONE, LANES), F32)
    box[me] = jnp.broadcast_to(jnp.sum(square_sum(own, ZERO, SMALL_OFF + EIGHT)), (STEP8, LANES))

    def tell(k):
        return pltpu.make_async_remote_copy(src_ref=box.at[me], dst_ref=box.at[me], send_sem=tiny_send.at[k], recv_sem=tiny_recv.at[k], device_id=((me + k) % DEVICES,), device_id_type=MESH_ID)
    for k in range(ONE, DEVICES):
        tell(k).start()
    for k in range(ONE, DEVICES):
        tell(k).wait()
    total = box[ZERO]
    for k in range(ONE, DEVICES):
        total = total + box[k]
    stat[ZERO] = total
    stat[ONE] = own[SMALL_OFF + EIGHT:SMALL_OFF + SIXTEEN, :]


def train_step(x0, labels, pack):
    vmem = pl.BlockSpec(memory_space=pltpu.VMEM)
    act = pltpu.VMEM((ALL_ROWS, CH), BF16)
    wide = pltpu.VMEM((ALL_ROWS, CH), F32)
    across = pltpu.VMEM((CH, ALL_ROWS), BF16)
    tall = pltpu.VMEM((TWO, FOUR * TH, QROWS), BF16)
    flat_mat = pltpu.VMEM((TWO, QROWS, FOUR * TH), BF16)
    acc = pltpu.VMEM((QROWS, FOUR * TH), F32)
    dma = pltpu.SemaphoreType.DMA
    return pl.pallas_call(
        step_kernel,
        out_shape=(jax.ShapeDtypeStruct((AG_ROWS, LANES), F32), jax.ShapeDtypeStruct((TWO, STEP8, LANES), F32), jax.ShapeDtypeStruct((TWO, TWO, TWO, TWO, AG_ROWS, LANES), BF16)),
        in_specs=[vmem] * THREE,
        out_specs=(vmem, vmem, pl.BlockSpec(memory_space=pl.ANY)),
        scratch_shapes=[act, act, act, wide, wide, act, act, across, across, pltpu.VMEM((EIGHT * TH, CH), BF16),
                        tall, flat_mat, flat_mat, tall, pltpu.VMEM((TWO, QROWS, LANES), F32), pltpu.VMEM((TWO, STEP8, HID), F32), pltpu.VMEM((IMAGES, LANES), F32), pltpu.VMEM((TWO * LANES, FOUR * TH), F32),
                        pltpu.VMEM((STEP8, CLASS_PAD), F32), pltpu.VMEM((IMAGES, CH), F32), pltpu.VMEM((FIVE, STEP8, CH), F32), pltpu.VMEM((STEP8, HID), F32), acc,
                        pltpu.VMEM((FOUR * TH, LANES), F32), pltpu.VMEM((TWO * LANES, LANES), F32), pltpu.VMEM((FLAT_ROWS + SIXTEEN, LANES), F32),
                        pltpu.VMEM((TWO, CH, HID), BF16), pltpu.VMEM((TWO, HID, CH), BF16), pltpu.VMEM((TWO, SLAB_ROWS, LANES), F32), pltpu.VMEM((CH, CLASS_PAD), BF16), pltpu.VMEM((SIXTEEN, LANES), F32),
                        pltpu.VMEM((TWO, TWO, TWO, SLOT_ROWS, LANES), F32), pltpu.VMEM((TWO, TWO, TWO, SLOT_ROWS, LANES), F32), pltpu.VMEM((TWO, TWO, SLOT_ROWS, LANES), F32), pltpu.VMEM((TWO, SLOT_ROWS, LANES), F32), pltpu.VMEM((SLOT_ROWS, LANES), F32),
                        pltpu.VMEM((DEVICES, STEP8, LANES), F32),
                        dma((42,)), dma((42,)), dma((12,)), dma((12,)), dma((SIXTEEN,)), dma, dma((DEVICES,)), dma((DEVICES,)), dma((FOUR,)), dma((FOUR,)), pltpu.SemaphoreType.REGULAR, pltpu.VMEM((TWO, SLAB_ROWS, LANES), F32), pltpu.VMEM((FOUR, SLAB_ROWS, LANES), F32)],
        compiler_params=pltpu.CompilerParams(collective_id=ZERO, has_side_effects=True, vmem_limit_bytes=67043328),
        name='train_step',
    )(x0, labels, pack)


LEARN_RATE = 0.003
BETA_ONE = 0.9
BETA_TWO = 0.999
ADAM_EPS = 1e-8
WEIGHT_DECAY = 0.03
ADAM_STEP = 10


def adam_update(master, gradient, moment, second, decay_rate):
    moment_new = BETA_ONE * moment + (F_ONE - BETA_ONE) * gradient
    second_new = BETA_TWO * second + (F_ONE - BETA_TWO) * gradient * gradient
    m_hat = moment_new / (F_ONE - BETA_ONE ** ADAM_STEP)
    v_hat = second_new / (F_ONE - BETA_TWO ** ADAM_STEP)
    master_new = master - LEARN_RATE * (m_hat / (jnp.sqrt(v_hat) + ADAM_EPS) + decay_rate * master)
    return master_new, moment_new, second_new

def adam_kernel(lp, lm, lv, hp, hm, hv, sp, sm, sv, own, stat, lp_o, lm_o, lv_o, hp_o, hm_o, hv_o, sp_o, sm_o, sv_o, loss, grad):
    step = pl.program_id(ZERO)
    clip = F_ONE / jnp.maximum(F_ONE, jnp.sqrt(stat[ZERO, ZERO:ONE, ZERO:ONE]))
    for l in range(TWO):
        for r in range(UPDATE_ROWS):
            grad[l:l + ONE, LANES * r:LANES * r + LANES] = own[pl.ds(l * SLOT_ROWS + UPDATE_ROWS * step + r, ONE), :]
    block = (TWO, UPDATE_ROWS * LANES)
    spot = iota(block, ONE) + (UPDATE_ROWS * LANES) * step + SHARD_ROWS * LANES * lax.axis_index('fsdp')
    decay = jnp.where(spot < ROW_VEC * LANES, WEIGHT_DECAY, F_ZERO)
    lp_o[...], lm_o[...], lv_o[...] = adam_update(lp[...], grad[...] * clip, lm[...], lv[...], decay)

    @pl.when(step == ZERO)
    def _():
        for j in range(EIGHT):
            lanes = slice(LANES * j, min(LANES * j + LANES, CLASSES))
            g = own[HEAD_OFF + IMAGES * j:HEAD_OFF + IMAGES * j + IMAGES, ZERO:lanes.stop - lanes.start] * clip
            hp_o[:, lanes], hm_o[:, lanes], hv_o[:, lanes] = adam_update(hp[:, lanes], g, hm[:, lanes], hv[:, lanes], WEIGHT_DECAY)
        sp_o[...], sm_o[...], sv_o[...] = adam_update(sp[...], own[SMALL_OFF:SMALL_OFF + ONE, :] * clip, sm[...], sv[...], F_ZERO)
        loss[...] = stat[ONE] / GLOBAL_IMAGES


def update(lp, lm, lv, hp, hm, hv, sp, sm, sv, own, stat):
    piece = pl.BlockSpec((TWO, UPDATE_ROWS * LANES), lambda i: (ZERO, i))

    def whole(x):
        return pl.BlockSpec(x.shape, lambda i: (ZERO,) * x.ndim)
    tile = jax.ShapeDtypeStruct((STEP8, LANES), F32)
    return pl.pallas_call(
        adam_kernel,
        grid=(pl.cdiv(SHARD_ROWS, UPDATE_ROWS),),
        out_shape=tuple(jax.ShapeDtypeStruct(x.shape, F32) for x in (lp, lm, lv, hp, hm, hv, sp, sm, sv)) + (tile,),
        in_specs=[piece] * THREE + [whole(x) for x in (hp, hm, hv, sp, sm, sv, own, stat)],
        out_specs=(piece,) * THREE + tuple(whole(x) for x in (hp, hm, hv, sp, sm, sv, tile)),
        scratch_shapes=[pltpu.VMEM((TWO, UPDATE_ROWS * LANES), F32)],
        name='update',
    )(lp, lm, lv, hp, hm, hv, sp, sm, sv, own, stat)


def solution(mesh):
    row_spec = P('fsdp')
    layer_spec = P(None, 'fsdp')
    in_specs = (row_spec, row_spec, layer_spec, row_spec, row_spec, layer_spec, row_spec, row_spec, layer_spec, row_spec, row_spec)
    out_specs = (P(),) + in_specs[TWO:]

    def device_step(act_in, labels, layer_p, head_w, small_p, layer_m, head_m, small_m, layer_v, head_v, small_v):
        quads = jnp.pad(act_in.reshape(QUADS, QVALID, CH), ((ZERO, ZERO), (ZERO, QROWS - QVALID), (ZERO, ZERO))).reshape(ALL_ROWS, CH)
        layer_bf = jnp.pad(layer_p.astype(BF16).reshape(TWO, SHARD_ROWS, LANES), ((ZERO, ZERO), (ZERO, ONE), (ZERO, ZERO)))
        head_bf = jnp.pad(head_w.astype(BF16), ((ZERO, ZERO), (ZERO, CLASS_PAD - CLASSES))).reshape(IMAGES, EIGHT, LANES).transpose(ONE, ZERO, TWO).reshape(TH, LANES)
        small_bf = jnp.pad(small_p.astype(BF16).reshape(ONE, LANES), ((ZERO, 15), (ZERO, ZERO)))
        pack = jnp.concatenate([layer_bf.reshape(TWO * SLOT_ROWS, LANES), head_bf, small_bf])
        own, stat, _ = train_step(quads, jnp.broadcast_to(labels[:, None], (IMAGES, LANES)), pack)
        flat_small = [x.reshape(ONE, LANES) for x in (small_p, small_m, small_v)]
        new_lp, new_lm, new_lv, new_hw, new_hm, new_hv, new_sp, new_sm, new_sv, loss = update(layer_p, layer_m, layer_v, head_w, head_m, head_v, *flat_small, own, stat)
        new_sp, new_sm, new_sv = [x.reshape(LANES) for x in (new_sp, new_sm, new_sv)]
        loss_value = loss[ZERO, ZERO]
        return (loss_value, new_lp, new_hw, new_sp, new_lm, new_hm, new_sm, new_lv, new_hv, new_sv)

    return jax.shard_map(device_step, mesh=mesh, in_specs=in_specs, out_specs=out_specs, check_vma=False)
```
